32 devices in a mesh: fsdp: 4 (over z), seq: 8 (over y, x, core).
Axes of the slice: x: 2, y: 2, z: 4, core: 2. Of those that a mesh axis runs over, the one named last changes fastest.
Arguments:
- tokens: bfloat16 [8, 1024, 2048], P('fsdp', 'seq'), may hold values from -6 to 6
- cotangent: bfloat16 [8, 1024, 2048], P('fsdp', 'seq'), may hold values from -6 to 6
- gain_first: bfloat16 [2048], P('fsdp'), may hold values from 0.5 to 1.5
- w_inputs: bfloat16 [3, 2048, 2048], P(None, 'fsdp'), may hold values from -0.125 to 0.125
- w_conv: bfloat16 [3, 4, 2048], P(None, None, 'fsdp'), may hold values from -3 to 3
- w_beta: bfloat16 [2048, 16], P('fsdp'), may hold values from -0.125 to 0.125
- gain_heads: bfloat16 [128], P('fsdp'), may hold values from 0.5 to 1.5
- w_output: bfloat16 [2048, 2048], P('fsdp'), may hold values from -0.125 to 0.125
- gain_second: bfloat16 [2048], P('fsdp'), may hold values from 0.5 to 1.5
- w_gate_up: bfloat16 [2, 2048, 5632], P(None, 'fsdp'), may hold values from -0.125 to 0.125
- w_down: bfloat16 [5632, 2048], P('fsdp'), may hold values from -0.078125 to 0.078125
Outputs:
- output: bfloat16 [8, 1024, 2048], P('fsdp', 'seq')
- input_grad: float32 [8, 1024, 2048], P('fsdp', 'seq')
- grad_gain_first: float32 [2048], P('fsdp')
- grad_w_inputs: float32 [3, 2048, 2048], P(None, 'fsdp')
- grad_w_conv: float32 [3, 4, 2048], P(None, None, 'fsdp')
- grad_w_beta: float32 [2048, 16], P('fsdp')
- grad_gain_heads: float32 [128], P('fsdp')
- grad_w_output: float32 [2048, 2048], P('fsdp')
- grad_gain_second: float32 [2048], P('fsdp')
- grad_w_gate_up: float32 [2, 2048, 5632], P(None, 'fsdp')
- grad_w_down: float32 [5632, 2048], P('fsdp')
The draws below stay inside these ranges and needn't reach their ends.
All inputs are finite; a program needn't handle non-finite values.
Results may differ from the reference program's by a relative error of at most 0.024.
Values may be sent and summed in bfloat16 or wider, within the bound.
No kernel may reach another device: no remote copies, remote signals or barrier semaphores. Data moves between devices by JAX's collectives and lax.ppermute only.
A program may use at most 704 MiB of HBM per device.

```python
import jax
import jax.numpy as jnp
from jax import lax

D = 2048
H = 16
DK = 128
FF = 5632
CONV = 4
BLOCK = 64
HD = 2048
LENGTH = 1024
SEQS = 8


def shard_levels(rng, extent, cuts, low, largest):
    def one(dim, blocks):
        draws = jax.random.uniform(jax.random.fold_in(jax.random.fold_in(rng, 6), dim), (blocks,), jnp.float32, low / len(cuts), largest / len(cuts))
        return jnp.repeat(jnp.exp(draws), extent[dim] // blocks).reshape((-1,) + (1,) * (len(extent) - dim - 1))

    factor_of = one(*cuts[0])
    for cut in cuts[1:]:
        factor_of = factor_of * one(*cut)
    return factor_of


def noise(stream_key, shape, width, limit, cuts=(), held_as=jnp.bfloat16):
    values = jax.random.normal(stream_key, shape, jnp.float32) * width
    if len(cuts) > 0:
        values = shard_levels(stream_key, shape, cuts, -0.22, 0.18) * values
    return jnp.clip(values, min=-limit, max=limit).astype(held_as)


def setup_inputs(seed: int = 0) -> dict:
    key_list = jax.random.split(jax.random.key(seed), 12)
    return {
        "tokens": noise(key_list[0], (SEQS, LENGTH, D), 1.0, 6.0, ((0, 4), (1, 8))),
        "cotangent": noise(key_list[1], (SEQS, LENGTH, D), 1.0, 6.0, ((0, 4), (1, 8))),
        "gain_first": jnp.clip(1.0 + 0.1 * jax.random.normal(key_list[2], (D,), jnp.float32), 0.5, 1.5).astype(jnp.bfloat16),
        "w_inputs": noise(key_list[3], (3, D, HD), D ** -0.5, 0.125, ((1, 4),)),
        "w_conv": noise(key_list[4], (3, CONV, HD), CONV ** -0.5, 3.0, ((2, 4),)),
        "w_beta": noise(key_list[5], (D, H), D ** -0.5, 0.125, ((0, 4),)),
        "gain_heads": jnp.clip(1.0 + 0.1 * jax.random.normal(key_list[6], (DK,), jnp.float32), 0.5, 1.5).astype(jnp.bfloat16),
        "w_output": noise(key_list[7], (HD, D), HD ** -0.5, 0.125, ((0, 4),)),
        "gain_second": jnp.clip(1.0 + 0.1 * jax.random.normal(key_list[8], (D,), jnp.float32), 0.5, 1.5).astype(jnp.bfloat16),
        "w_gate_up": noise(key_list[9], (2, D, FF), D ** -0.5, 0.125, ((1, 4),)),
        "w_down": noise(key_list[10], (FF, D), FF ** -0.5, 0.078125, ((0, 4),)),
    }


@jax.custom_vjp
def low(v):
    return lax.optimization_barrier(v.astype(jnp.bfloat16)).astype(jnp.float32)

@jax.custom_vjp
def low_back(v):
    return v

def low_keep(v):
    return (low(v), None)

def low_pass(kept, grad):
    return (grad,)

def back_keep(v):
    return (v, None)

def back_low(kept, grad):
    return (low(grad),)
low.defvjp(low_keep, low_pass)
low_back.defvjp(back_keep, back_low)

def contract(pattern, left_op, right_op):
    return jnp.einsum(pattern, left_op, right_op, precision=lax.Precision.HIGHEST)

def rms_rows(values, gain):
    return values * lax.rsqrt(lax.optimization_barrier(jnp.mean(values * values, axis=-1, keepdims=True)) + 1e-05) * gain

def unit_rows(values, factor):
    return values * lax.rsqrt(lax.optimization_barrier(jnp.sum(values * values, axis=-1, keepdims=True)) + 1e-06) * factor

def to_blocks(values):
    seq_count, length, head_count, head_dim = values.shape
    shaped = values.reshape(seq_count, length // BLOCK, BLOCK, head_count, head_dim)
    return shaped.transpose(1, 0, 3, 2, 4)

def strength_blocks(values):
    seq_count, length, head_count = values.shape
    return values.reshape(seq_count, length // BLOCK, BLOCK, head_count).transpose(1, 0, 3, 2)

def block_step(state, block_in):
    queries, key_rows, value_rows, strength = block_in
    block_len = key_rows.shape[-2]
    gram_mat = contract('bhck,bhdk->bhcd', key_rows, key_rows)
    lower_mat = jnp.eye(block_len, dtype=key_rows.dtype) + jnp.tril(strength[..., :, None] * gram_mat, -1)
    w_rows = lax.linalg.triangular_solve(lower_mat, strength[..., None] * key_rows, left_side=True, lower=True, unit_diagonal=True)
    u_rows = lax.linalg.triangular_solve(lower_mat, strength[..., None] * value_rows, left_side=True, lower=True, unit_diagonal=True)
    fresh_values = u_rows - contract('bhck,bhkv->bhcv', w_rows, state)
    scores = jnp.tril(contract('bhck,bhdk->bhcd', queries, key_rows))
    mixed = contract('bhck,bhkv->bhcv', queries, state) + contract('bhcd,bhdv->bhcv', scores, fresh_values)
    state = state + contract('bhck,bhcv->bhkv', key_rows, fresh_values)
    return (state, mixed)

def layer(tokens, gain_first, w_inputs, w_conv, w_beta, gain_heads, w_output, gain_second, w_gate_up, w_down):
    seq_count, length, model_width = tokens.shape
    normed = low(rms_rows(tokens, gain_first))
    project = low_back(low(contract('bld,cde->cble', normed, w_inputs)))
    padded = jnp.pad(project, ((0, 0), (0, 0), (CONV - 1, 0), (0, 0)))
    conved = jnp.zeros_like(project)
    for offset in range(CONV):
        conved = conved + w_conv[:, offset, None, None, :] * padded[:, :, offset:offset + length, :]
    active = jax.nn.silu(conved)
    pieces = active.reshape(3, seq_count, length, H, DK)
    queries = low(unit_rows(pieces[0], DK ** (-0.5)))
    key_rows = low(unit_rows(pieces[1], 1.0))
    value_rows = low(pieces[2])
    strength = jax.nn.sigmoid(low_back(contract('bld,dh->blh', normed, w_beta)))
    blocks = (to_blocks(queries), to_blocks(key_rows), to_blocks(value_rows), strength_blocks(strength))
    start_state = jnp.zeros((seq_count, H, DK, DK), tokens.dtype)
    final_state, mixed_blocks = lax.scan(jax.checkpoint(block_step), start_state, blocks)
    mixed = mixed_blocks.transpose(1, 0, 3, 2, 4).reshape(seq_count, length, H, DK)
    normed_out = low(rms_rows(mixed, gain_heads)).reshape(seq_count, length, HD)
    hidden = tokens + low_back(contract('ble,ed->bld', normed_out, w_output))
    normed_two = low(rms_rows(hidden, gain_second))
    gate_up = low_back(contract('bld,cdf->cblf', normed_two, w_gate_up))
    inner_act = low(jax.nn.silu(gate_up[0]) * gate_up[1])
    return hidden + low_back(contract('blf,fd->bld', inner_act, w_down))

def reference(tokens, cotangent, gain_first, w_inputs, w_conv, w_beta, gain_heads, w_output, gain_second, w_gate_up, w_down):
    params = tuple((weight.astype(jnp.float32) for weight in (gain_first, w_inputs, w_conv, w_beta, gain_heads, w_output, gain_second, w_gate_up, w_down)))
    result, pull_back = jax.vjp(layer, tokens.astype(jnp.float32), *params)
    grads = pull_back(cotangent.astype(jnp.float32))
    return (result.astype(jnp.bfloat16), grads[0], grads[1], grads[2], grads[3], grads[4], grads[5], grads[6], grads[7], grads[8], grads[9])
```

```python
import functools

import jax
import jax.numpy as jnp
from jax import lax
from jax.experimental import pallas as pl
from jax.experimental.pallas import tpu as pltpu
from jax.sharding import PartitionSpec as P

LOW = jnp.bfloat16
WIDE = jnp.float32


def swap(x, bits):
    count = lax.axis_size("seq")
    return lax.ppermute(x, "seq", [(i, i ^ bits) for i in range(count)])


def gather_start(x):
    if lax.axis_size("seq") == 8:
        return [x, swap(x, 1), swap(x, 2), swap(x, 4)]
    return [x]


def gather_far(first):
    if lax.axis_size("seq") != 8:
        return []
    x, _, side, back = first
    half = x.shape[0] // 2
    if x.shape[0] % 32 == 0:
        return [swap(back[:half], 2), swap(side[half:], 4)]
    return [swap(back, 2)]


def gather_rest(first, far):
    count, x = lax.axis_size("seq"), first[0]
    if count == 8:
        _, twin, side, back = first
        side_twin, back_twin = swap(side, 1), swap(back, 1)
        return [[x], [twin], [side], [side_twin], [back], [back_twin], far, [swap(f, 1) for f in far]]
    held, bits = x[None], 1
    while bits < count:
        held = jnp.concatenate([held, swap(held, bits)])
        bits *= 2
    return [[held[b]] for b in range(count)]


def gather_xor(x):
    first = gather_start(x)
    return gather_rest(first, gather_far(first))


def add(first, second):
    return (first.astype(WIDE) + second.astype(WIDE)).astype(LOW)


def reduce_start(odd):
    return swap(odd, 1) if lax.axis_size("seq") == 8 else odd


def reduce_far(even, twin):
    count = lax.axis_size("seq")
    if count == 8:
        half = even.shape[1] // 2
        far, side, back = (add(even[b], twin[b]) for b in (3, 1, 2))
        far_top, far_low = swap(far[:half], 2), swap(far[half:], 4)
        side_top, back_low = swap(side[:half], 2), swap(back[half:], 4)
        return [even[0], twin[0], side[half:], back[:half], side_top, back_low, far_top, far_low]
    parts = jnp.stack([even, twin], axis=1).reshape((count,) + even.shape[1:])
    bits = count // 2
    while bits:
        parts = add(parts[:bits], swap(parts[bits:], bits))
        bits //= 2
    return [parts[0]]


def reduce_last(state):
    if len(state) == 1:
        return [state]
    own, twin, side, back, side_top, back_low, far_top, far_low = state
    side_low = swap(add(side, far_low), 2)
    back_top = swap(add(back, far_top), 4)
    return [[own], [twin], [side_top, side_low], [back_top, back_low]]


def exchange_xor(parts):
    count = lax.axis_size("seq")
    if count == 8:
        twin = swap(parts[1], 1)
        out = [parts[0, :1], twin[:1]]
        for n in (1, 2, 3):
            out.append(swap(jnp.concatenate([parts[0, n : n + 1], twin[n : n + 1]]), 2 * n))
        return out
    return [parts[0, :1]] + [swap(parts[b % 2, b // 2][None], b) for b in range(1, count)]


def sum_over(axis, x):
    count, bits = lax.axis_size(axis), 1
    while bits < count:
        x = x + lax.ppermute(x, axis, [(i, i ^ bits) for i in range(count)])
        bits *= 2
    return x


def after(x, *others):
    return lax.optimization_barrier((x,) + others)[0]


def dot(a, b, left=1, right=0):
    return lax.dot_general(
        a.astype(LOW), b.astype(LOW), (((left,), (right,)), ((), ())), preferred_element_type=WIDE
    )


def iota(shape, dim):
    return lax.broadcasted_iota(jnp.int32, shape, dim)


def shifted(x, by):
    rows = x.shape[0]
    turned = pltpu.roll(x, by % rows, 0)
    row = iota(x.shape, 0)
    return jnp.where(row >= by if by > 0 else row < rows + by, turned, 0.0)


def conv_silu(x, taps):
    count = taps.shape[0]
    moved = [shifted(x, count - 1 - j) if j < count - 1 else x for j in range(count)]
    conved = sum(taps[j : j + 1] * moved[j] for j in range(count))
    gate = jax.nn.sigmoid(conved)
    return moved, conved, gate, conved * gate


def unit_scale(values):
    return lax.rsqrt(jnp.sum(values * values, axis=-1, keepdims=True) + 1e-06)


def pick_lane(block, lane):
    return jnp.sum(jnp.where(iota(block.shape, 1) == lane, block, 0.0), axis=-1, keepdims=True)


def invert_unit_lower(mats):
    size = mats[0].shape[0]
    row, col = iota((size, size), 0), iota((size, size), 1)
    invs = [jnp.where(row == col, 1.0, jnp.where(row // 2 == col // 2, -a, 0.0)) for a in mats]
    width = 2
    while width < size:
        mask = (row // (2 * width) == col // (2 * width)) & (row // width != col // width)
        part = [dot(t, jnp.where(mask, a, 0.0)) for t, a in zip(invs, mats)]
        invs = [t - dot(p, t) for t, p in zip(invs, part)]
        width *= 2
    return invs


def mixer_forward(
    place_ref, proj_ref, taps_ref, logit_ref, gain_ref, out_ref, mixed_ref, state_ref, inv_ref, w_ref, fresh_ref
):
    place, head = place_ref[0], pl.program_id(0)
    count, _, length, _ = proj_ref.shape
    dim = mixed_ref.shape[-1]
    spot = [jnp.bitwise_xor(place, i) for i in range(count)]
    whole = jnp.concatenate([proj_ref[j, 0] for j in spot]).astype(WIDE)
    acts = [conv_silu(whole[:, c * dim : (c + 1) * dim], taps_ref[0, c])[3] for c in range(3)]
    queries = (acts[0] * (unit_scale(acts[0]) * dim ** (-0.5))).astype(LOW)
    key_rows = (acts[1] * unit_scale(acts[1])).astype(LOW)
    value_rows = acts[2].astype(LOW)

    def cut(x):
        return [x[i * length : (i + 1) * length] for i in range(count)]

    q, k, v = cut(queries), cut(key_rows), cut(value_rows)
    beta = [jax.nn.sigmoid(pick_lane(logit_ref[j, 0], head)) for j in spot]
    row, col = iota((length, length), 0), iota((length, length), 1)
    lower = [jnp.where(row > col, b * dot(x, x, 1, 1), 0.0) for b, x in zip(beta, k)]
    invs = [t.astype(LOW) for t in invert_unit_lower(lower)]
    w = [dot(t, b * x.astype(WIDE)).astype(LOW) for t, b, x in zip(invs, beta, k)]
    u = [dot(t, b * x.astype(WIDE)) for t, b, x in zip(invs, beta, v)]
    scores = [jnp.where(row >= col, dot(a, b, 1, 1), 0.0).astype(LOW) for a, b in zip(q, k)]
    turn = [dot(a, b, 0, 0).astype(LOW) for a, b in zip(k, w)]
    push = [dot(a, b, 0, 0) for a, b in zip(k, u)]
    state = jnp.zeros((dim, dim), WIDE)
    states = []
    for i in range(count):
        states.append(state.astype(LOW))
        state = state + (push[i] - dot(turn[i], states[i]))
    fresh = [(a - dot(b, c)).astype(LOW) for a, b, c in zip(u, w, states)]
    gain = gain_ref[...]
    for i in range(count):
        mixed = dot(q[i], states[i]) + dot(scores[i], fresh[i])
        scale = lax.rsqrt(jnp.mean(mixed * mixed, axis=-1, keepdims=True) + 1e-05)
        mixed_ref[0, 0, i] = mixed
        out_ref[spot[i] & 1, spot[i] >> 1] = (mixed * scale * gain).astype(LOW)
        state_ref[0, 0, i] = states[i]
        inv_ref[0, 0, i] = invs[i]
        w_ref[0, 0, i] = w[i]
        fresh_ref[0, 0, i] = fresh[i]


def mixer_backward(stacks, place_ref, proj_ref, taps_ref, logit_ref, gain_ref, *refs):
    gout_refs, refs = refs[: len(stacks)], refs[len(stacks) :]
    mixed_ref, state_ref, inv_ref, w_ref, fresh_ref = refs[:5]
    gproj_ref, glogit_ref, gtaps_ref, ggain_ref, gout_ref = refs[-5:]
    at = 0
    for ref, size in zip(gout_refs, stacks):
        gout_ref[at : at + size] = ref[...]
        at += size
    place, head = place_ref[0], pl.program_id(0)
    count, _, length, _ = proj_ref.shape
    dim = mixed_ref.shape[-1]
    spot = [jnp.bitwise_xor(place, i) for i in range(count)]
    whole = jnp.concatenate([proj_ref[j, 0] for j in spot]).astype(WIDE)
    convs = [conv_silu(whole[:, c * dim : (c + 1) * dim], taps_ref[0, c]) for c in range(3)]
    acts = [c[3] for c in convs]
    q_scale, k_scale = unit_scale(acts[0]), unit_scale(acts[1])
    factor = dim ** (-0.5)

    def cut(x):
        return [x[i * length : (i + 1) * length] for i in range(count)]

    q = cut((acts[0] * (q_scale * factor)).astype(LOW))
    k = cut((acts[1] * k_scale).astype(LOW))
    v = cut(acts[2].astype(LOW))
    beta = [jax.nn.sigmoid(pick_lane(logit_ref[j, 0], head)) for j in spot]
    row, col = iota((length, length), 0), iota((length, length), 1)
    gain = gain_ref[...]
    gain_sum = jnp.zeros((1, dim), WIDE)
    gm = []
    for i in range(count):
        mixed = mixed_ref[0, 0, i]
        scale = lax.rsqrt(jnp.mean(mixed * mixed, axis=-1, keepdims=True) + 1e-05)
        grad = gout_ref[spot[i]].astype(WIDE)
        gain_sum = gain_sum + jnp.sum(grad * mixed * scale, axis=0, keepdims=True)
        weighted = grad * gain
        back = scale * weighted - mixed * (
            scale * scale * scale * jnp.mean(mixed * weighted, axis=-1, keepdims=True)
        )
        gm.append(back.astype(LOW))
    ggain_ref[0] = gain_sum
    inv, w, fresh, states = ([r[0, 0, i] for i in range(count)] for r in (inv_ref, w_ref, fresh_ref, state_ref))
    gram = [dot(x, x, 1, 1) for x in k]
    scores = [jnp.where(row >= col, dot(a, b, 1, 1), 0.0).astype(LOW) for a, b in zip(q, k)]
    turn = [dot(a, b, 0, 0).astype(LOW) for a, b in zip(k, w)]
    direct = [dot(a, b, 0, 0) for a, b in zip(scores, gm)]
    enter = [dot(a, b, 0, 0) - dot(c, d, 0, 0) for a, b, c, d in zip(q, gm, w, direct)]
    gstate = jnp.zeros((dim, dim), WIDE)
    late = [None] * count
    for i in reversed(range(count)):
        late[i] = gstate.astype(LOW)
        gstate = gstate + (enter[i] - dot(turn[i], late[i], 0, 0))
    gfresh = [a + dot(b, c) for a, b, c in zip(direct, k, late)]
    g = [dot(a, b, 0, 0) for a, b in zip(inv, gfresh)]
    g_low = [x.astype(LOW) for x in g]
    gs = [dot(a, b, 1, 1) for a, b in zip(g_low, states)]
    ga = [jnp.where(row > col, -dot(a, b, 1, 1), 0.0) for a, b in zip(g_low, fresh)]
    gscore = [jnp.where(row >= col, dot(a, b, 1, 1), 0.0).astype(LOW) for a, b in zip(gm, fresh)]
    gq = [dot(a, b, 1, 1) + dot(c, d) for a, b, c, d in zip(gm, states, gscore, k)]
    weighted_a = [b * a for b, a in zip(beta, ga)]
    gk = [
        dot(f, d, 1, 1) + dot(sc, qq, 0, 0) - b * s + dot(wa, kk) + dot(wa, kk, 0, 0)
        for f, d, sc, qq, b, s, wa, kk in zip(fresh, late, gscore, q, beta, gs, weighted_a, k)
    ]
    gv = [b * x for b, x in zip(beta, g)]
    lane = iota((length, glogit_ref.shape[-1]), 1)
    for i in range(count):
        gbeta = jnp.sum(
            g[i] * v[i].astype(WIDE) - gs[i] * k[i].astype(WIDE) + ga[i] * gram[i], axis=-1, keepdims=True
        )
        glogit = gbeta * beta[i] * (1.0 - beta[i])
        before = glogit_ref[spot[i], 0]
        keep = jnp.where(lane < head, before.astype(WIDE), 0.0)
        glogit_ref[spot[i], 0] = jnp.where(lane == head, glogit, keep).astype(LOW)

    def unit_back(values, scale, grad):
        return scale * grad - values * (
            scale * scale * scale * jnp.sum(values * grad, axis=-1, keepdims=True)
        )

    gacts = [
        unit_back(acts[0], q_scale, jnp.concatenate(gq) * factor),
        unit_back(acts[1], k_scale, jnp.concatenate(gk)),
        jnp.concatenate(gv),
    ]
    for c in range(3):
        moved, conved, gate, _ = convs[c]
        gconv = gacts[c] * gate * (1.0 + conved * (1.0 - gate))
        taps = taps_ref[0, c]
        gtaps_ref[0, c] = jnp.concatenate([jnp.sum(gconv * m, axis=0, keepdims=True) for m in moved])
        last = len(moved) - 1
        gp = taps[last : last + 1] * gconv
        for j in range(last):
            gp = gp + taps[j : j + 1] * shifted(gconv, j - last)
        gp = gp.astype(LOW)
        for i in range(count):
            gproj_ref[spot[i], 0, :, c * dim : (c + 1) * dim] = gp[i * length : (i + 1) * length]


def mixer_specs(b, count, length, dim, lanes, taps):
    small = [
        pl.BlockSpec((count, 1, length, 3 * dim), lambda h, p: (0, b, 0, h)),
        pl.BlockSpec((1, 3, taps, dim), lambda h, p: (h, 0, 0, 0)),
        pl.BlockSpec((count, 1, length, lanes), lambda h, p: (0, b, 0, 0)),
        pl.BlockSpec((1, dim), lambda h, p: (0, 0)),
    ]
    saved = pl.BlockSpec((1, 1, count, length, dim), lambda h, p: (0, h, 0, 0, 0))
    square = pl.BlockSpec((1, 1, count, dim, dim), lambda h, p: (0, h, 0, 0, 0))
    inverse = pl.BlockSpec((1, 1, count, length, length), lambda h, p: (0, h, 0, 0, 0))
    return small, [saved, square, inverse, saved, saved]


def run_mixer_forward(b, place, proj, taps, logits, gain):
    count, _, length, width = proj.shape
    heads, _, tap_count, dim = taps.shape
    small, saved = mixer_specs(b, count, length, dim, logits.shape[-1], tap_count)
    shapes = [
        jax.ShapeDtypeStruct((2, count // 2, length, heads * dim), LOW),
        jax.ShapeDtypeStruct((1, heads, count, length, dim), WIDE),
        jax.ShapeDtypeStruct((1, heads, count, dim, dim), LOW),
        jax.ShapeDtypeStruct((1, heads, count, length, length), LOW),
        jax.ShapeDtypeStruct((1, heads, count, length, dim), LOW),
        jax.ShapeDtypeStruct((1, heads, count, length, dim), LOW),
    ]
    out = pl.BlockSpec((2, count // 2, length, dim), lambda h, p: (0, 0, 0, h))
    return pl.pallas_call(
        mixer_forward,
        out_shape=shapes,
        grid_spec=pltpu.PrefetchScalarGridSpec(
            num_scalar_prefetch=1, grid=(heads,), in_specs=small, out_specs=[out] + saved
        ),
        compiler_params=pltpu.CompilerParams(vmem_limit_bytes=56 * 2**20),
        cost_estimate=cost(10),
        name="mixer_forward",
    )(place, proj, taps, logits, gain)


def run_mixer_backward(b, place, proj, taps, logits, gain, gout, saved_values, held):
    count, _, length, width = proj.shape
    heads, _, tap_count, dim = taps.shape
    small, saved = mixer_specs(b, count, length, dim, logits.shape[-1], tap_count)
    shapes = [
        jax.ShapeDtypeStruct(proj.shape, LOW),
        jax.ShapeDtypeStruct(logits.shape, LOW),
        jax.ShapeDtypeStruct((heads, 3, tap_count, dim), WIDE),
        jax.ShapeDtypeStruct((heads, 1, dim), WIDE),
    ]
    outs = [
        small[0],
        small[2],
        pl.BlockSpec((1, 3, tap_count, dim), lambda h, p: (h, 0, 0, 0)),
        pl.BlockSpec((1, 1, dim), lambda h, p: (h, 0, 0)),
    ]
    sizes = [g.shape[0] for g in gout]
    gouts = [pl.BlockSpec((n, length, dim), lambda h, p: (0, 0, h)) for n in sizes]
    held = list(held or [])
    first = 1 + len(small) + len(gouts) + len(saved)
    return pl.pallas_call(
        functools.partial(mixer_backward, sizes),
        out_shape=shapes,
        grid_spec=pltpu.PrefetchScalarGridSpec(
            num_scalar_prefetch=1,
            grid=(heads,),
            in_specs=small + gouts + saved + [ANY] * len(held),
            out_specs=outs,
            scratch_shapes=[pltpu.VMEM((count, length, dim), LOW)],
        ),
        input_output_aliases={first + n: n for n in range(len(held))},
        compiler_params=pltpu.CompilerParams(vmem_limit_bytes=56 * 2**20),
        cost_estimate=cost(13),
        name="mixer_backward",
    )(place, proj, taps, logits, gain, *gout, *saved_values, *held)


ANY = pl.BlockSpec(memory_space=pl.ANY)
FULL = pltpu.VMEM
PARAMS = pltpu.CompilerParams(vmem_limit_bytes=60 * 2**20)


def cost(micros):
    return pl.CostEstimate(flops=int(micros * 0.5e9), transcendentals=0, bytes_accessed=0)


def fetch(entries, refs, buf, sems):
    copies, n = [], 0
    for b, entry in enumerate(entries):
        row, mine = 0, []
        for size in entry:
            copy = pltpu.make_async_copy(refs[n], buf.at[b, pl.ds(row, size)], sems.at[n])
            copy.start()
            mine.append(copy)
            row, n = row + size, n + 1
        copies.append(mine)
    return copies


def heights(entries):
    return [[a.shape[0] for a in entry] for entry in entries]


def flat(entries):
    return [a for entry in entries for a in entry]


def project_kernel(entries, *refs):
    n = sum(len(e) for e in entries)
    w_ref, beta_ref, proj_ref, logit_ref, all_ref, buf, sems, out_sems = refs[n:]
    copies = fetch(entries, refs[:n], buf, sems)
    outs = []
    for b, mine in enumerate(copies):
        for c in mine:
            c.wait()
        out = pltpu.make_async_copy(buf.at[b], all_ref.at[b], out_sems.at[b])
        out.start()
        outs.append(out)
        x = buf[b]
        proj_ref[b] = dot(x, w_ref[...]).astype(LOW)
        logit_ref[b] = dot(x, beta_ref[...], 1, 1)
    for out in outs:
        out.wait()


def run_project(entries, w, beta, cols):
    sizes = heights(entries)
    count, rows = len(sizes), sum(sizes[0])
    pieces = flat(entries)
    width = pieces[0].shape[1]
    return pl.pallas_call(
        functools.partial(project_kernel, sizes),
        grid=(1,),
        in_specs=[ANY] * len(pieces)
        + [pl.BlockSpec((width, cols), lambda g: (0, 0)), pl.BlockSpec(beta.shape, lambda g: (0, 0))],
        out_specs=[
            pl.BlockSpec((count, rows, cols), lambda g: (0, 0, 0)),
            pl.BlockSpec((count, rows, beta.shape[0]), lambda g: (0, 0, 0)),
            ANY,
        ],
        out_shape=[
            jax.ShapeDtypeStruct((count, rows, cols), LOW),
            jax.ShapeDtypeStruct((count, rows, beta.shape[0]), WIDE),
            jax.ShapeDtypeStruct((count, rows, width), LOW),
        ],
        scratch_shapes=[
            pltpu.VMEM((count, rows, width), LOW),
            pltpu.SemaphoreType.DMA((len(pieces),)),
            pltpu.SemaphoreType.DMA((count,)),
        ],
        compiler_params=PARAMS,
        cost_estimate=cost(16),
        name="project",
    )(*pieces, w, beta)


def gate_kernel(entries, others, *refs):
    n = sum(len(e) for e in entries)
    m = n + sum(len(e) for e in others)
    w_ref, inner_ref, up_ref, gate_ref, all_ref, side_ref = refs[m : m + 6]
    buf, side, sems, out_sems, side_sems, back_sems = refs[m + 6 :]
    copies = fetch(entries, refs[:n], buf, sems)
    beside = fetch(others, refs[n:m], side, side_sems)
    ff = inner_ref.shape[-1]
    outs = []
    for b, mine in enumerate(copies):
        for c in mine:
            c.wait()
        out = pltpu.make_async_copy(buf.at[b], all_ref.at[b], out_sems.at[b])
        out.start()
        outs.append(out)
        both = dot(buf[b], w_ref[...])
        gate, up = both[:, :ff], both[:, ff:]
        sig = jax.nn.sigmoid(gate)
        swish = gate * sig
        inner_ref[b] = (swish * up).astype(LOW)
        gate_ref[b] = (up * sig * (1.0 + gate * (1.0 - sig))).astype(LOW)
        up_ref[b] = swish.astype(LOW)
        for c in beside[b]:
            c.wait()
        out = pltpu.make_async_copy(side.at[b], side_ref.at[b], back_sems.at[b])
        out.start()
        outs.append(out)
    for out in outs:
        out.wait()


def run_gate(entries, others, w):
    sizes = heights(entries)
    beside = flat(others)
    count, rows = len(sizes), sum(sizes[0])
    pieces = flat(entries)
    width, ff = pieces[0].shape[1], w.shape[1] // 2
    return pl.pallas_call(
        functools.partial(gate_kernel, sizes, heights(others)),
        in_specs=[ANY] * (len(pieces) + len(beside)) + [pl.BlockSpec(memory_space=FULL)],
        out_specs=[pl.BlockSpec(memory_space=FULL)] * 3 + [ANY] * 2,
        out_shape=[jax.ShapeDtypeStruct((count, rows, ff), LOW)] * 3
        + [jax.ShapeDtypeStruct((count, rows, width), LOW)] * 2,
        scratch_shapes=[
            pltpu.VMEM((count, rows, width), LOW),
            pltpu.VMEM((count, rows, width), LOW),
            pltpu.SemaphoreType.DMA((len(pieces),)),
            pltpu.SemaphoreType.DMA((count,)),
            pltpu.SemaphoreType.DMA((len(beside),)),
            pltpu.SemaphoreType.DMA((count,)),
        ],
        compiler_params=PARAMS,
        cost_estimate=cost(25),
        name="gate",
    )(*pieces, *beside, w)


def gate_back_kernel(cot_ref, up_ref, gate_ref, down_ref, w_ref, grad_ref, even_ref, odd_ref):
    _, rows, width = cot_ref.shape
    grad = dot(cot_ref[...].reshape(2 * rows, width), down_ref[...], 1, 1)
    gate, up = (r[...].reshape(2 * rows, r.shape[-1]).astype(WIDE) for r in (gate_ref, up_ref))
    both = jnp.concatenate([grad * gate, grad * up], axis=1).astype(LOW)
    grad_ref[...] = both.reshape(grad_ref.shape)
    two = dot(both, w_ref[...], 1, 1).astype(LOW)
    even_ref[0] = two[:rows]
    odd_ref[0] = two[rows:]


def run_gate_back(cot, up, gate, down, w):
    count, rows, width = cot.shape
    ff = up.shape[-1]

    def block(cols, depth=2):
        return pl.BlockSpec((depth, rows, cols), lambda b: (b, 0, 0))

    def once(x):
        return pl.BlockSpec(x.shape, lambda b: (0, 0), pipeline_mode=pl.Buffered(1))

    half = jax.ShapeDtypeStruct((count // 2, rows, width), LOW)
    return pl.pallas_call(
        gate_back_kernel,
        grid=(count // 2,),
        in_specs=[block(width), block(ff), block(ff), once(down), once(w)],
        out_specs=[block(2 * ff), block(width, 1), block(width, 1)],
        out_shape=[jax.ShapeDtypeStruct((count, rows, 2 * ff), LOW), half, half],
        compiler_params=PARAMS,
        cost_estimate=cost(32),
        name="gate_back",
    )(cot, up, gate, down, w)


def pairs_kernel(count, right, *refs):
    even_ref, odd_ref = refs[2 * count :]
    rows = even_ref.shape[1]
    total = 0.0
    for n in range(count):
        x, w = refs[n], refs[count + n]
        total = total + dot(x[...].reshape(2 * rows, x.shape[-1]), w[...], 1, right[n])
    total = total.astype(LOW)
    even_ref[0] = total[:rows]
    odd_ref[0] = total[rows:]


def run_pairs(terms, width, name):
    count, rows, _ = terms[0][0].shape
    half = jax.ShapeDtypeStruct((count // 2, rows, width), LOW)
    weight_specs = []
    for x, w, right in terms:
        shape = (x.shape[-1], width) if right == 0 else (width, x.shape[-1])
        weight_specs.append(pl.BlockSpec(shape, lambda b: (0, 0), pipeline_mode=pl.Buffered(1)))
    return pl.pallas_call(
        functools.partial(pairs_kernel, len(terms), [t[2] for t in terms]),
        grid=(count // 2,),
        in_specs=[pl.BlockSpec((2, rows, t[0].shape[-1]), lambda b: (b, 0, 0)) for t in terms] + weight_specs,
        out_specs=[pl.BlockSpec((1, rows, width), lambda b: (b, 0, 0))] * 2,
        out_shape=[half, half],
        compiler_params=PARAMS,
        cost_estimate=cost(12),
        name=name,
    )(*[t[0] for t in terms], *[t[1] for t in terms])


def branch_kernel(entries, place_ref, *refs):
    n = sum(len(e) for e in entries)
    count = len(entries)
    parts, (token_ref, gain_ref, hidden_ref, two_ref, rows_ref, buf, sems) = refs[n:-7], refs[-7:]
    copies = fetch(entries, refs[:n], buf, sems)
    place = place_ref[0]
    wide = parts[0].shape[-1]

    def spot(b):
        return pl.ds(pl.multiple_of(jnp.bitwise_xor(place, b) * wide, wide), wide)

    row, at = 0, 0
    for ref in parts:
        size, length, _ = ref.shape
        for i in range(size):
            rows_ref[row : row + length, spot(at + i)] = ref[i]
        at += size
        if at == count:
            row, at = row + length, 0
    rows = rows_ref[...]
    for b, mine in enumerate(copies):
        for c in mine:
            c.wait()
        hidden_ref[:, spot(b)] = dot(rows, buf[b])
    hidden = hidden_ref[...] + token_ref[...].astype(WIDE)
    hidden_ref[...] = hidden
    scale = lax.rsqrt(jnp.mean(hidden * hidden, axis=-1, keepdims=True) + 1e-05)
    two_ref[...] = (hidden * scale * gain_ref[...]).astype(LOW)


def run_branch(place, entries, parts, tokens, gain):
    sizes = heights(entries)
    pieces = flat(entries)
    depth, wide = sum(sizes[0]), parts[0].shape[-1]
    vmem = pl.BlockSpec(memory_space=FULL)
    return pl.pallas_call(
        functools.partial(branch_kernel, sizes),
        in_specs=[pl.BlockSpec(memory_space=pltpu.SMEM)] + [ANY] * len(pieces) + [vmem] * (len(parts) + 2),
        out_specs=[vmem] * 3,
        out_shape=[
            jax.ShapeDtypeStruct(tokens.shape, WIDE),
            jax.ShapeDtypeStruct(tokens.shape, LOW),
            jax.ShapeDtypeStruct((tokens.shape[0], depth), LOW),
        ],
        scratch_shapes=[
            pltpu.VMEM((len(sizes), depth, wide), LOW),
            pltpu.SemaphoreType.DMA((len(pieces),)),
        ],
        compiler_params=PARAMS,
        cost_estimate=cost(10),
        name="branch",
    )(place, *pieces, *parts, tokens, gain)


def branch_back_kernel(entries, grads, place_ref, *refs):
    n = sum(len(e) for e in entries)
    m = sum(len(e) for e in grads)
    count = len(entries)
    adds, (hidden_ref, cot_ref, gain_ref) = refs[n : n + m], refs[n + m : n + m + 3]
    ghidden_ref, gsum_ref, gbranch_ref, *gout_refs, buf, gout_all, sems = refs[n + m + 3 :]
    copies = fetch(entries, refs[:n], buf, sems)
    place = place_ref[0]
    wide = gbranch_ref.shape[-1]
    total, at = 0.0, 0
    for entry in grads:
        here = [adds[at + i][...].astype(WIDE) for i in range(len(entry))]
        at += len(entry)
        total = total + (jnp.concatenate(here) if len(here) > 1 else here[0])
    hidden = hidden_ref[...]
    scale = lax.rsqrt(jnp.mean(hidden * hidden, axis=-1, keepdims=True) + 1e-05)
    gsum_ref[...] = jnp.sum(total * hidden * scale, axis=0, keepdims=True)
    weighted = total * gain_ref[...]
    back = scale * weighted - hidden * (
        scale * scale * scale * jnp.mean(hidden * weighted, axis=-1, keepdims=True)
    )
    ghidden_ref[...] = cot_ref[...].astype(WIDE) + back

    def spot(b):
        return pl.ds(pl.multiple_of(jnp.bitwise_xor(place, b) * wide, wide), wide)

    for b, mine in enumerate(copies):
        for c in mine:
            c.wait()
        gbranch = ghidden_ref[:, spot(b)].astype(LOW)
        gbranch_ref[b % 2, b // 2] = gbranch
        part = dot(gbranch, buf[b], 1, 1)
        if b == 0:
            gout_all[...] = part
        else:
            gout_all[...] += part
    for b in range(count):
        for i, ref in enumerate(gout_refs):
            length = ref.shape[2]
            ref[b % 2, b // 2] = gout_all[i * length : (i + 1) * length, spot(b)].astype(LOW)


def run_branch_back(place, entries, grads, hidden, cot, gain, seqs):
    sizes, grad_sizes = heights(entries), heights(grads)
    pieces, adds = flat(entries), flat(grads)
    count, depth, wide = len(sizes), sum(sizes[0]), pieces[0].shape[1]
    rows = hidden.shape[0]
    vmem = pl.BlockSpec(memory_space=FULL)
    return pl.pallas_call(
        functools.partial(branch_back_kernel, sizes, grad_sizes),
        in_specs=[pl.BlockSpec(memory_space=pltpu.SMEM)] + [ANY] * len(pieces) + [vmem] * (len(adds) + 3),
        out_specs=[vmem] * (3 + seqs),
        out_shape=[
            jax.ShapeDtypeStruct(hidden.shape, WIDE),
            jax.ShapeDtypeStruct((1, hidden.shape[1]), WIDE),
            jax.ShapeDtypeStruct((2, count // 2, rows, wide), LOW),
        ]
        + [jax.ShapeDtypeStruct((2, count // 2, rows // seqs, wide), LOW)] * seqs,
        scratch_shapes=[
            pltpu.VMEM((count, depth, wide), LOW),
            pltpu.VMEM((rows, depth), WIDE),
            pltpu.SemaphoreType.DMA((len(pieces),)),
        ],
        compiler_params=PARAMS,
        cost_estimate=cost(10),
        name="branch_back",
    )(place, *pieces, *adds, hidden, cot, gain)


def outer_kernel(entries, stacks, *refs):
    n = sum(len(e) for e in entries)
    cols, out_ref, total_ref = refs[n : n + len(stacks)], refs[-2], refs[-1]
    spots = [(ref, i) for ref, size in zip(cols, stacks) for i in range(size)]
    at = 0
    for (ref, i), entry in zip(spots, entries):
        row = 0
        for size in entry:
            part = dot(refs[at][...], ref[i, row : row + size], 0, 0)
            total_ref[...] = part if at == 0 else total_ref[...] + part
            row, at = row + size, at + 1
    out_ref[...] = total_ref[...].astype(LOW)


def run_outer(entries, cols, name):
    pieces = flat(entries)
    shape = (pieces[0].shape[1], cols[0].shape[-1])
    vmem = pl.BlockSpec(memory_space=FULL)
    return pl.pallas_call(
        functools.partial(outer_kernel, heights(entries), [c.shape[0] for c in cols]),
        in_specs=[vmem] * (len(pieces) + len(cols)),
        out_specs=vmem,
        out_shape=jax.ShapeDtypeStruct(shape, LOW),
        scratch_shapes=[pltpu.VMEM(shape, WIDE)],
        compiler_params=PARAMS,
        cost_estimate=cost(8),
        name=name,
    )(*pieces, *cols)


def spread_kernel(entries, layout, place_ref, *refs):
    n = sum(len(e) for e in entries)
    out_ref, held = refs[n:]
    step, steps, at = pl.program_id(0), pl.num_programs(0), 0
    for b, entry in enumerate(entries):
        value = refs[at][...]
        if len(entry) > 1:
            value = jnp.where(step < steps // 2, value, refs[at + 1][...])
        held[jnp.bitwise_xor(place_ref[0], b)] = value
        at += len(entry)
    for i in range(len(entries)):
        for src, width, index in layout(i):
            out_ref[index] = held[i, :, src : src + width].astype(WIDE)


def run_spread(place, entries, piece_block, steps, layout, shape, block, index, name):
    specs = []
    for entry in entries:
        if len(entry) > 1:
            specs.append(pl.BlockSpec(piece_block, lambda g: (jnp.minimum(g, steps // 2 - 1), 0)))
            specs.append(pl.BlockSpec(piece_block, lambda g: (jnp.maximum(g - steps // 2, 0), 0)))
        elif piece_block[0] == entry[0].shape[0]:
            specs.append(pl.BlockSpec(piece_block, lambda g: (0, g)))
        else:
            specs.append(pl.BlockSpec(piece_block, lambda g: (g, 0)))
    return pl.pallas_call(
        functools.partial(spread_kernel, heights(entries), layout),
        grid=(steps,),
        in_specs=[pl.BlockSpec(memory_space=pltpu.SMEM)] + specs,
        out_specs=pl.BlockSpec(block, index),
        out_shape=jax.ShapeDtypeStruct(shape, WIDE),
        scratch_shapes=[pltpu.VMEM((len(entries),) + piece_block, LOW)],
        compiler_params=PARAMS,
        cost_estimate=cost(10),
        name=name,
    )(place, *flat(entries))


def norm_back(values, scale, grad, gain):
    weighted = grad * gain
    return scale * weighted - values * scale**3 * jnp.mean(values * weighted, axis=-1, keepdims=True)


def local(
    tokens,
    cotangent,
    gain_first,
    w_inputs,
    w_conv,
    w_beta,
    gain_heads,
    w_output,
    gain_second,
    w_gate_up,
    w_down,
):
    shards, count, place = lax.axis_size("fsdp"), lax.axis_size("seq"), lax.axis_index("seq")
    shard = lax.axis_index("fsdp")
    seqs, length, width = tokens.shape
    rows = seqs * length
    part = width // shards
    all_heads = w_beta.shape[1]
    heads = all_heads // count
    wide = heads * (w_output.shape[0] * shards // all_heads)
    dim = wide // heads
    hidden_part = w_down.shape[0]
    piece = hidden_part // count
    taps = w_conv.shape[1]
    place_arr = jnp.reshape(place, (1,)).astype(jnp.int32)

    def over_shards(x, axis=0):
        return lax.all_gather(x, "fsdp", axis=axis, tiled=True)

    packed = jnp.concatenate(
        [
            gain_first[None],
            gain_second[None],
            jnp.pad(gain_heads[None], ((0, 0), (0, part - gain_heads.shape[0]))),
            w_conv.reshape(3 * taps, part),
            w_beta.T,
        ]
    )
    packed = lax.all_gather(packed, "fsdp", axis=0)
    first_weight = packed[:, 0].reshape(width).astype(WIDE)
    second_weight = packed[:, 1].reshape(width).astype(WIDE)
    head_weight = packed[:, 2, : gain_heads.shape[0]].reshape(1, dim).astype(WIDE)
    conv_all = packed[:, 3 : 3 + 3 * taps].transpose(1, 0, 2).reshape(3, taps, width)
    conv_own = lax.dynamic_slice_in_dim(conv_all, place * wide, wide, 2).astype(WIDE)
    conv_own = conv_own.reshape(3, taps, heads, dim).transpose(2, 0, 1, 3)
    beta_all = packed[:, 3 + 3 * taps :].transpose(1, 0, 2).reshape(all_heads, width)
    beta_own = lax.dynamic_slice_in_dim(beta_all, place * heads, heads, 0)
    beta_own = jnp.pad(beta_own, ((0, 128 - heads), (0, 0)))

    ff = piece * shards
    win = lax.dynamic_slice_in_dim(w_inputs, place * wide, wide, 2)
    win = win.reshape(3, part, heads, dim).transpose(1, 2, 0, 3).reshape(part, 3 * wide)
    wio = jnp.concatenate([win, lax.dynamic_slice_in_dim(w_output, place * wide, wide, 1)], axis=1)
    later = after(place, wio)
    pieces = [
        lax.dynamic_slice(w_gate_up, (0, 0, f * hidden_part + later * piece), (2, part, piece)) for f in range(shards)
    ]
    wgu_own = jnp.concatenate([p[c] for c in range(2) for p in pieces], axis=1)
    later = after(later, wgu_own)
    wdown_own = lax.dynamic_slice_in_dim(w_down, later * piece, piece, 0)
    wio = over_shards(wio)
    wgu = over_shards(wgu_own)
    wdown = over_shards(wdown_own)

    inputs = tokens.reshape(rows, width).astype(WIDE)
    first_scale = lax.rsqrt(jnp.mean(inputs * inputs, axis=-1, keepdims=True) + 1e-05)
    normed = (inputs * first_scale * first_weight).astype(LOW)
    cot_own = cotangent.reshape(rows, width)
    cot_first = gather_start(cot_own)
    normed_first = gather_start(after(normed, wgu_own, wdown_own, *cot_first))
    normed_far = gather_far(normed_first)
    normed_parts = gather_rest(normed_first, normed_far)
    cot_far = gather_far([after(c, *normed_far) for c in cot_first])
    cot_parts = gather_rest(cot_first, cot_far)

    wio_late = after(wio, *cot_far)
    proj, logits, normed_all = run_project(normed_parts, wio_late, beta_own, 3 * wide)
    wout_first = gather_start(wio[:, 3 * wide :])
    proj = proj.reshape(count, seqs, length, 3 * wide)
    logits = logits.reshape(count, seqs, length, 128)
    wout_far, out_parts, saved = [], [], []
    for b in range(seqs):
        late = [after(proj, *wout_first), after(proj, *wout_far)][min(b - 1, 1)] if b else proj
        mixed_out, *kept = run_mixer_forward(b, place_arr, late, conv_own, logits, head_weight)
        saved.append(kept)
        if b == 0:
            wout_far = gather_far(wout_first)
        if b == seqs - 1:
            mixed_out = after(mixed_out, *wout_far)
        out_parts += exchange_xor(mixed_out)
    wout_parts = gather_rest(wout_first, wout_far)
    hidden, normed_two, out_rows = run_branch(
        place_arr, wout_parts, out_parts, tokens.reshape(rows, width), second_weight[None]
    )
    two_parts = gather_xor(normed_two)
    inner, up_slope, gate_slope, two_all, cot_all = run_gate(two_parts, cot_parts, wgu)

    def to_owner(partial):
        return lax.psum_scatter(partial, "fsdp", scatter_dimension=0, tiled=True)

    out_first = gather_start(after(out_rows, inner))
    inner_late = after(inner, wdown)
    gwdown = jnp.einsum("brf,brd->fd", inner_late, cot_all, preferred_element_type=WIDE).astype(LOW)
    up_slope, gwdown = lax.optimization_barrier((up_slope, gwdown, *out_first))[:2]
    gwdown = to_owner(gwdown)

    ggu, gtwo_even, gtwo_odd = run_gate_back(cot_all, up_slope, gate_slope, wdown, wgu)
    gtwo_twin = reduce_start(gtwo_odd)
    out_far = gather_far(out_first)
    ggu = after(ggu, *out_far)
    gwgu = jnp.einsum("brd,brf->df", two_all, ggu, preferred_element_type=WIDE).astype(LOW)
    gtwo_even, gwgu = lax.optimization_barrier((gtwo_even, gwgu))
    gtwo_state = reduce_far(gtwo_even, gtwo_twin)
    down_even, down_odd = run_pairs([(after(inner, gwgu), wdown, 0)], width, "down")
    gwgu = to_owner(after(gwgu, gwdown))
    gtwo_parts = reduce_last(gtwo_state)
    hidden_late = after(hidden, down_odd)

    ghidden, gsecond, gbranch, *gouts = run_branch_back(
        place_arr, wout_parts, gtwo_parts, hidden_late, cot_own, second_weight[None], seqs
    )
    gouts = [exchange_xor(g) for g in gouts]
    gwdown_first = gather_start(after(gwdown, ghidden))
    gwdown_far = gather_far(gwdown_first)
    down_twin = reduce_start(after(down_odd, ghidden))
    held, gtaps, ggain = None, [], []
    for b in range(seqs):
        gout = gouts[b]
        if b == seqs - 1:
            gout[0] = after(gout[0], *gwdown_first)
        *held, gtap, ghead = run_mixer_backward(
            b, place_arr, proj, conv_own, logits, head_weight, gout, saved[b], held
        )
        gtaps.append(gtap)
        ggain.append(ghead)
    gproj, glogit = held
    gproj = after(gproj, *gwdown_far, gwgu, down_twin)
    gproj = gproj.reshape(count, rows, 3 * wide)
    glogit = glogit.reshape(count, rows, 128)
    gwin = jnp.einsum("brd,bre->de", normed_all, gproj, preferred_element_type=WIDE).astype(LOW)
    down_state = reduce_far(down_even, down_twin)
    gbranch_cols = exchange_xor(after(gbranch, gouts[-1][-1]))
    gproj, gwin = lax.optimization_barrier((gproj, gwin, *down_state, *gbranch_cols))[:2]
    gwin = to_owner(gwin)
    gnormed_even, gnormed_odd = run_pairs([(gproj, wio, 1), (glogit, beta_own, 0)], width, "input_back")
    gnormed_twin = reduce_start(gnormed_odd)
    down = reduce_last(down_state)
    output = (hidden + sum(jnp.concatenate(e).astype(WIDE) for e in down)).astype(LOW)
    gnormed_state = reduce_far(gnormed_even, after(gnormed_twin, output))
    out_all_parts = gather_rest(out_first, out_far)
    gwout = run_outer(out_all_parts, [after(gbranch_cols[0], *gnormed_twin)] + gbranch_cols[1:], "output_weights")
    gnormed_state[0], gwout = lax.optimization_barrier((gnormed_state[0], gwout))
    gnormed = reduce_last(gnormed_state)
    gwgu_first = gather_start(after(gwgu, *gnormed_state[4:]))
    gwdown_parts = gather_rest(gwdown_first, gwdown_far)
    gnormed[0][0], gwin, *_ = lax.optimization_barrier((gnormed[0][0], gwin, *gwgu_first))
    gwout = to_owner(after(gwout, gwin))

    gnormed = sum(jnp.concatenate(e).astype(WIDE) for e in gnormed)
    input_grad = ghidden + norm_back(inputs, first_scale, gnormed, first_weight)
    gfirst = jnp.sum(gnormed * inputs * first_scale, axis=0)
    gtaps, ggain = sum(gtaps), sum(ggain)

    lanes = min(256, width)
    gwdown = run_spread(
        place_arr,
        gwdown_parts,
        (piece, lanes),
        width // lanes,
        lambda i: [(0, lanes, (slice(i * piece, (i + 1) * piece), slice(None)))],
        (hidden_part, width),
        (hidden_part, lanes),
        lambda g: (0, g),
        "spread_down",
    )
    tall = min(64, part)
    gwgu_far = gather_far([after(g, gwdown) for g in gwgu_first])
    gwgu_parts = gather_rest(gwgu_first, gwgu_far)
    gwin_first = gather_start(after(gwin, *gwgu_far))
    gwgu = run_spread(
        place_arr,
        gwgu_parts,
        (tall, 2 * ff),
        part // tall,
        lambda i: [
            (
                c * ff + f * piece,
                piece,
                (c, slice(None), slice(f * hidden_part + i * piece, f * hidden_part + (i + 1) * piece)),
            )
            for c in range(2)
            for f in range(shards)
        ],
        (2, part, hidden_part * shards),
        (2, tall, hidden_part * shards),
        lambda g: (0, g, 0),
        "spread_gate_up",
    )
    gwin_far = gather_far([after(g, gwgu) for g in gwin_first])
    gwin_parts = gather_rest(gwin_first, gwin_far)
    gwout_parts = gather_xor(after(gwout, *gwin_far))
    gwin = run_spread(
        place_arr,
        gwin_parts,
        (tall, 3 * wide),
        part // tall,
        lambda i: [
            (
                (h * 3 + c) * dim,
                dim,
                (c, slice(None), slice((i * heads + h) * dim, (i * heads + h + 1) * dim)),
            )
            for c in range(3)
            for h in range(heads)
        ],
        (3, part, width),
        (3, tall, width),
        lambda g: (0, g, 0),
        "spread_inputs",
    )
    gwout = run_spread(
        after(place_arr, gwin),
        gwout_parts,
        (tall, wide),
        part // tall,
        lambda i: [(0, wide, (slice(None), slice(i * wide, (i + 1) * wide)))],
        (part, width),
        (tall, width),
        lambda g: (g, 0),
        "spread_output",
    )

    gbeta = jnp.einsum("brh,brd->hd", glogit, normed_all, preferred_element_type=WIDE)[:heads]
    gtaps = gtaps.transpose(1, 2, 0, 3).reshape(3 * taps, wide)
    ggain = jnp.pad(jnp.sum(ggain, axis=0), ((0, 0), (0, width - dim)))
    small = sum_over("fsdp", jnp.concatenate([gsecond, ggain, gbeta]))
    gbeta = lax.dynamic_update_slice(
        jnp.zeros((all_heads, width), WIDE), small[2:], (place * heads, 0)
    )
    gtaps = lax.dynamic_update_slice(
        jnp.zeros((3 * taps, width), WIDE), sum_over("fsdp", gtaps), (0, place * wide)
    )
    small = sum_over("seq", jnp.concatenate([small[:2], gtaps, gbeta]))
    own = lax.dynamic_slice_in_dim(small, shard * part, part, 1)
    gfirst = lax.dynamic_slice_in_dim(sum_over("fsdp", sum_over("seq", gfirst[None])), shard * part, part, 1)
    ggain = lax.dynamic_slice_in_dim(small[1], shard * (dim // shards), dim // shards, 0)
    return (
        output.reshape(tokens.shape),
        input_grad.reshape(tokens.shape),
        gfirst[0],
        gwin,
        own[2 : 2 + 3 * taps].reshape(3, taps, part),
        own[2 + 3 * taps :].T,
        ggain,
        gwout,
        own[0],
        gwgu,
        gwdown,
    )


def solution(mesh):
    in_specs = (
        P("fsdp", "seq", None),
        P("fsdp", "seq", None),
        P("fsdp"),
        P(None, "fsdp", None),
        P(None, None, "fsdp"),
        P("fsdp", None),
        P("fsdp"),
        P("fsdp", None),
        P("fsdp"),
        P(None, "fsdp", None),
        P("fsdp", None),
    )
    out_specs = (
        P("fsdp", "seq", None),
        P("fsdp", "seq", None),
        P("fsdp"),
        P(None, "fsdp", None),
        P(None, None, "fsdp"),
        P("fsdp", None),
        P("fsdp"),
        P("fsdp", None),
        P("fsdp"),
        P(None, "fsdp", None),
        P("fsdp", None),
    )
    return jax.shard_map(local, mesh=mesh, in_specs=in_specs, out_specs=out_specs, check_vma=False)
```

```python
import functools

import jax
import jax.numpy as jnp
from jax import lax
from jax.experimental import pallas as pl
from jax.experimental.pallas import tpu as pltpu
from jax.sharding import PartitionSpec as P

LOW = jnp.bfloat16
WIDE = jnp.float32


def swap(x, bits):
    count = lax.axis_size("seq")
    return lax.ppermute(x, "seq", [(i, i ^ bits) for i in range(count)])


def gather_start(x, together=False):
    if lax.axis_size("seq") == 8:
        got = [swap(x, 1), swap(x, 2), swap(x, 4)]
        return [x] + list(lax.optimization_barrier(got) if together else got)
    return [x]


def gather_far(first, split=True):
    if lax.axis_size("seq") != 8:
        return []
    x, _, side, back = first
    half = x.shape[0] // 2
    if split and x.shape[0] % 32 == 0:
        return [swap(back[:half], 2), swap(side[half:], 4)]
    return [swap(back, 2)]


def gather_rest(first, far):
    count, x = lax.axis_size("seq"), first[0]
    if count == 8:
        _, twin, side, back = first
        side_twin, back_twin = swap(side, 1), swap(back, 1)
        return [[x], [twin], [side], [side_twin], [back], [back_twin], far, [swap(f, 1) for f in far]]
    held, bits = x[None], 1
    while bits < count:
        held = jnp.concatenate([held, swap(held, bits)])
        bits *= 2
    return [[held[b]] for b in range(count)]


def gather_xor(x):
    first = gather_start(x)
    return gather_rest(first, gather_far(first))


def add(first, second):
    return (first.astype(WIDE) + second.astype(WIDE)).astype(LOW)


def reduce_start(odd):
    return swap(odd, 1) if lax.axis_size("seq") == 8 else odd


def reduce_add(even, twin):
    count = lax.axis_size("seq")
    if count == 8:
        half = even.shape[1] // 2
        top, low = slice(None, half), slice(half, None)
        return [
            even,
            twin,
            add(even[1, low], twin[1, low]),
            add(even[2, top], twin[2, top]),
            add(even[1::2, top], twin[1::2, top]),
            add(even[2:, low], twin[2:, low]),
        ]
    parts = jnp.stack([even, twin], axis=1).reshape((count,) + even.shape[1:])
    bits = count // 2
    while bits:
        parts = add(parts[:bits], swap(parts[bits:], bits))
        bits //= 2
    return [parts]


def reduce_far(state):
    if len(state) == 1:
        return state
    sends = lax.optimization_barrier(state[4:])
    return state[:4] + list(lax.optimization_barrier([swap(sends[0], 2), swap(sends[1], 4)]))


def reduce_more(state):
    if len(state) == 1:
        return state
    even, twin, side, back, from_side, from_back = state
    return [even, twin, add(side, from_back[1]), add(back, from_side[1]), from_side, from_back]


def reduce_last(state):
    if len(state) == 1:
        return [state]
    even, twin, side, back, from_side, from_back = state
    side, back = lax.optimization_barrier([swap(side, 2), swap(back, 4)])
    return [[even], [twin], [from_side, side], [back, from_back]]


def total_of(parts):
    width = parts[0][0].shape[-1]
    rows = [jnp.concatenate([a[0] if a.ndim == 3 else a for a in e]) for e in parts]
    return sum(r.reshape(-1, width).astype(WIDE) for r in rows)


def exchange(parts):
    return lax.all_to_all(parts, "seq", split_axis=0, concat_axis=0, tiled=True)


def after(x, *others):
    return lax.optimization_barrier((x,) + others)[0]


def dot(a, b, left=1, right=0):
    return lax.dot_general(
        a.astype(LOW), b.astype(LOW), (((left,), (right,)), ((), ())), preferred_element_type=WIDE
    )


def iota(shape, dim):
    return lax.broadcasted_iota(jnp.int32, shape, dim)


def shifted(x, by):
    rows = x.shape[0]
    turned = pltpu.roll(x, by % rows, 0)
    row = iota(x.shape, 0)
    return jnp.where(row >= by if by > 0 else row < rows + by, turned, 0.0)


def conv_silu(x, taps):
    count = taps.shape[0]
    moved = [shifted(x, count - 1 - j) if j < count - 1 else x for j in range(count)]
    conved = sum(taps[j : j + 1] * moved[j] for j in range(count))
    gate = jax.nn.sigmoid(conved)
    return moved, conved, gate, conved * gate


def unit_scale(values):
    return lax.rsqrt(jnp.sum(values * values, axis=-1, keepdims=True) + 1e-06)


def pick_lane(block, lane):
    return jnp.sum(jnp.where(iota(block.shape, 1) == lane, block, 0.0), axis=-1, keepdims=True)


def invert_unit_lower(mats):
    size = mats[0].shape[0]
    row, col = iota((size, size), 0), iota((size, size), 1)
    invs = [jnp.where(row == col, 1.0, jnp.where(row // 2 == col // 2, -a, 0.0)) for a in mats]
    width = 2
    while width < size:
        mask = (row // (2 * width) == col // (2 * width)) & (row // width != col // width)
        part = [dot(t, jnp.where(mask, a, 0.0)) for t, a in zip(invs, mats)]
        invs = [t - dot(p, t) for t, p in zip(invs, part)]
        width *= 2
    return invs


def mixer_forward(
    place_ref, proj_ref, taps_ref, logit_ref, gain_ref, *refs
):
    out_ref, mixed_ref, state_ref, inv_ref, w_ref, fresh_ref = refs[-6:]
    place, head = place_ref[0], pl.program_id(0)
    count, _, length, _ = proj_ref.shape
    dim = mixed_ref.shape[-1]
    spot = [jnp.bitwise_xor(place, i) for i in range(count)]
    whole = jnp.concatenate([proj_ref[j, 0] for j in spot]).astype(WIDE)
    acts = [conv_silu(whole[:, c * dim : (c + 1) * dim], taps_ref[0, c])[3] for c in range(3)]
    queries = (acts[0] * (unit_scale(acts[0]) * dim ** (-0.5))).astype(LOW)
    key_rows = (acts[1] * unit_scale(acts[1])).astype(LOW)
    value_rows = acts[2].astype(LOW)

    def cut(x):
        return [x[i * length : (i + 1) * length] for i in range(count)]

    q, k, v = cut(queries), cut(key_rows), cut(value_rows)
    beta = [jax.nn.sigmoid(pick_lane(logit_ref[j, 0], head)) for j in spot]
    row, col = iota((length, length), 0), iota((length, length), 1)
    lower = [jnp.where(row > col, b * dot(x, x, 1, 1), 0.0) for b, x in zip(beta, k)]
    invs = [t.astype(LOW) for t in invert_unit_lower(lower)]
    w = [dot(t, b * x.astype(WIDE)).astype(LOW) for t, b, x in zip(invs, beta, k)]
    u = [dot(t, b * x.astype(WIDE)) for t, b, x in zip(invs, beta, v)]
    scores = [jnp.where(row >= col, dot(a, b, 1, 1), 0.0).astype(LOW) for a, b in zip(q, k)]
    turn = [dot(a, b, 0, 0).astype(LOW) for a, b in zip(k, w)]
    push = [dot(a, b, 0, 0) for a, b in zip(k, u)]
    state = jnp.zeros((dim, dim), WIDE)
    states = []
    for i in range(count):
        states.append(state.astype(LOW))
        state = state + (push[i] - dot(turn[i], states[i]))
    fresh = [(a - dot(b, c)).astype(LOW) for a, b, c in zip(u, w, states)]
    gain = gain_ref[...]
    for i in range(count):
        mixed = dot(q[i], states[i]) + dot(scores[i], fresh[i])
        scale = lax.rsqrt(jnp.mean(mixed * mixed, axis=-1, keepdims=True) + 1e-05)
        mixed_ref[0, 0, i] = mixed
        out_ref[i] = (mixed * scale * gain).astype(LOW)
        state_ref[0, 0, i] = states[i]
        inv_ref[0, 0, i] = invs[i]
        w_ref[0, 0, i] = w[i]
        fresh_ref[0, 0, i] = fresh[i]


def mixer_backward(place_ref, proj_ref, taps_ref, logit_ref, gain_ref, gout_ref, *refs):
    mixed_ref, state_ref, inv_ref, w_ref, fresh_ref = refs[:5]
    gproj_ref, glogit_ref, gtaps_ref, ggain_ref = refs[-4:]
    place, head = place_ref[0], pl.program_id(1)
    count, _, length, _ = proj_ref.shape
    dim = mixed_ref.shape[-1]
    spot = [jnp.bitwise_xor(place, i) for i in range(count)]
    whole = jnp.concatenate([proj_ref[j, 0] for j in spot]).astype(WIDE)
    convs = [conv_silu(whole[:, c * dim : (c + 1) * dim], taps_ref[0, c]) for c in range(3)]
    acts = [c[3] for c in convs]
    q_scale, k_scale = unit_scale(acts[0]), unit_scale(acts[1])
    factor = dim ** (-0.5)

    def cut(x):
        return [x[i * length : (i + 1) * length] for i in range(count)]

    q = cut((acts[0] * (q_scale * factor)).astype(LOW))
    k = cut((acts[1] * k_scale).astype(LOW))
    v = cut(acts[2].astype(LOW))
    beta = [jax.nn.sigmoid(pick_lane(logit_ref[j, 0], head)) for j in spot]
    row, col = iota((length, length), 0), iota((length, length), 1)
    gain = gain_ref[...]
    gain_sum = jnp.zeros((1, dim), WIDE)
    gm = []
    for i in range(count):
        mixed = mixed_ref[0, 0, i]
        scale = lax.rsqrt(jnp.mean(mixed * mixed, axis=-1, keepdims=True) + 1e-05)
        grad = gout_ref[i].astype(WIDE)
        gain_sum = gain_sum + jnp.sum(grad * mixed * scale, axis=0, keepdims=True)
        weighted = grad * gain
        back = scale * weighted - mixed * (
            scale * scale * scale * jnp.mean(mixed * weighted, axis=-1, keepdims=True)
        )
        gm.append(back.astype(LOW))
    ggain_ref[0, 0] = gain_sum
    inv, w, fresh, states = ([r[0, 0, i] for i in range(count)] for r in (inv_ref, w_ref, fresh_ref, state_ref))
    gram = [dot(x, x, 1, 1) for x in k]
    scores = [jnp.where(row >= col, dot(a, b, 1, 1), 0.0).astype(LOW) for a, b in zip(q, k)]
    turn = [dot(a, b, 0, 0).astype(LOW) for a, b in zip(k, w)]
    direct = [dot(a, b, 0, 0) for a, b in zip(scores, gm)]
    enter = [dot(a, b, 0, 0) - dot(c, d, 0, 0) for a, b, c, d in zip(q, gm, w, direct)]
    gstate = jnp.zeros((dim, dim), WIDE)
    late = [None] * count
    for i in reversed(range(count)):
        late[i] = gstate.astype(LOW)
        gstate = gstate + (enter[i] - dot(turn[i], late[i], 0, 0))
    gfresh = [a + dot(b, c) for a, b, c in zip(direct, k, late)]
    g = [dot(a, b, 0, 0) for a, b in zip(inv, gfresh)]
    g_low = [x.astype(LOW) for x in g]
    gs = [dot(a, b, 1, 1) for a, b in zip(g_low, states)]
    ga = [jnp.where(row > col, -dot(a, b, 1, 1), 0.0) for a, b in zip(g_low, fresh)]
    gscore = [jnp.where(row >= col, dot(a, b, 1, 1), 0.0).astype(LOW) for a, b in zip(gm, fresh)]
    gq = [dot(a, b, 1, 1) + dot(c, d) for a, b, c, d in zip(gm, states, gscore, k)]
    weighted_a = [b * a for b, a in zip(beta, ga)]
    gk = [
        dot(f, d, 1, 1) + dot(sc, qq, 0, 0) - b * s + dot(wa, kk) + dot(wa, kk, 0, 0)
        for f, d, sc, qq, b, s, wa, kk in zip(fresh, late, gscore, q, beta, gs, weighted_a, k)
    ]
    gv = [b * x for b, x in zip(beta, g)]
    lane = iota((length, glogit_ref.shape[-1]), 1)
    for i in range(count):
        gbeta = jnp.sum(
            g[i] * v[i].astype(WIDE) - gs[i] * k[i].astype(WIDE) + ga[i] * gram[i], axis=-1, keepdims=True
        )
        glogit = gbeta * beta[i] * (1.0 - beta[i])
        before = glogit_ref[spot[i], 0]
        keep = jnp.where(lane < head, before.astype(WIDE), 0.0)
        glogit_ref[spot[i], 0] = jnp.where(lane == head, glogit, keep).astype(LOW)

    def unit_back(values, scale, grad):
        return scale * grad - values * (
            scale * scale * scale * jnp.sum(values * grad, axis=-1, keepdims=True)
        )

    gacts = [
        unit_back(acts[0], q_scale, jnp.concatenate(gq) * factor),
        unit_back(acts[1], k_scale, jnp.concatenate(gk)),
        jnp.concatenate(gv),
    ]
    for c in range(3):
        moved, conved, gate, _ = convs[c]
        gconv = gacts[c] * gate * (1.0 + conved * (1.0 - gate))
        taps = taps_ref[0, c]
        gtaps_ref[0, 0, c] = jnp.concatenate([jnp.sum(gconv * m, axis=0, keepdims=True) for m in moved])
        last = len(moved) - 1
        gp = taps[last : last + 1] * gconv
        for j in range(last):
            gp = gp + taps[j : j + 1] * shifted(gconv, j - last)
        gp = gp.astype(LOW)
        for i in range(count):
            gproj_ref[spot[i], 0, :, c * dim : (c + 1) * dim] = gp[i * length : (i + 1) * length]


def mixer_specs(at, count, length, dim, lanes, taps):
    def spec(shape, place):
        return pl.BlockSpec(shape, lambda *g: place(*at(*g)))

    small = [
        spec((count, 1, length, 3 * dim), lambda b, h: (0, b, 0, h)),
        spec((1, 3, taps, dim), lambda b, h: (h, 0, 0, 0)),
        spec((count, 1, length, lanes), lambda b, h: (0, b, 0, 0)),
        spec((1, dim), lambda b, h: (0, 0)),
    ]
    saved = spec((1, 1, count, length, dim), lambda b, h: (b, h, 0, 0, 0))
    square = spec((1, 1, count, dim, dim), lambda b, h: (b, h, 0, 0, 0))
    inverse = spec((1, 1, count, length, length), lambda b, h: (b, h, 0, 0, 0))
    return small, [saved, square, inverse, saved, saved], spec


def run_mixer_forward(b, place, proj, taps, logits, gain, held):
    count, seqs, length, width = proj.shape
    heads, _, tap_count, dim = taps.shape
    small, saved, spec = mixer_specs(lambda h, p: (b, h), count, length, dim, logits.shape[-1], tap_count)
    shapes = [
        jax.ShapeDtypeStruct((count, length, heads * dim), LOW),
        jax.ShapeDtypeStruct((seqs, heads, count, length, dim), WIDE),
        jax.ShapeDtypeStruct((seqs, heads, count, dim, dim), LOW),
        jax.ShapeDtypeStruct((seqs, heads, count, length, length), LOW),
        jax.ShapeDtypeStruct((seqs, heads, count, length, dim), LOW),
        jax.ShapeDtypeStruct((seqs, heads, count, length, dim), LOW),
    ]
    held = list(held or [])
    return pl.pallas_call(
        mixer_forward,
        out_shape=shapes,
        grid_spec=pltpu.PrefetchScalarGridSpec(
            num_scalar_prefetch=1,
            grid=(heads,),
            in_specs=small + [ANY] * len(held),
            out_specs=[spec((count, length, dim), lambda b, h: (0, 0, h))] + saved,
        ),
        input_output_aliases={1 + len(small) + n: 1 + n for n in range(len(held))},
        compiler_params=pltpu.CompilerParams(vmem_limit_bytes=56 * 2**20),
        cost_estimate=cost(10),
        name="mixer_forward",
    )(place, proj, taps, logits, gain, *held)


def run_mixer_backward(place, proj, taps, logits, gain, gout, saved_values):
    count, seqs, length, width = proj.shape
    heads, _, tap_count, dim = taps.shape
    small, saved, spec = mixer_specs(lambda b, h, p: (b, h), count, length, dim, logits.shape[-1], tap_count)
    shapes = [
        jax.ShapeDtypeStruct(proj.shape, LOW),
        jax.ShapeDtypeStruct(logits.shape, LOW),
        jax.ShapeDtypeStruct((seqs, heads, 3, tap_count, dim), WIDE),
        jax.ShapeDtypeStruct((seqs, heads, 1, dim), WIDE),
    ]
    outs = [
        small[0],
        small[2],
        spec((1, 1, 3, tap_count, dim), lambda b, h: (b, h, 0, 0, 0)),
        spec((1, 1, 1, dim), lambda b, h: (b, h, 0, 0)),
    ]
    return pl.pallas_call(
        mixer_backward,
        out_shape=shapes,
        grid_spec=pltpu.PrefetchScalarGridSpec(
            num_scalar_prefetch=1,
            grid=(seqs, heads),
            in_specs=small + [spec((count, length, dim), lambda b, h: (0, b, h))] + saved,
            out_specs=outs,
        ),
        compiler_params=pltpu.CompilerParams(vmem_limit_bytes=56 * 2**20),
        cost_estimate=cost(26),
        name="mixer_backward",
    )(place, proj, taps, logits, gain, gout, *saved_values)


ANY = pl.BlockSpec(memory_space=pl.ANY)
FULL = pltpu.VMEM
PARAMS = pltpu.CompilerParams(vmem_limit_bytes=60 * 2**20)


def cost(micros):
    return pl.CostEstimate(flops=int(micros * 1.15e9), transcendentals=0, bytes_accessed=int(micros * 3.5e6))


def fetch(entries, refs, buf, sems):
    copies, n = [], 0
    for b, entry in enumerate(entries):
        row, mine = 0, []
        for size in entry:
            mine.append(pltpu.make_async_copy(refs[n], buf.at[b, pl.ds(row, size)], sems.at[n]))
            row, n = row + size, n + 1
        copies.append(mine)
    return copies


def start_all(copies):
    for mine in copies:
        for c in mine:
            c.start()


def stream(copies, outs):
    step, last = pl.program_id(0), len(copies) // 2 - 1

    @pl.when(step == 0)
    def _():
        start_all(copies)

    for i in range(last + 1):

        @pl.when(step == i)
        def _(i=i):
            for b in (2 * i, 2 * i + 1):
                for c in copies[b]:
                    c.wait()
                outs[b].start()

    def finish():
        @pl.when(step == last)
        def _():
            for out in outs:
                out.wait()

    return finish


def heights(entries):
    return [[a.shape[0] for a in entry] for entry in entries]


def flat(entries):
    return [a for entry in entries for a in entry]


def project_kernel(entries, *refs):
    n = sum(len(e) for e in entries)
    w_ref, beta_ref, proj_ref, logit_ref, all_ref, buf, sems, out_sems = refs[n:]
    count, rows, width = buf.shape
    outs = [pltpu.make_async_copy(buf.at[b], all_ref.at[b], out_sems.at[b]) for b in range(count)]
    finish = stream(fetch(entries, refs[:n], buf, sems), outs)
    x = buf[pl.ds(2 * pl.program_id(0), 2)].reshape(2 * rows, width)
    proj_ref[...] = dot(x, w_ref[...]).astype(LOW).reshape(proj_ref.shape)
    logit_ref[...] = dot(x, beta_ref[...], 1, 1).reshape(logit_ref.shape)
    finish()


def run_project(entries, w, beta, cols):
    sizes = heights(entries)
    count, rows = len(sizes), sum(sizes[0])
    pieces = flat(entries)
    width = pieces[0].shape[1]
    lanes = beta.shape[0]
    return pl.pallas_call(
        functools.partial(project_kernel, sizes),
        grid=(count // 2,),
        in_specs=[ANY] * len(pieces)
        + [
            pl.BlockSpec((width, cols), lambda g: (0, 0), pipeline_mode=pl.Buffered(1)),
            pl.BlockSpec(beta.shape, lambda g: (0, 0), pipeline_mode=pl.Buffered(1)),
        ],
        out_specs=[
            pl.BlockSpec((2, rows, cols), lambda g: (g, 0, 0)),
            pl.BlockSpec((2, rows, lanes), lambda g: (g, 0, 0)),
            ANY,
        ],
        out_shape=[
            jax.ShapeDtypeStruct((count, rows, cols), LOW),
            jax.ShapeDtypeStruct((count, rows, lanes), WIDE),
            jax.ShapeDtypeStruct((count, rows, width), LOW),
        ],
        scratch_shapes=[
            pltpu.VMEM((count, rows, width), LOW),
            pltpu.SemaphoreType.DMA((len(pieces),)),
            pltpu.SemaphoreType.DMA((count,)),
        ],
        compiler_params=PARAMS,
        cost_estimate=cost(16),
        name="project",
    )(*pieces, w, beta)


def gate_kernel(entries, others, *refs):
    n = sum(len(e) for e in entries)
    m = n + sum(len(e) for e in others)
    w_ref, inner_ref, up_ref, gate_ref, all_ref, side_ref = refs[m : m + 6]
    buf, side, sems, out_sems, side_sems, back_sems = refs[m + 6 :]
    count, rows, width = buf.shape
    outs = [pltpu.make_async_copy(buf.at[b], all_ref.at[b], out_sems.at[b]) for b in range(count)]
    backs = [pltpu.make_async_copy(side.at[b], side_ref.at[b], back_sems.at[b]) for b in range(count)]
    finish = stream(fetch(entries, refs[:n], buf, sems), outs)
    finish_side = stream(fetch(others, refs[n:m], side, side_sems), backs)
    ff = inner_ref.shape[-1]
    both = dot(buf[pl.ds(2 * pl.program_id(0), 2)].reshape(2 * rows, width), w_ref[...])
    gate, up = both[:, :ff], both[:, ff:]
    sig = jax.nn.sigmoid(gate)
    swish = gate * sig
    inner_ref[...] = (swish * up).astype(LOW).reshape(inner_ref.shape)
    gate_ref[...] = (up * sig * (1.0 + gate * (1.0 - sig))).astype(LOW).reshape(gate_ref.shape)
    up_ref[...] = swish.astype(LOW).reshape(up_ref.shape)
    finish()
    finish_side()


def run_gate(entries, others, w):
    sizes = heights(entries)
    beside = flat(others)
    count, rows = len(sizes), sum(sizes[0])
    pieces = flat(entries)
    width, ff = pieces[0].shape[1], w.shape[1] // 2
    return pl.pallas_call(
        functools.partial(gate_kernel, sizes, heights(others)),
        grid=(count // 2,),
        in_specs=[ANY] * (len(pieces) + len(beside))
        + [pl.BlockSpec(w.shape, lambda g: (0, 0), pipeline_mode=pl.Buffered(1))],
        out_specs=[pl.BlockSpec((2, rows, ff), lambda g: (g, 0, 0))] * 3 + [ANY] * 2,
        out_shape=[jax.ShapeDtypeStruct((count, rows, ff), LOW)] * 3
        + [jax.ShapeDtypeStruct((count, rows, width), LOW)] * 2,
        scratch_shapes=[
            pltpu.VMEM((count, rows, width), LOW),
            pltpu.VMEM((count, rows, width), LOW),
            pltpu.SemaphoreType.DMA((len(pieces),)),
            pltpu.SemaphoreType.DMA((count,)),
            pltpu.SemaphoreType.DMA((len(beside),)),
            pltpu.SemaphoreType.DMA((count,)),
        ],
        compiler_params=PARAMS,
        cost_estimate=cost(25),
        name="gate",
    )(*pieces, *beside, w)


def gate_back_kernel(cot_ref, up_ref, gate_ref, down_ref, w_ref, grad_ref, even_ref, odd_ref):
    _, rows, width = cot_ref.shape
    grad = dot(cot_ref[...].reshape(2 * rows, width), down_ref[...], 1, 1)
    gate, up = (r[...].reshape(2 * rows, r.shape[-1]).astype(WIDE) for r in (gate_ref, up_ref))
    both = jnp.concatenate([grad * gate, grad * up], axis=1).astype(LOW)
    grad_ref[...] = both.reshape(grad_ref.shape)
    two = dot(both, w_ref[...], 1, 1).astype(LOW)
    even_ref[0] = two[:rows]
    odd_ref[0] = two[rows:]


def run_gate_back(cot, up, gate, down, w):
    count, rows, width = cot.shape
    ff = up.shape[-1]

    def block(cols, depth=2):
        return pl.BlockSpec((depth, rows, cols), lambda b: (b, 0, 0))

    def once(x):
        return pl.BlockSpec(x.shape, lambda b: (0, 0), pipeline_mode=pl.Buffered(1))

    half = jax.ShapeDtypeStruct((count // 2, rows, width), LOW)
    return pl.pallas_call(
        gate_back_kernel,
        grid=(count // 2,),
        in_specs=[block(width), block(ff), block(ff), once(down), once(w)],
        out_specs=[block(2 * ff), block(width, 1), block(width, 1)],
        out_shape=[jax.ShapeDtypeStruct((count, rows, 2 * ff), LOW), half, half],
        compiler_params=PARAMS,
        cost_estimate=cost(32),
        name="gate_back",
    )(cot, up, gate, down, w)


def pairs_kernel(count, right, *refs):
    even_ref, odd_ref = refs[2 * count :]
    rows = even_ref.shape[1]
    total = 0.0
    for n in range(count):
        x, w = refs[n], refs[count + n]
        total = total + dot(x[...].reshape(2 * rows, x.shape[-1]), w[...], 1, right[n])
    total = total.astype(LOW)
    even_ref[0] = total[:rows]
    odd_ref[0] = total[rows:]


def run_pairs(terms, width, name, micros):
    count, rows, _ = terms[0][0].shape
    half = jax.ShapeDtypeStruct((count // 2, rows, width), LOW)
    weight_specs = []
    for x, w, right in terms:
        shape = (x.shape[-1], width) if right == 0 else (width, x.shape[-1])
        weight_specs.append(pl.BlockSpec(shape, lambda b: (0, 0), pipeline_mode=pl.Buffered(1)))
    return pl.pallas_call(
        functools.partial(pairs_kernel, len(terms), [t[2] for t in terms]),
        grid=(count // 2,),
        in_specs=[pl.BlockSpec((2, rows, t[0].shape[-1]), lambda b: (b, 0, 0)) for t in terms] + weight_specs,
        out_specs=[pl.BlockSpec((1, rows, width), lambda b: (b, 0, 0))] * 2,
        out_shape=[half, half],
        compiler_params=PARAMS,
        cost_estimate=cost(micros),
        name=name,
    )(*[t[0] for t in terms], *[t[1] for t in terms])


def branch_kernel(entries, place_ref, *refs):
    n = sum(len(e) for e in entries)
    count = len(entries)
    parts, (token_ref, gain_ref, hidden_ref, two_ref, rows_ref, buf, sems) = refs[n:-7], refs[-7:]
    copies = fetch(entries, refs[:n], buf, sems)
    start_all(copies)
    place = place_ref[0]
    wide = parts[0].shape[-1]

    def spot(b):
        return pl.ds(pl.multiple_of(jnp.bitwise_xor(place, b) * wide, wide), wide)

    for n, ref in enumerate(parts):
        length = ref.shape[1]
        for i in range(count):
            rows_ref[n * length : (n + 1) * length, i * wide : (i + 1) * wide] = ref[i]
    rows = rows_ref[...]
    for b, mine in enumerate(copies):
        for c in mine:
            c.wait()
        hidden_ref[:, spot(b)] = dot(rows, buf[b])
    hidden = hidden_ref[...] + token_ref[...].astype(WIDE)
    hidden_ref[...] = hidden
    scale = lax.rsqrt(jnp.mean(hidden * hidden, axis=-1, keepdims=True) + 1e-05)
    two_ref[...] = (hidden * scale * gain_ref[...]).astype(LOW)


def run_branch(place, entries, parts, tokens, gain):
    sizes = heights(entries)
    pieces = flat(entries)
    depth, wide = sum(sizes[0]), parts[0].shape[-1]
    vmem = pl.BlockSpec(memory_space=FULL)
    return pl.pallas_call(
        functools.partial(branch_kernel, sizes),
        in_specs=[pl.BlockSpec(memory_space=pltpu.SMEM)] + [ANY] * len(pieces) + [vmem] * (len(parts) + 2),
        out_specs=[vmem] * 3,
        out_shape=[
            jax.ShapeDtypeStruct(tokens.shape, WIDE),
            jax.ShapeDtypeStruct(tokens.shape, LOW),
            jax.ShapeDtypeStruct((tokens.shape[0], depth), LOW),
        ],
        scratch_shapes=[
            pltpu.VMEM((len(sizes), depth, wide), LOW),
            pltpu.SemaphoreType.DMA((len(pieces),)),
        ],
        compiler_params=PARAMS,
        cost_estimate=cost(10),
        name="branch",
    )(place, *pieces, *parts, tokens, gain)


def branch_back_kernel(entries, grads, place_ref, *refs):
    n = sum(len(e) for e in entries)
    m = sum(len(e) for e in grads)
    count = len(entries)
    adds, (hidden_ref, cot_ref, gain_ref) = refs[n : n + m], refs[n + m : n + m + 3]
    ghidden_ref, gsum_ref, gbranch_ref, gout_ref, buf, gout_all, sems = refs[n + m + 3 :]
    copies = fetch(entries, refs[:n], buf, sems)
    start_all(copies)
    place = place_ref[0]
    wide = gbranch_ref.shape[-1]
    total, at = 0.0, 0
    for entry in grads:
        here = [adds[at + i][...].astype(WIDE).reshape(-1, hidden_ref.shape[-1]) for i in range(len(entry))]
        at += len(entry)
        total = total + (jnp.concatenate(here) if len(here) > 1 else here[0])
    hidden = hidden_ref[...]
    scale = lax.rsqrt(jnp.mean(hidden * hidden, axis=-1, keepdims=True) + 1e-05)
    gsum_ref[...] = jnp.sum(total * hidden * scale, axis=0, keepdims=True)
    weighted = total * gain_ref[...]
    back = scale * weighted - hidden * (
        scale * scale * scale * jnp.mean(hidden * weighted, axis=-1, keepdims=True)
    )
    ghidden_ref[...] = cot_ref[...].astype(WIDE) + back

    def spot(b):
        return pl.ds(pl.multiple_of(jnp.bitwise_xor(place, b) * wide, wide), wide)

    for b, mine in enumerate(copies):
        for c in mine:
            c.wait()
        gbranch_ref[b] = ghidden_ref[:, b * wide : (b + 1) * wide].astype(LOW)
        part = dot(ghidden_ref[:, spot(b)], buf[b], 1, 1)
        if b == 0:
            gout_all[...] = part
        else:
            gout_all[...] += part
    for b in range(count):
        gout_ref[b] = gout_all[:, b * wide : (b + 1) * wide].astype(LOW)


def run_branch_back(place, entries, grads, hidden, cot, gain):
    sizes, grad_sizes = heights(entries), heights(grads)
    pieces, adds = flat(entries), flat(grads)
    count, depth, wide = len(sizes), sum(sizes[0]), pieces[0].shape[1]
    rows = hidden.shape[0]

    def first(x):
        shape = x.shape if len(x.shape) == 2 else (1,) + x.shape[1:]
        return pl.BlockSpec(shape, lambda g: (0,) * len(shape))

    def whole(shape):
        return pl.BlockSpec(shape, lambda g: (0,) * len(shape))

    return pl.pallas_call(
        functools.partial(branch_back_kernel, sizes, grad_sizes),
        grid=(1,),
        in_specs=[pl.BlockSpec(memory_space=pltpu.SMEM)]
        + [ANY] * len(pieces)
        + [first(x) for x in adds]
        + [whole(x.shape) for x in (hidden, cot, gain)],
        out_specs=[
            whole(hidden.shape),
            whole((1, hidden.shape[1])),
            whole((count, rows, wide)),
            whole((count, rows, wide)),
        ],
        out_shape=[
            jax.ShapeDtypeStruct(hidden.shape, WIDE),
            jax.ShapeDtypeStruct((1, hidden.shape[1]), WIDE),
            jax.ShapeDtypeStruct((count, rows, wide), LOW),
            jax.ShapeDtypeStruct((count, rows, wide), LOW),
        ],
        scratch_shapes=[
            pltpu.VMEM((count, depth, wide), LOW),
            pltpu.VMEM((rows, depth), WIDE),
            pltpu.SemaphoreType.DMA((len(pieces),)),
        ],
        compiler_params=PARAMS,
        cost_estimate=cost(10),
        name="branch_back",
    )(place, *pieces, *adds, hidden, cot, gain)


def outer_kernel(entries, place_ref, cols_ref, *refs):
    out_ref, total_ref = refs[-2:]
    at = 0
    for b, entry in enumerate(entries):
        cols = cols_ref[jnp.bitwise_xor(place_ref[0], b)]
        row = 0
        for size in entry:
            part = dot(refs[at][...], cols[row : row + size], 0, 0)
            total_ref[...] = part if at == 0 else total_ref[...] + part
            row, at = row + size, at + 1
    out_ref[...] = total_ref[...].astype(LOW)


def run_outer(place, entries, cols, name):
    pieces = flat(entries)
    shape = (pieces[0].shape[1], cols.shape[-1])
    vmem = pl.BlockSpec(memory_space=FULL)
    return pl.pallas_call(
        functools.partial(outer_kernel, heights(entries)),
        in_specs=[pl.BlockSpec(memory_space=pltpu.SMEM)] + [vmem] * (len(pieces) + 1),
        out_specs=vmem,
        out_shape=jax.ShapeDtypeStruct(shape, LOW),
        scratch_shapes=[pltpu.VMEM(shape, WIDE)],
        compiler_params=PARAMS,
        cost_estimate=cost(8),
        name=name,
    )(place, cols, *pieces)


def spread_kernel(entries, layout, place_ref, *refs):
    n = sum(len(e) for e in entries)
    out_ref, held = refs[n:]
    step, steps, at = pl.program_id(0), pl.num_programs(0), 0
    for b, entry in enumerate(entries):
        value = refs[at][...]
        if len(entry) > 1:
            value = jnp.where(step < steps // 2, value, refs[at + 1][...])
        held[jnp.bitwise_xor(place_ref[0], b)] = value
        at += len(entry)
    for i in range(len(entries)):
        for src, width, index in layout(i):
            out_ref[index] = held[i, :, src : src + width].astype(WIDE)


def run_spread(place, entries, piece_block, steps, layout, shape, block, index, name):
    specs = []
    for entry in entries:
        if len(entry) > 1:
            specs.append(pl.BlockSpec(piece_block, lambda g: (jnp.minimum(g, steps // 2 - 1), 0)))
            specs.append(pl.BlockSpec(piece_block, lambda g: (jnp.maximum(g - steps // 2, 0), 0)))
        elif piece_block[0] == entry[0].shape[0]:
            specs.append(pl.BlockSpec(piece_block, lambda g: (0, g)))
        else:
            specs.append(pl.BlockSpec(piece_block, lambda g: (g, 0)))
    return pl.pallas_call(
        functools.partial(spread_kernel, heights(entries), layout),
        grid=(steps,),
        in_specs=[pl.BlockSpec(memory_space=pltpu.SMEM)] + specs,
        out_specs=pl.BlockSpec(block, index),
        out_shape=jax.ShapeDtypeStruct(shape, WIDE),
        scratch_shapes=[pltpu.VMEM((len(entries),) + piece_block, LOW)],
        compiler_params=PARAMS,
        cost_estimate=cost(10),
        name=name,
    )(place, *flat(entries))


def norm_back(values, scale, grad, gain):
    weighted = grad * gain
    return scale * weighted - values * scale**3 * jnp.mean(values * weighted, axis=-1, keepdims=True)


def local(
    tokens,
    cotangent,
    gain_first,
    w_inputs,
    w_conv,
    w_beta,
    gain_heads,
    w_output,
    gain_second,
    w_gate_up,
    w_down,
):
    shards, count, place = lax.axis_size("fsdp"), lax.axis_size("seq"), lax.axis_index("seq")
    shard = lax.axis_index("fsdp")
    seqs, length, width = tokens.shape
    rows = seqs * length
    part = width // shards
    all_heads = w_beta.shape[1]
    heads = all_heads // count
    wide = heads * (w_output.shape[0] * shards // all_heads)
    dim = wide // heads
    hidden_part = w_down.shape[0]
    piece = hidden_part // count
    taps = w_conv.shape[1]
    place_arr = jnp.reshape(place, (1,)).astype(jnp.int32)

    def over_shards(x, axis=0):
        return lax.all_gather(x, "fsdp", axis=axis, tiled=True)

    packed = jnp.concatenate(
        [
            gain_first[None],
            gain_second[None],
            jnp.pad(gain_heads[None], ((0, 0), (0, part - gain_heads.shape[0]))),
            w_conv.reshape(3 * taps, part),
            w_beta.T,
        ]
    )
    packed = lax.all_gather(packed, "fsdp", axis=0)
    first_weight = packed[:, 0].reshape(width).astype(WIDE)
    second_weight = packed[:, 1].reshape(width).astype(WIDE)
    head_weight = packed[:, 2, : gain_heads.shape[0]].reshape(1, dim).astype(WIDE)
    conv_all = packed[:, 3 : 3 + 3 * taps].transpose(1, 0, 2).reshape(3, taps, width)
    conv_own = lax.dynamic_slice_in_dim(conv_all, place * wide, wide, 2).astype(WIDE)
    conv_own = conv_own.reshape(3, taps, heads, dim).transpose(2, 0, 1, 3)
    beta_all = packed[:, 3 + 3 * taps :].transpose(1, 0, 2).reshape(all_heads, width)
    beta_own = lax.dynamic_slice_in_dim(beta_all, place * heads, heads, 0)
    beta_own = jnp.pad(beta_own, ((0, 128 - heads), (0, 0)))

    ff = piece * shards
    win = lax.dynamic_slice_in_dim(w_inputs, place * wide, wide, 2)
    win = win.reshape(3, part, heads, dim).transpose(1, 2, 0, 3).reshape(part, 3 * wide)
    wio = jnp.concatenate([win, lax.dynamic_slice_in_dim(w_output, place * wide, wide, 1)], axis=1)
    later = after(place, wio)
    pieces = [
        lax.dynamic_slice(w_gate_up, (0, 0, f * hidden_part + later * piece), (2, part, piece)) for f in range(shards)
    ]
    wgu_own = jnp.concatenate([p[c] for c in range(2) for p in pieces], axis=1)
    later = after(later, wgu_own)
    wdown_own = lax.dynamic_slice_in_dim(w_down, later * piece, piece, 0)
    wio = over_shards(wio)
    wgu = over_shards(wgu_own)
    wdown = over_shards(wdown_own)

    inputs = tokens.reshape(rows, width).astype(WIDE)
    first_scale = lax.rsqrt(jnp.mean(inputs * inputs, axis=-1, keepdims=True) + 1e-05)
    normed = (inputs * first_scale * first_weight).astype(LOW)
    cot_own = cotangent.reshape(rows, width)
    cot_first = gather_start(cot_own)
    normed_first = gather_start(after(normed, wgu_own, wdown_own, *cot_first))
    normed_far = gather_far(normed_first)
    normed_parts = gather_rest(normed_first, normed_far)
    cot_far = gather_far([after(c, *normed_far) for c in cot_first])
    cot_parts = gather_rest(cot_first, cot_far)

    wio_late = after(wio, *normed_far, *cot_far)
    proj, logits, normed_all = run_project(normed_parts, wio_late, beta_own, 3 * wide)
    wout_first = gather_start(wio_late[:, 3 * wide :])
    proj = proj.reshape(count, seqs, length, 3 * wide)
    logits = logits.reshape(count, seqs, length, 128)
    wout_far, out_parts, saved = [], [], None
    for b in range(seqs):
        late = [after(proj, *wout_first), after(proj, *wout_far)][min(b - 1, 1)] if b else proj
        mixed_out, *saved = run_mixer_forward(b, place_arr, late, conv_own, logits, head_weight, saved)
        if b == 0:
            wout_far = gather_far(wout_first)
            wout_parts = gather_rest(wout_first, wout_far)
        if b == seqs - 1:
            mixed_out = after(mixed_out, *wout_far, *out_parts)
        out_parts.append(exchange(mixed_out))
    hidden, normed_two, out_rows = run_branch(
        place_arr, wout_parts, out_parts, tokens.reshape(rows, width), second_weight[None]
    )
    two_parts = gather_xor(normed_two)
    inner, up_slope, gate_slope, two_all, cot_all = run_gate(two_parts, cot_parts, wgu)

    def to_owner(partial):
        return lax.psum_scatter(partial, "fsdp", scatter_dimension=0, tiled=True)

    out_first = gather_start(after(out_rows, *two_parts[6]))
    up_slope = after(up_slope, *out_first)
    ggu, gtwo_even, gtwo_odd = run_gate_back(cot_all, up_slope, gate_slope, wdown, wgu)
    gtwo_twin = reduce_start(gtwo_odd)
    gwdown = jnp.einsum("brf,brd->fd", after(inner, ggu), cot_all, preferred_element_type=WIDE).astype(LOW)
    gtwo_even, gwdown = lax.optimization_barrier((gtwo_even, gwdown))
    gwdown = to_owner(gwdown)
    gtwo_state = reduce_add(gtwo_even, gtwo_twin)
    ggu, *gtwo_state = lax.optimization_barrier((ggu, *gtwo_state))
    gtwo_state = reduce_far(gtwo_state)
    gwgu = jnp.einsum("brd,brf->df", two_all, ggu, preferred_element_type=WIDE).astype(LOW)
    gtwo_state[0], gwgu = lax.optimization_barrier((gtwo_state[0], gwgu))
    gtwo_parts = reduce_last(reduce_more(gtwo_state))
    down_even, down_odd = run_pairs([(after(inner, gwgu), wdown, 0)], width, "down", 12)
    hidden_late = after(hidden, down_odd)
    gwgu = to_owner(gwgu)

    ghidden, gsecond, gbranch, gout = run_branch_back(
        place_arr, wout_parts, gtwo_parts, hidden_late, cot_own, second_weight[None]
    )
    down_twin = reduce_start(after(down_odd, ghidden))
    gout = exchange(gout)
    down_state = reduce_add(down_even, down_twin)
    gout, gwdown, *down_state = lax.optimization_barrier((gout, gwdown, *down_state))
    gwdown_first = gather_start(gwdown, True)
    out_far = gather_far([after(x, gout) for x in out_first])
    down_state = reduce_far(down_state)
    gproj, glogit, gtaps, ggain = run_mixer_backward(
        place_arr, proj, conv_own, logits, head_weight, gout, saved
    )
    gproj, *both = lax.optimization_barrier((gproj, *out_far, *down_state))
    out_far, down_state = both[: len(out_far)], both[len(out_far) :]
    gproj = gproj.reshape(count, rows, 3 * wide)
    glogit = glogit.reshape(count, rows, 128)
    gnormed_even, gnormed_odd = run_pairs([(gproj, wio, 1), (glogit, beta_own, 0)], width, "input_back", 1)
    gnormed_twin = reduce_start(gnormed_odd)
    gbeta = jnp.einsum(
        "brh,brd->hd", after(glogit, gnormed_even), normed_all, preferred_element_type=WIDE
    )[:heads]
    gnormed_twin, gbeta, *gwdown_first = lax.optimization_barrier((gnormed_twin, gbeta, *gwdown_first))
    gwdown_far = gather_far(gwdown_first)
    gwdown_parts = gather_rest(gwdown_first, gwdown_far)
    gnormed_state = reduce_add(gnormed_even, gnormed_twin)
    gproj, *gnormed_state = lax.optimization_barrier((gproj, *gnormed_state))
    gproj, gwgu = lax.optimization_barrier((gproj, gwgu))
    gwin = jnp.einsum("brd,bre->de", normed_all, gproj, preferred_element_type=WIDE).astype(LOW)
    gnormed_state = reduce_far(gnormed_state)
    lanes = min(256, width)
    gwdown = run_spread(
        place_arr,
        gwdown_parts,
        (piece, lanes),
        width // lanes,
        lambda i: [(0, lanes, (slice(i * piece, (i + 1) * piece), slice(None)))],
        (hidden_part, width),
        (hidden_part, lanes),
        lambda g: (0, g),
        "spread_down",
    )
    gnormed_state[0], gwin = lax.optimization_barrier((gnormed_state[0], gwin))
    gwin = to_owner(gwin)
    gnormed_state = reduce_more(gnormed_state)
    gnormed = reduce_last(gnormed_state)
    down_state[0] = after(down_state[0], *gnormed_state)
    down_state = reduce_more(down_state)
    gbranch_cols = exchange(after(gbranch, *gnormed_state[2:4]))
    gwgu_first = gather_start(after(gwgu, *gnormed_state[2:]), True)
    gnormed = total_of(gnormed)
    input_grad = ghidden + norm_back(inputs, first_scale, gnormed, first_weight)
    gfirst = jnp.sum(gnormed * inputs * first_scale, axis=0)
    down_state[0], gfirst = lax.optimization_barrier((down_state[0], gfirst))
    down = reduce_last(down_state)
    output = (hidden + total_of(down)).astype(LOW)


    out_all_parts = gather_rest(out_first, out_far)
    gwout = run_outer(place_arr, out_all_parts, gbranch_cols, "output_weights")
    gtaps = jnp.sum(gtaps, axis=0).transpose(1, 2, 0, 3).reshape(3 * taps, wide)
    ggain = jnp.sum(ggain, axis=(0, 1)).reshape(shards, 1, dim // shards)
    ggain = jnp.pad(ggain, ((0, 0), (0, 0), (0, wide - dim // shards)))
    owner = (iota((shards, 1, 1), 0) == place * wide // part).astype(WIDE)
    cells = part // wide
    gains = jnp.stack([gfirst, gsecond[0]]).reshape(2, shards, cells, wide).transpose(1, 0, 2, 3)
    gbeta = gbeta.reshape(heads, shards, cells, wide).transpose(1, 0, 2, 3)
    extra = jnp.concatenate(
        [
            gains.reshape(shards, 2 * cells, wide),
            gbeta.reshape(shards, heads * cells, wide),
            owner * gtaps[None],
            ggain,
        ],
        axis=1,
    )
    used = extra.shape[1]
    extra = jnp.pad(extra, ((0, 0), (0, -used % 32), (0, 0))).astype(LOW)
    more = extra.shape[1]
    gwout = jnp.concatenate([gwout.reshape(shards, part, wide), extra], axis=1)
    gwout = gwout.reshape(shards * (part + more), wide)
    gwgu_first[0], gwout, gwdown = lax.optimization_barrier((gwgu_first[0], gwout, gwdown))
    gwgu_far = gather_far([after(x, gwgu_first[0]) for x in gwgu_first])
    gwout = to_owner(gwout)

    gwgu_parts = gather_rest(gwgu_first, gwgu_far)
    tall = min(128, part)
    gwin_first = gather_start(after(gwin, *gwgu_far))
    gwgu = run_spread(
        place_arr,
        gwgu_parts,
        (tall, 2 * ff),
        part // tall,
        lambda i: [
            (
                c * ff + f * piece,
                piece,
                (c, slice(None), slice(f * hidden_part + i * piece, f * hidden_part + (i + 1) * piece)),
            )
            for c in range(2)
            for f in range(shards)
        ],
        (2, part, hidden_part * shards),
        (2, tall, hidden_part * shards),
        lambda g: (0, g, 0),
        "spread_gate_up",
    )
    gwin_far = gather_far([after(g, gwgu) for g in gwin_first])
    gwin_parts = gather_rest(gwin_first, gwin_far)
    gwout_first = gather_start(after(gwout, *gwin_far))
    gwout_parts = gather_rest(gwout_first, gather_far(gwout_first, False))
    gwin = run_spread(
        place_arr,
        gwin_parts,
        (tall, 3 * wide),
        part // tall,
        lambda i: [
            (
                (h * 3 + c) * dim,
                dim,
                (c, slice(None), slice((i * heads + h) * dim, (i * heads + h + 1) * dim)),
            )
            for c in range(3)
            for h in range(heads)
        ],
        (3, part, width),
        (3, tall, width),
        lambda g: (0, g, 0),
        "spread_inputs",
    )
    gwout = run_spread(
        place_arr,
        gwout_parts,
        (tall, wide),
        part // tall,
        lambda i: [(0, wide, (slice(None), slice(i * wide, (i + 1) * wide)))],
        (part, width),
        (tall, width),
        lambda g: (g, 0),
        "spread_output",
    )
    extra = jnp.stack([e[0][part:] for e in gwout_parts]).astype(WIDE)
    summed = jnp.sum(extra, axis=0)
    gains = summed[: 2 * cells].reshape(2, part)
    ggain = summed[used - 1, : dim // shards]
    gbeta, gtaps = [], []
    for i in range(count):
        rows_i = lax.dynamic_index_in_dim(extra, place ^ i, 0, False)
        gbeta.append(rows_i[2 * cells : (2 + heads) * cells].reshape(heads, part))
    for i in range(cells):
        rows_i = lax.dynamic_index_in_dim(extra, place ^ (shard * cells + i), 0, False)
        gtaps.append(rows_i[(2 + heads) * cells : used - 1])
    gbeta = jnp.concatenate(gbeta).T
    gtaps = jnp.concatenate(gtaps, axis=1).reshape(3, taps, part)
    return (
        output.reshape(tokens.shape),
        input_grad.reshape(tokens.shape),
        gains[0],
        gwin,
        gtaps,
        gbeta,
        ggain,
        gwout,
        gains[1],
        gwgu,
        gwdown,
    )


def solution(mesh):
    in_specs = (
        P("fsdp", "seq", None),
        P("fsdp", "seq", None),
        P("fsdp"),
        P(None, "fsdp", None),
        P(None, None, "fsdp"),
        P("fsdp", None),
        P("fsdp"),
        P("fsdp", None),
        P("fsdp"),
        P(None, "fsdp", None),
        P("fsdp", None),
    )
    out_specs = (
        P("fsdp", "seq", None),
        P("fsdp", "seq", None),
        P("fsdp"),
        P(None, "fsdp", None),
        P(None, None, "fsdp"),
        P("fsdp", None),
        P("fsdp"),
        P("fsdp", None),
        P("fsdp"),
        P(None, "fsdp", None),
        P("fsdp", None),
    )
    return jax.shard_map(local, mesh=mesh, in_specs=in_specs, out_specs=out_specs, check_vma=False)
```

```python
import functools

import jax
import jax.numpy as jnp
from jax import lax
from jax.experimental import pallas as pl
from jax.experimental.pallas import tpu as pltpu
from jax.sharding import PartitionSpec as P

LOW = jnp.bfloat16
WIDE = jnp.float32


def swap(x, bits):
    count = lax.axis_size("seq")
    return lax.ppermute(x, "seq", [(i, i ^ bits) for i in range(count)])


def gather_start(x, together=False):
    if lax.axis_size("seq") == 8:
        got = [swap(x, 1), swap(x, 2), swap(x, 4)]
        return [x] + list(lax.optimization_barrier(got) if together else got)
    return [x]


def gather_far(first, split=True):
    if lax.axis_size("seq") != 8:
        return []
    x, _, side, back = first
    half = x.shape[0] // 2
    if split and x.shape[0] % 32 == 0:
        return [swap(back[:half], 2), swap(side[half:], 4)]
    return [swap(back, 2)]


def gather_rest(first, far):
    count, x = lax.axis_size("seq"), first[0]
    if count == 8:
        _, twin, side, back = first
        side_twin, back_twin = swap(side, 1), swap(back, 1)
        return [[x], [twin], [side], [side_twin], [back], [back_twin], far, [swap(f, 1) for f in far]]
    held, bits = x[None], 1
    while bits < count:
        held = jnp.concatenate([held, swap(held, bits)])
        bits *= 2
    return [[held[b]] for b in range(count)]


def gather_xor(x):
    first = gather_start(x)
    return gather_rest(first, gather_far(first))


def add(first, second):
    return (first.astype(WIDE) + second.astype(WIDE)).astype(LOW)


def reduce_start(odd):
    return swap(odd, 1) if lax.axis_size("seq") == 8 else odd


def reduce_add(even, twin):
    count = lax.axis_size("seq")
    if count == 8:
        half = even.shape[1] // 2
        top, low = slice(None, half), slice(half, None)
        return [
            even,
            twin,
            add(even[1, low], twin[1, low]),
            add(even[2, top], twin[2, top]),
            add(even[1::2, top], twin[1::2, top]),
            add(even[2:, low], twin[2:, low]),
        ]
    parts = jnp.stack([even, twin], axis=1).reshape((count,) + even.shape[1:])
    bits = count // 2
    while bits:
        parts = add(parts[:bits], swap(parts[bits:], bits))
        bits //= 2
    return [parts]


def reduce_far(state):
    if len(state) == 1:
        return state
    sends = lax.optimization_barrier(state[4:])
    return state[:4] + list(lax.optimization_barrier([swap(sends[0], 2), swap(sends[1], 4)]))


def reduce_more(state):
    if len(state) == 1:
        return state
    even, twin, side, back, from_side, from_back = state
    return [even, twin, add(side, from_back[1]), add(back, from_side[1]), from_side, from_back]


def reduce_last(state):
    if len(state) == 1:
        return [state]
    even, twin, side, back, from_side, from_back = state
    side, back = lax.optimization_barrier([swap(side, 2), swap(back, 4)])
    return [[even], [twin], [from_side, side], [back, from_back]]


def total_of(parts):
    width = parts[0][0].shape[-1]
    rows = [jnp.concatenate([a[0] if a.ndim == 3 else a for a in e]) for e in parts]
    return sum(r.reshape(-1, width).astype(WIDE) for r in rows)


def exchange(parts):
    return lax.all_to_all(parts, "seq", split_axis=0, concat_axis=0, tiled=True)


def after(x, *others):
    return lax.optimization_barrier((x,) + others)[0]


def dot(a, b, left=1, right=0):
    return lax.dot_general(
        a.astype(LOW), b.astype(LOW), (((left,), (right,)), ((), ())), preferred_element_type=WIDE
    )


def iota(shape, dim):
    return lax.broadcasted_iota(jnp.int32, shape, dim)


def shifted(x, by):
    rows = x.shape[0]
    turned = pltpu.roll(x, by % rows, 0)
    row = iota(x.shape, 0)
    return jnp.where(row >= by if by > 0 else row < rows + by, turned, 0.0)


def conv_silu(x, taps):
    count = taps.shape[0]
    moved = [shifted(x, count - 1 - j) if j < count - 1 else x for j in range(count)]
    conved = sum(taps[j : j + 1] * moved[j] for j in range(count))
    gate = jax.nn.sigmoid(conved)
    return moved, conved, gate, conved * gate


def unit_scale(values):
    return lax.rsqrt(jnp.sum(values * values, axis=-1, keepdims=True) + 1e-06)


def pick_lane(block, lane):
    return jnp.sum(jnp.where(iota(block.shape, 1) == lane, block, 0.0), axis=-1, keepdims=True)


def invert_unit_lower(mats):
    size = mats[0].shape[0]
    row, col = iota((size, size), 0), iota((size, size), 1)
    invs = [jnp.where(row == col, 1.0, jnp.where(row // 2 == col // 2, -a, 0.0)) for a in mats]
    width = 2
    while width < size:
        mask = (row // (2 * width) == col // (2 * width)) & (row // width != col // width)
        part = [dot(t, jnp.where(mask, a, 0.0)) for t, a in zip(invs, mats)]
        invs = [t - dot(p, t) for t, p in zip(invs, part)]
        width *= 2
    return invs


def mixer_forward(
    place_ref, proj_ref, taps_ref, logit_ref, gain_ref, *refs
):
    out_ref, mixed_ref, state_ref, inv_ref, w_ref, fresh_ref = refs[-6:]
    place, head = place_ref[0], pl.program_id(0)
    count, _, length, _ = proj_ref.shape
    dim = mixed_ref.shape[-1]
    spot = [jnp.bitwise_xor(place, i) for i in range(count)]
    whole = jnp.concatenate([proj_ref[j, 0] for j in spot]).astype(WIDE)
    acts = [conv_silu(whole[:, c * dim : (c + 1) * dim], taps_ref[0, c])[3] for c in range(3)]
    queries = (acts[0] * (unit_scale(acts[0]) * dim ** (-0.5))).astype(LOW)
    key_rows = (acts[1] * unit_scale(acts[1])).astype(LOW)
    value_rows = acts[2].astype(LOW)

    def cut(x):
        return [x[i * length : (i + 1) * length] for i in range(count)]

    q, k, v = cut(queries), cut(key_rows), cut(value_rows)
    beta = [jax.nn.sigmoid(pick_lane(logit_ref[j, 0], head)) for j in spot]
    row, col = iota((length, length), 0), iota((length, length), 1)
    lower = [jnp.where(row > col, b * dot(x, x, 1, 1), 0.0) for b, x in zip(beta, k)]
    invs = [t.astype(LOW) for t in invert_unit_lower(lower)]
    w = [dot(t, b * x.astype(WIDE)).astype(LOW) for t, b, x in zip(invs, beta, k)]
    u = [dot(t, b * x.astype(WIDE)) for t, b, x in zip(invs, beta, v)]
    scores = [jnp.where(row >= col, dot(a, b, 1, 1), 0.0).astype(LOW) for a, b in zip(q, k)]
    turn = [dot(a, b, 0, 0).astype(LOW) for a, b in zip(k, w)]
    push = [dot(a, b, 0, 0) for a, b in zip(k, u)]
    state = jnp.zeros((dim, dim), WIDE)
    states = []
    for i in range(count):
        states.append(state.astype(LOW))
        state = state + (push[i] - dot(turn[i], states[i]))
    fresh = [(a - dot(b, c)).astype(LOW) for a, b, c in zip(u, w, states)]
    gain = gain_ref[...]
    for i in range(count):
        mixed = dot(q[i], states[i]) + dot(scores[i], fresh[i])
        scale = lax.rsqrt(jnp.mean(mixed * mixed, axis=-1, keepdims=True) + 1e-05)
        mixed_ref[0, 0, i] = mixed
        out_ref[i] = (mixed * scale * gain).astype(LOW)
        state_ref[0, 0, i] = states[i]
        inv_ref[0, 0, i] = invs[i]
        w_ref[0, 0, i] = w[i]
        fresh_ref[0, 0, i] = fresh[i]


def mixer_backward(place_ref, proj_ref, taps_ref, logit_ref, gain_ref, gout_ref, *refs):
    mixed_ref, state_ref, inv_ref, w_ref, fresh_ref = refs[:5]
    gproj_ref, glogit_ref, gtaps_ref, ggain_ref = refs[-4:]
    place, head = place_ref[0], pl.program_id(1)
    count, _, length, _ = proj_ref.shape
    dim = mixed_ref.shape[-1]
    spot = [jnp.bitwise_xor(place, i) for i in range(count)]
    whole = jnp.concatenate([proj_ref[j, 0] for j in spot]).astype(WIDE)
    convs = [conv_silu(whole[:, c * dim : (c + 1) * dim], taps_ref[0, c]) for c in range(3)]
    acts = [c[3] for c in convs]
    q_scale, k_scale = unit_scale(acts[0]), unit_scale(acts[1])
    factor = dim ** (-0.5)

    def cut(x):
        return [x[i * length : (i + 1) * length] for i in range(count)]

    q = cut((acts[0] * (q_scale * factor)).astype(LOW))
    k = cut((acts[1] * k_scale).astype(LOW))
    v = cut(acts[2].astype(LOW))
    beta = [jax.nn.sigmoid(pick_lane(logit_ref[j, 0], head)) for j in spot]
    row, col = iota((length, length), 0), iota((length, length), 1)
    gain = gain_ref[...]
    gain_sum = jnp.zeros((1, dim), WIDE)
    gm = []
    for i in range(count):
        mixed = mixed_ref[0, 0, i]
        scale = lax.rsqrt(jnp.mean(mixed * mixed, axis=-1, keepdims=True) + 1e-05)
        grad = gout_ref[i].astype(WIDE)
        gain_sum = gain_sum + jnp.sum(grad * mixed * scale, axis=0, keepdims=True)
        weighted = grad * gain
        back = scale * weighted - mixed * (
            scale * scale * scale * jnp.mean(mixed * weighted, axis=-1, keepdims=True)
        )
        gm.append(back.astype(LOW))
    ggain_ref[0, 0] = gain_sum
    inv, w, fresh, states = ([r[0, 0, i] for i in range(count)] for r in (inv_ref, w_ref, fresh_ref, state_ref))
    gram = [dot(x, x, 1, 1) for x in k]
    scores = [jnp.where(row >= col, dot(a, b, 1, 1), 0.0).astype(LOW) for a, b in zip(q, k)]
    turn = [dot(a, b, 0, 0).astype(LOW) for a, b in zip(k, w)]
    direct = [dot(a, b, 0, 0) for a, b in zip(scores, gm)]
    enter = [dot(a, b, 0, 0) - dot(c, d, 0, 0) for a, b, c, d in zip(q, gm, w, direct)]
    gstate = jnp.zeros((dim, dim), WIDE)
    late = [None] * count
    for i in reversed(range(count)):
        late[i] = gstate.astype(LOW)
        gstate = gstate + (enter[i] - dot(turn[i], late[i], 0, 0))
    gfresh = [a + dot(b, c) for a, b, c in zip(direct, k, late)]
    g = [dot(a, b, 0, 0) for a, b in zip(inv, gfresh)]
    g_low = [x.astype(LOW) for x in g]
    gs = [dot(a, b, 1, 1) for a, b in zip(g_low, states)]
    ga = [jnp.where(row > col, -dot(a, b, 1, 1), 0.0) for a, b in zip(g_low, fresh)]
    gscore = [jnp.where(row >= col, dot(a, b, 1, 1), 0.0).astype(LOW) for a, b in zip(gm, fresh)]
    gq = [dot(a, b, 1, 1) + dot(c, d) for a, b, c, d in zip(gm, states, gscore, k)]
    weighted_a = [b * a for b, a in zip(beta, ga)]
    gk = [
        dot(f, d, 1, 1) + dot(sc, qq, 0, 0) - b * s + dot(wa, kk) + dot(wa, kk, 0, 0)
        for f, d, sc, qq, b, s, wa, kk in zip(fresh, late, gscore, q, beta, gs, weighted_a, k)
    ]
    gv = [b * x for b, x in zip(beta, g)]
    lane = iota((length, glogit_ref.shape[-1]), 1)
    for i in range(count):
        gbeta = jnp.sum(
            g[i] * v[i].astype(WIDE) - gs[i] * k[i].astype(WIDE) + ga[i] * gram[i], axis=-1, keepdims=True
        )
        glogit = gbeta * beta[i] * (1.0 - beta[i])
        before = glogit_ref[spot[i], 0]
        keep = jnp.where(lane < head, before.astype(WIDE), 0.0)
        glogit_ref[spot[i], 0] = jnp.where(lane == head, glogit, keep).astype(LOW)

    def unit_back(values, scale, grad):
        return scale * grad - values * (
            scale * scale * scale * jnp.sum(values * grad, axis=-1, keepdims=True)
        )

    gacts = [
        unit_back(acts[0], q_scale, jnp.concatenate(gq) * factor),
        unit_back(acts[1], k_scale, jnp.concatenate(gk)),
        jnp.concatenate(gv),
    ]
    for c in range(3):
        moved, conved, gate, _ = convs[c]
        gconv = gacts[c] * gate * (1.0 + conved * (1.0 - gate))
        taps = taps_ref[0, c]
        gtaps_ref[0, 0, c] = jnp.concatenate([jnp.sum(gconv * m, axis=0, keepdims=True) for m in moved])
        last = len(moved) - 1
        gp = taps[last : last + 1] * gconv
        for j in range(last):
            gp = gp + taps[j : j + 1] * shifted(gconv, j - last)
        gp = gp.astype(LOW)
        for i in range(count):
            gproj_ref[spot[i], 0, :, c * dim : (c + 1) * dim] = gp[i * length : (i + 1) * length]


def mixer_specs(at, count, length, dim, lanes, taps):
    def spec(shape, place):
        return pl.BlockSpec(shape, lambda *g: place(*at(*g)))

    small = [
        spec((count, 1, length, 3 * dim), lambda b, h: (0, b, 0, h)),
        spec((1, 3, taps, dim), lambda b, h: (h, 0, 0, 0)),
        spec((count, 1, length, lanes), lambda b, h: (0, b, 0, 0)),
        spec((1, dim), lambda b, h: (0, 0)),
    ]
    saved = spec((1, 1, count, length, dim), lambda b, h: (b, h, 0, 0, 0))
    square = spec((1, 1, count, dim, dim), lambda b, h: (b, h, 0, 0, 0))
    inverse = spec((1, 1, count, length, length), lambda b, h: (b, h, 0, 0, 0))
    return small, [saved, square, inverse, saved, saved], spec


def run_mixer_forward(b, place, proj, taps, logits, gain, held):
    count, seqs, length, width = proj.shape
    heads, _, tap_count, dim = taps.shape
    small, saved, spec = mixer_specs(lambda h, p: (b, h), count, length, dim, logits.shape[-1], tap_count)
    shapes = [
        jax.ShapeDtypeStruct((count, length, heads * dim), LOW),
        jax.ShapeDtypeStruct((seqs, heads, count, length, dim), WIDE),
        jax.ShapeDtypeStruct((seqs, heads, count, dim, dim), LOW),
        jax.ShapeDtypeStruct((seqs, heads, count, length, length), LOW),
        jax.ShapeDtypeStruct((seqs, heads, count, length, dim), LOW),
        jax.ShapeDtypeStruct((seqs, heads, count, length, dim), LOW),
    ]
    held = list(held or [])
    return pl.pallas_call(
        mixer_forward,
        out_shape=shapes,
        grid_spec=pltpu.PrefetchScalarGridSpec(
            num_scalar_prefetch=1,
            grid=(heads,),
            in_specs=small + [ANY] * len(held),
            out_specs=[spec((count, length, dim), lambda b, h: (0, 0, h))] + saved,
        ),
        input_output_aliases={1 + len(small) + n: 1 + n for n in range(len(held))},
        compiler_params=pltpu.CompilerParams(vmem_limit_bytes=56 * 2**20),
        cost_estimate=cost(10),
        name="mixer_forward",
    )(place, proj, taps, logits, gain, *held)


def run_mixer_backward(place, proj, taps, logits, gain, gout, saved_values):
    count, seqs, length, width = proj.shape
    heads, _, tap_count, dim = taps.shape
    small, saved, spec = mixer_specs(lambda b, h, p: (b, h), count, length, dim, logits.shape[-1], tap_count)
    shapes = [
        jax.ShapeDtypeStruct(proj.shape, LOW),
        jax.ShapeDtypeStruct(logits.shape, LOW),
        jax.ShapeDtypeStruct((seqs, heads, 3, tap_count, dim), WIDE),
        jax.ShapeDtypeStruct((seqs, heads, 1, dim), WIDE),
    ]
    outs = [
        small[0],
        small[2],
        spec((1, 1, 3, tap_count, dim), lambda b, h: (b, h, 0, 0, 0)),
        spec((1, 1, 1, dim), lambda b, h: (b, h, 0, 0)),
    ]
    return pl.pallas_call(
        mixer_backward,
        out_shape=shapes,
        grid_spec=pltpu.PrefetchScalarGridSpec(
            num_scalar_prefetch=1,
            grid=(seqs, heads),
            in_specs=small + [spec((count, length, dim), lambda b, h: (0, b, h))] + saved,
            out_specs=outs,
        ),
        compiler_params=pltpu.CompilerParams(vmem_limit_bytes=56 * 2**20),
        cost_estimate=cost(26),
        name="mixer_backward",
    )(place, proj, taps, logits, gain, gout, *saved_values)


ANY = pl.BlockSpec(memory_space=pl.ANY)
FULL = pltpu.VMEM
PARAMS = pltpu.CompilerParams(vmem_limit_bytes=60 * 2**20)


def cost(micros):
    return pl.CostEstimate(flops=int(micros * 1.15e9), transcendentals=0, bytes_accessed=int(micros * 3.5e6))


def fetch(entries, refs, buf, sems):
    copies, n = [], 0
    for b, entry in enumerate(entries):
        row, mine = 0, []
        for size in entry:
            mine.append(pltpu.make_async_copy(refs[n], buf.at[b, pl.ds(row, size)], sems.at[n]))
            row, n = row + size, n + 1
        copies.append(mine)
    return copies


def start_all(copies):
    for mine in copies:
        for c in mine:
            c.start()


def stream(copies, outs):
    step, last = pl.program_id(0), len(copies) // 2 - 1

    @pl.when(step == 0)
    def _():
        start_all(copies)

    for i in range(last + 1):

        @pl.when(step == i)
        def _(i=i):
            for b in (2 * i, 2 * i + 1):
                for c in copies[b]:
                    c.wait()
                outs[b].start()

    def finish():
        @pl.when(step == last)
        def _():
            for out in outs:
                out.wait()

    return finish


def heights(entries):
    return [[a.shape[0] for a in entry] for entry in entries]


def flat(entries):
    return [a for entry in entries for a in entry]


def project_kernel(entries, *refs):
    n = sum(len(e) for e in entries)
    w_ref, beta_ref, proj_ref, logit_ref, all_ref, buf, sems, out_sems = refs[n:]
    count, rows, width = buf.shape
    outs = [pltpu.make_async_copy(buf.at[b], all_ref.at[b], out_sems.at[b]) for b in range(count)]
    finish = stream(fetch(entries, refs[:n], buf, sems), outs)
    x = buf[pl.ds(2 * pl.program_id(0), 2)].reshape(2 * rows, width)
    proj_ref[...] = dot(x, w_ref[...]).astype(LOW).reshape(proj_ref.shape)
    logit_ref[...] = dot(x, beta_ref[...], 1, 1).reshape(logit_ref.shape)
    finish()


def run_project(entries, w, beta, cols):
    sizes = heights(entries)
    count, rows = len(sizes), sum(sizes[0])
    pieces = flat(entries)
    width = pieces[0].shape[1]
    lanes = beta.shape[0]
    return pl.pallas_call(
        functools.partial(project_kernel, sizes),
        grid=(count // 2,),
        in_specs=[ANY] * len(pieces)
        + [
            pl.BlockSpec((width, cols), lambda g: (0, 0), pipeline_mode=pl.Buffered(1)),
            pl.BlockSpec(beta.shape, lambda g: (0, 0), pipeline_mode=pl.Buffered(1)),
        ],
        out_specs=[
            pl.BlockSpec((2, rows, cols), lambda g: (g, 0, 0)),
            pl.BlockSpec((2, rows, lanes), lambda g: (g, 0, 0)),
            ANY,
        ],
        out_shape=[
            jax.ShapeDtypeStruct((count, rows, cols), LOW),
            jax.ShapeDtypeStruct((count, rows, lanes), WIDE),
            jax.ShapeDtypeStruct((count, rows, width), LOW),
        ],
        scratch_shapes=[
            pltpu.VMEM((count, rows, width), LOW),
            pltpu.SemaphoreType.DMA((len(pieces),)),
            pltpu.SemaphoreType.DMA((count,)),
        ],
        compiler_params=PARAMS,
        cost_estimate=cost(16),
        name="project",
    )(*pieces, w, beta)


def gate_kernel(entries, others, *refs):
    n = sum(len(e) for e in entries)
    m = n + sum(len(e) for e in others)
    w_ref, inner_ref, up_ref, gate_ref, all_ref, side_ref = refs[m : m + 6]
    buf, side, sems, out_sems, side_sems, back_sems = refs[m + 6 :]
    count, rows, width = buf.shape
    outs = [pltpu.make_async_copy(buf.at[b], all_ref.at[b], out_sems.at[b]) for b in range(count)]
    backs = [pltpu.make_async_copy(side.at[b], side_ref.at[b], back_sems.at[b]) for b in range(count)]
    finish = stream(fetch(entries, refs[:n], buf, sems), outs)
    finish_side = stream(fetch(others, refs[n:m], side, side_sems), backs)
    ff = inner_ref.shape[-1]
    both = dot(buf[pl.ds(2 * pl.program_id(0), 2)].reshape(2 * rows, width), w_ref[...])
    gate, up = both[:, :ff], both[:, ff:]
    sig = jax.nn.sigmoid(gate)
    swish = gate * sig
    inner_ref[...] = (swish * up).astype(LOW).reshape(inner_ref.shape)
    gate_ref[...] = (up * sig * (1.0 + gate * (1.0 - sig))).astype(LOW).reshape(gate_ref.shape)
    up_ref[...] = swish.astype(LOW).reshape(up_ref.shape)
    finish()
    finish_side()


def run_gate(entries, others, w):
    sizes = heights(entries)
    beside = flat(others)
    count, rows = len(sizes), sum(sizes[0])
    pieces = flat(entries)
    width, ff = pieces[0].shape[1], w.shape[1] // 2
    return pl.pallas_call(
        functools.partial(gate_kernel, sizes, heights(others)),
        grid=(count // 2,),
        in_specs=[ANY] * (len(pieces) + len(beside))
        + [pl.BlockSpec(w.shape, lambda g: (0, 0), pipeline_mode=pl.Buffered(1))],
        out_specs=[pl.BlockSpec((2, rows, ff), lambda g: (g, 0, 0))] * 3 + [ANY] * 2,
        out_shape=[jax.ShapeDtypeStruct((count, rows, ff), LOW)] * 3
        + [jax.ShapeDtypeStruct((count, rows, width), LOW)] * 2,
        scratch_shapes=[
            pltpu.VMEM((count, rows, width), LOW),
            pltpu.VMEM((count, rows, width), LOW),
            pltpu.SemaphoreType.DMA((len(pieces),)),
            pltpu.SemaphoreType.DMA((count,)),
            pltpu.SemaphoreType.DMA((len(beside),)),
            pltpu.SemaphoreType.DMA((count,)),
        ],
        compiler_params=PARAMS,
        cost_estimate=cost(25),
        name="gate",
    )(*pieces, *beside, w)


def gate_back_kernel(cot_ref, up_ref, gate_ref, down_ref, w_ref, grad_ref, even_ref, odd_ref):
    _, rows, width = cot_ref.shape
    grad = dot(cot_ref[...].reshape(2 * rows, width), down_ref[...], 1, 1)
    gate, up = (r[...].reshape(2 * rows, r.shape[-1]).astype(WIDE) for r in (gate_ref, up_ref))
    both = jnp.concatenate([grad * gate, grad * up], axis=1).astype(LOW)
    grad_ref[...] = both.reshape(grad_ref.shape)
    two = dot(both, w_ref[...], 1, 1).astype(LOW)
    even_ref[0] = two[:rows]
    odd_ref[0] = two[rows:]


def run_gate_back(cot, up, gate, down, w):
    count, rows, width = cot.shape
    ff = up.shape[-1]

    def block(cols, depth=2):
        return pl.BlockSpec((depth, rows, cols), lambda b: (b, 0, 0))

    def once(x):
        return pl.BlockSpec(x.shape, lambda b: (0, 0), pipeline_mode=pl.Buffered(1))

    half = jax.ShapeDtypeStruct((count // 2, rows, width), LOW)
    return pl.pallas_call(
        gate_back_kernel,
        grid=(count // 2,),
        in_specs=[block(width), block(ff), block(ff), once(down), once(w)],
        out_specs=[block(2 * ff), block(width, 1), block(width, 1)],
        out_shape=[jax.ShapeDtypeStruct((count, rows, 2 * ff), LOW), half, half],
        compiler_params=PARAMS,
        cost_estimate=cost(32),
        name="gate_back",
    )(cot, up, gate, down, w)


def pairs_kernel(count, right, *refs):
    even_ref, odd_ref = refs[2 * count :]
    rows = even_ref.shape[1]
    total = 0.0
    for n in range(count):
        x, w = refs[n], refs[count + n]
        total = total + dot(x[...].reshape(2 * rows, x.shape[-1]), w[...], 1, right[n])
    total = total.astype(LOW)
    even_ref[0] = total[:rows]
    odd_ref[0] = total[rows:]


def run_pairs(terms, width, name, micros):
    count, rows, _ = terms[0][0].shape
    half = jax.ShapeDtypeStruct((count // 2, rows, width), LOW)
    weight_specs = []
    for x, w, right in terms:
        shape = (x.shape[-1], width) if right == 0 else (width, x.shape[-1])
        weight_specs.append(pl.BlockSpec(shape, lambda b: (0, 0), pipeline_mode=pl.Buffered(1)))
    return pl.pallas_call(
        functools.partial(pairs_kernel, len(terms), [t[2] for t in terms]),
        grid=(count // 2,),
        in_specs=[pl.BlockSpec((2, rows, t[0].shape[-1]), lambda b: (b, 0, 0)) for t in terms] + weight_specs,
        out_specs=[pl.BlockSpec((1, rows, width), lambda b: (b, 0, 0))] * 2,
        out_shape=[half, half],
        compiler_params=PARAMS,
        cost_estimate=cost(micros),
        name=name,
    )(*[t[0] for t in terms], *[t[1] for t in terms])


def branch_kernel(entries, place_ref, *refs):
    n = sum(len(e) for e in entries)
    count = len(entries)
    parts, (token_ref, gain_ref, hidden_ref, two_ref, rows_ref, buf, sems) = refs[n:-7], refs[-7:]
    copies = fetch(entries, refs[:n], buf, sems)
    start_all(copies)
    place = place_ref[0]
    wide = parts[0].shape[-1]

    def spot(b):
        return pl.ds(pl.multiple_of(jnp.bitwise_xor(place, b) * wide, wide), wide)

    for n, ref in enumerate(parts):
        length = ref.shape[1]
        for i in range(count):
            rows_ref[n * length : (n + 1) * length, i * wide : (i + 1) * wide] = ref[i]
    rows = rows_ref[...]
    for b, mine in enumerate(copies):
        for c in mine:
            c.wait()
        hidden_ref[:, spot(b)] = dot(rows, buf[b])
    hidden = hidden_ref[...] + token_ref[...].astype(WIDE)
    hidden_ref[...] = hidden
    scale = lax.rsqrt(jnp.mean(hidden * hidden, axis=-1, keepdims=True) + 1e-05)
    two_ref[...] = (hidden * scale * gain_ref[...]).astype(LOW)


def run_branch(place, entries, parts, tokens, gain):
    sizes = heights(entries)
    pieces = flat(entries)
    depth, wide = sum(sizes[0]), parts[0].shape[-1]
    vmem = pl.BlockSpec(memory_space=FULL)
    return pl.pallas_call(
        functools.partial(branch_kernel, sizes),
        in_specs=[pl.BlockSpec(memory_space=pltpu.SMEM)] + [ANY] * len(pieces) + [vmem] * (len(parts) + 2),
        out_specs=[vmem] * 3,
        out_shape=[
            jax.ShapeDtypeStruct(tokens.shape, WIDE),
            jax.ShapeDtypeStruct(tokens.shape, LOW),
            jax.ShapeDtypeStruct((tokens.shape[0], depth), LOW),
        ],
        scratch_shapes=[
            pltpu.VMEM((len(sizes), depth, wide), LOW),
            pltpu.SemaphoreType.DMA((len(pieces),)),
        ],
        compiler_params=PARAMS,
        cost_estimate=cost(10),
        name="branch",
    )(place, *pieces, *parts, tokens, gain)


def branch_back_kernel(entries, grads, place_ref, *refs):
    n = sum(len(e) for e in entries)
    m = sum(len(e) for e in grads)
    count = len(entries)
    adds, (hidden_ref, cot_ref, gain_ref) = refs[n : n + m], refs[n + m : n + m + 3]
    ghidden_ref, gsum_ref, gbranch_ref, gout_ref, buf, gout_all, sems = refs[n + m + 3 :]
    copies = fetch(entries, refs[:n], buf, sems)
    start_all(copies)
    place = place_ref[0]
    wide = gbranch_ref.shape[-1]
    total, at = 0.0, 0
    for entry in grads:
        here = [adds[at + i][...].astype(WIDE).reshape(-1, hidden_ref.shape[-1]) for i in range(len(entry))]
        at += len(entry)
        total = total + (jnp.concatenate(here) if len(here) > 1 else here[0])
    hidden = hidden_ref[...]
    scale = lax.rsqrt(jnp.mean(hidden * hidden, axis=-1, keepdims=True) + 1e-05)
    gsum_ref[...] = jnp.sum(total * hidden * scale, axis=0, keepdims=True)
    weighted = total * gain_ref[...]
    back = scale * weighted - hidden * (
        scale * scale * scale * jnp.mean(hidden * weighted, axis=-1, keepdims=True)
    )
    ghidden_ref[...] = cot_ref[...].astype(WIDE) + back

    def spot(b):
        return pl.ds(pl.multiple_of(jnp.bitwise_xor(place, b) * wide, wide), wide)

    for b, mine in enumerate(copies):
        for c in mine:
            c.wait()
        gbranch_ref[b] = ghidden_ref[:, b * wide : (b + 1) * wide].astype(LOW)
        part = dot(ghidden_ref[:, spot(b)], buf[b], 1, 1)
        if b == 0:
            gout_all[...] = part
        else:
            gout_all[...] += part
    for b in range(count):
        gout_ref[b] = gout_all[:, b * wide : (b + 1) * wide].astype(LOW)


def run_branch_back(place, entries, grads, hidden, cot, gain):
    sizes, grad_sizes = heights(entries), heights(grads)
    pieces, adds = flat(entries), flat(grads)
    count, depth, wide = len(sizes), sum(sizes[0]), pieces[0].shape[1]
    rows = hidden.shape[0]

    def first(x):
        shape = x.shape if len(x.shape) == 2 else (1,) + x.shape[1:]
        return pl.BlockSpec(shape, lambda g: (0,) * len(shape))

    def whole(shape):
        return pl.BlockSpec(shape, lambda g: (0,) * len(shape))

    return pl.pallas_call(
        functools.partial(branch_back_kernel, sizes, grad_sizes),
        grid=(1,),
        in_specs=[pl.BlockSpec(memory_space=pltpu.SMEM)]
        + [ANY] * len(pieces)
        + [first(x) for x in adds]
        + [whole(x.shape) for x in (hidden, cot, gain)],
        out_specs=[
            whole(hidden.shape),
            whole((1, hidden.shape[1])),
            whole((count, rows, wide)),
            whole((count, rows, wide)),
        ],
        out_shape=[
            jax.ShapeDtypeStruct(hidden.shape, WIDE),
            jax.ShapeDtypeStruct((1, hidden.shape[1]), WIDE),
            jax.ShapeDtypeStruct((count, rows, wide), LOW),
            jax.ShapeDtypeStruct((count, rows, wide), LOW),
        ],
        scratch_shapes=[
            pltpu.VMEM((count, depth, wide), LOW),
            pltpu.VMEM((rows, depth), WIDE),
            pltpu.SemaphoreType.DMA((len(pieces),)),
        ],
        compiler_params=PARAMS,
        cost_estimate=cost(10),
        name="branch_back",
    )(place, *pieces, *adds, hidden, cot, gain)


def outer_kernel(entries, place_ref, cols_ref, *refs):
    out_ref, total_ref = refs[-2:]
    at = 0
    for b, entry in enumerate(entries):
        cols = cols_ref[jnp.bitwise_xor(place_ref[0], b)]
        row = 0
        for size in entry:
            part = dot(refs[at][...], cols[row : row + size], 0, 0)
            total_ref[...] = part if at == 0 else total_ref[...] + part
            row, at = row + size, at + 1
    out_ref[...] = total_ref[...].astype(LOW)


def run_outer(place, entries, cols, name):
    pieces = flat(entries)
    shape = (pieces[0].shape[1], cols.shape[-1])
    vmem = pl.BlockSpec(memory_space=FULL)
    return pl.pallas_call(
        functools.partial(outer_kernel, heights(entries)),
        in_specs=[pl.BlockSpec(memory_space=pltpu.SMEM)] + [vmem] * (len(pieces) + 1),
        out_specs=vmem,
        out_shape=jax.ShapeDtypeStruct(shape, LOW),
        scratch_shapes=[pltpu.VMEM(shape, WIDE)],
        compiler_params=PARAMS,
        cost_estimate=cost(8),
        name=name,
    )(place, cols, *pieces)


def spread_kernel(entries, layout, place_ref, *refs):
    n = sum(len(e) for e in entries)
    out_ref, held = refs[n:]
    step, steps, at = pl.program_id(0), pl.num_programs(0), 0
    for b, entry in enumerate(entries):
        value = refs[at][...]
        if len(entry) > 1:
            value = jnp.where(step < steps // 2, value, refs[at + 1][...])
        held[jnp.bitwise_xor(place_ref[0], b)] = value
        at += len(entry)
    for i in range(len(entries)):
        for src, width, index in layout(i):
            out_ref[index] = held[i, :, src : src + width].astype(WIDE)


def run_spread(place, entries, piece_block, steps, layout, shape, block, index, name):
    specs = []
    for entry in entries:
        if len(entry) > 1:
            specs.append(pl.BlockSpec(piece_block, lambda g: (jnp.minimum(g, steps // 2 - 1), 0)))
            specs.append(pl.BlockSpec(piece_block, lambda g: (jnp.maximum(g - steps // 2, 0), 0)))
        elif piece_block[0] == entry[0].shape[0]:
            specs.append(pl.BlockSpec(piece_block, lambda g: (0, g)))
        else:
            specs.append(pl.BlockSpec(piece_block, lambda g: (g, 0)))
    return pl.pallas_call(
        functools.partial(spread_kernel, heights(entries), layout),
        grid=(steps,),
        in_specs=[pl.BlockSpec(memory_space=pltpu.SMEM)] + specs,
        out_specs=pl.BlockSpec(block, index),
        out_shape=jax.ShapeDtypeStruct(shape, WIDE),
        scratch_shapes=[pltpu.VMEM((len(entries),) + piece_block, LOW)],
        compiler_params=PARAMS,
        cost_estimate=cost(10),
        name=name,
    )(place, *flat(entries))


def norm_back(values, scale, grad, gain):
    weighted = grad * gain
    return scale * weighted - values * scale**3 * jnp.mean(values * weighted, axis=-1, keepdims=True)


def local(
    tokens,
    cotangent,
    gain_first,
    w_inputs,
    w_conv,
    w_beta,
    gain_heads,
    w_output,
    gain_second,
    w_gate_up,
    w_down,
):
    shards, count, place = lax.axis_size("fsdp"), lax.axis_size("seq"), lax.axis_index("seq")
    shard = lax.axis_index("fsdp")
    seqs, length, width = tokens.shape
    rows = seqs * length
    part = width // shards
    all_heads = w_beta.shape[1]
    heads = all_heads // count
    wide = heads * (w_output.shape[0] * shards // all_heads)
    dim = wide // heads
    hidden_part = w_down.shape[0]
    piece = hidden_part // count
    taps = w_conv.shape[1]
    place_arr = jnp.reshape(place, (1,)).astype(jnp.int32)

    def over_shards(x, axis=0):
        return lax.all_gather(x, "fsdp", axis=axis, tiled=True)

    packed = jnp.concatenate(
        [
            gain_first[None],
            gain_second[None],
            jnp.pad(gain_heads[None], ((0, 0), (0, part - gain_heads.shape[0]))),
            w_conv.reshape(3 * taps, part),
            w_beta.T,
        ]
    )
    packed = lax.all_gather(packed, "fsdp", axis=0)
    first_weight = packed[:, 0].reshape(width).astype(WIDE)
    second_weight = packed[:, 1].reshape(width).astype(WIDE)
    head_weight = packed[:, 2, : gain_heads.shape[0]].reshape(1, dim).astype(WIDE)
    conv_all = packed[:, 3 : 3 + 3 * taps].transpose(1, 0, 2).reshape(3, taps, width)
    conv_own = lax.dynamic_slice_in_dim(conv_all, place * wide, wide, 2).astype(WIDE)
    conv_own = conv_own.reshape(3, taps, heads, dim).transpose(2, 0, 1, 3)
    beta_all = packed[:, 3 + 3 * taps :].transpose(1, 0, 2).reshape(all_heads, width)
    beta_own = lax.dynamic_slice_in_dim(beta_all, place * heads, heads, 0)
    beta_own = jnp.pad(beta_own, ((0, 128 - heads), (0, 0)))

    ff = piece * shards
    win = lax.dynamic_slice_in_dim(w_inputs, place * wide, wide, 2)
    win = win.reshape(3, part, heads, dim).transpose(1, 2, 0, 3).reshape(part, 3 * wide)
    wio = jnp.concatenate([win, lax.dynamic_slice_in_dim(w_output, place * wide, wide, 1)], axis=1)
    later = after(place, wio)
    pieces = [
        lax.dynamic_slice(w_gate_up, (0, 0, f * hidden_part + later * piece), (2, part, piece)) for f in range(shards)
    ]
    wgu_own = jnp.concatenate([p[c] for c in range(2) for p in pieces], axis=1)
    later = after(later, wgu_own)
    wdown_own = lax.dynamic_slice_in_dim(w_down, later * piece, piece, 0)
    wio = over_shards(wio)
    wgu = over_shards(wgu_own)
    wdown = over_shards(wdown_own)

    inputs = tokens.reshape(rows, width).astype(WIDE)
    first_scale = lax.rsqrt(jnp.mean(inputs * inputs, axis=-1, keepdims=True) + 1e-05)
    normed = (inputs * first_scale * first_weight).astype(LOW)
    cot_own = cotangent.reshape(rows, width)
    cot_first = gather_start(cot_own)
    normed_first = gather_start(after(normed, wgu_own, wdown_own, *cot_first))
    normed_far = gather_far(normed_first)
    normed_parts = gather_rest(normed_first, normed_far)
    cot_far = gather_far([after(c, *normed_far) for c in cot_first])
    cot_parts = gather_rest(cot_first, cot_far)

    wio_late = after(wio, *normed_far, *cot_far)
    proj, logits, normed_all = run_project(normed_parts, wio_late, beta_own, 3 * wide)
    wout_first = gather_start(wio_late[:, 3 * wide :])
    proj = proj.reshape(count, seqs, length, 3 * wide)
    logits = logits.reshape(count, seqs, length, 128)
    wout_far, out_parts, saved = [], [], None
    for b in range(seqs):
        late = [after(proj, *wout_first), after(proj, *wout_far)][min(b - 1, 1)] if b else proj
        mixed_out, *saved = run_mixer_forward(b, place_arr, late, conv_own, logits, head_weight, saved)
        if b == 0:
            wout_far = gather_far(wout_first)
            wout_parts = gather_rest(wout_first, wout_far)
        if b == seqs - 1:
            mixed_out = after(mixed_out, *wout_far, *out_parts)
        out_parts.append(exchange(mixed_out))
    hidden, normed_two, out_rows = run_branch(
        place_arr, wout_parts, out_parts, tokens.reshape(rows, width), second_weight[None]
    )
    two_parts = gather_xor(normed_two)
    inner, up_slope, gate_slope, two_all, cot_all = run_gate(two_parts, cot_parts, wgu)

    def to_owner(partial):
        return lax.psum_scatter(partial, "fsdp", scatter_dimension=0, tiled=True)

    out_first = gather_start(after(out_rows, *two_parts[6]))
    up_slope = after(up_slope, *out_first)
    ggu, gtwo_even, gtwo_odd = run_gate_back(cot_all, up_slope, gate_slope, wdown, wgu)
    gtwo_twin = reduce_start(gtwo_odd)
    gwdown = jnp.einsum("brf,brd->fd", after(inner, ggu), cot_all, preferred_element_type=WIDE).astype(LOW)
    gtwo_even, gwdown = lax.optimization_barrier((gtwo_even, gwdown))
    gwdown = to_owner(gwdown)
    gtwo_state = reduce_add(gtwo_even, gtwo_twin)
    ggu, *gtwo_state = lax.optimization_barrier((ggu, *gtwo_state))
    gtwo_state = reduce_far(gtwo_state)
    gwgu = jnp.einsum("brd,brf->df", two_all, ggu, preferred_element_type=WIDE).astype(LOW)
    gtwo_state[0], gwgu = lax.optimization_barrier((gtwo_state[0], gwgu))
    gtwo_parts = reduce_last(reduce_more(gtwo_state))
    down_even, down_odd = run_pairs([(after(inner, gwgu), wdown, 0)], width, "down", 12)
    hidden_late = after(hidden, down_odd)
    gwgu = to_owner(gwgu)

    ghidden, gsecond, gbranch, gout = run_branch_back(
        place_arr, wout_parts, gtwo_parts, hidden_late, cot_own, second_weight[None]
    )
    down_twin = reduce_start(after(down_odd, ghidden))
    gout = exchange(gout)
    down_state = reduce_add(down_even, down_twin)
    gout, gwdown, *down_state = lax.optimization_barrier((gout, gwdown, *down_state))
    gwdown_first = gather_start(gwdown, True)
    out_far = gather_far([after(x, gout) for x in out_first])
    down_state = reduce_far(down_state)
    gproj, glogit, gtaps, ggain = run_mixer_backward(
        place_arr, proj, conv_own, logits, head_weight, gout, saved
    )
    gbranch_cols = exchange(after(gbranch, gproj))
    gproj, *both = lax.optimization_barrier((gproj, *out_far, *down_state))
    out_far, down_state = both[: len(out_far)], both[len(out_far) :]
    gproj = gproj.reshape(count, rows, 3 * wide)
    glogit = glogit.reshape(count, rows, 128)
    gnormed_even, gnormed_odd = run_pairs([(gproj, wio, 1), (glogit, beta_own, 0)], width, "input_back", 1)
    gnormed_twin = reduce_start(gnormed_odd)
    gbeta = jnp.einsum(
        "brh,brd->hd", after(glogit, gnormed_even), normed_all, preferred_element_type=WIDE
    )[:heads]
    gnormed_twin, gbeta, gbranch_cols, *gwdown_first = lax.optimization_barrier(
        (gnormed_twin, gbeta, gbranch_cols, *gwdown_first)
    )
    gnormed_state = reduce_add(gnormed_even, gnormed_twin)
    gproj, gnormed_odd = lax.optimization_barrier((gproj, gnormed_odd))
    gwin = jnp.einsum("brd,bre->de", normed_all, gproj, preferred_element_type=WIDE).astype(LOW)
    gnormed_state = reduce_far(gnormed_state)
    gwin = to_owner(gwin)
    gnormed_state = reduce_more(gnormed_state)
    gnormed = reduce_last(gnormed_state)
    down_state[0] = after(down_state[0], *gnormed_state)
    down_state = reduce_more(down_state)
    gwgu_first = gather_start(after(gwgu, *[e[-1] for e in gnormed]), True)
    gnormed = total_of(gnormed)
    input_grad = ghidden + norm_back(inputs, first_scale, gnormed, first_weight)
    gfirst = jnp.sum(gnormed * inputs * first_scale, axis=0)


    out_all_parts = gather_rest(out_first, out_far)
    gwout = run_outer(place_arr, out_all_parts, after(gbranch_cols, *gnormed_state), "output_weights")
    gtaps = jnp.sum(gtaps, axis=0).transpose(1, 2, 0, 3).reshape(3 * taps, wide)
    ggain = jnp.sum(ggain, axis=(0, 1)).reshape(shards, 1, dim // shards)
    ggain = jnp.pad(ggain, ((0, 0), (0, 0), (0, wide - dim // shards)))
    owner = (iota((shards, 1, 1), 0) == place * wide // part).astype(WIDE)
    cells = part // wide
    gains = jnp.stack([gfirst, gsecond[0]]).reshape(2, shards, cells, wide).transpose(1, 0, 2, 3)
    gbeta = gbeta.reshape(heads, shards, cells, wide).transpose(1, 0, 2, 3)
    extra = jnp.concatenate(
        [
            gains.reshape(shards, 2 * cells, wide),
            gbeta.reshape(shards, heads * cells, wide),
            owner * gtaps[None],
            ggain,
        ],
        axis=1,
    )
    used = extra.shape[1]
    extra = jnp.pad(extra, ((0, 0), (0, -used % 32), (0, 0))).astype(LOW)
    more = extra.shape[1]
    gwout = jnp.concatenate([gwout.reshape(shards, part, wide), extra], axis=1)
    gwout = gwout.reshape(shards * (part + more), wide)
    gwgu_first, gwout = lax.optimization_barrier((gwgu_first, gwout))
    gwgu_far = gather_far(gwgu_first)
    gwout = to_owner(gwout)

    gwgu_parts = gather_rest(gwgu_first, gwgu_far)
    tall = min(128, part)
    gwin_first = gather_start(after(gwin, *gwgu_first))
    gwgu = run_spread(
        place_arr,
        gwgu_parts,
        (tall, 2 * ff),
        part // tall,
        lambda i: [
            (
                c * ff + f * piece,
                piece,
                (c, slice(None), slice(f * hidden_part + i * piece, f * hidden_part + (i + 1) * piece)),
            )
            for c in range(2)
            for f in range(shards)
        ],
        (2, part, hidden_part * shards),
        (2, tall, hidden_part * shards),
        lambda g: (0, g, 0),
        "spread_gate_up",
    )
    gwin_far = gather_far([after(g, gwgu) for g in gwin_first])
    down_state, gwdown_first, gwin_far = lax.optimization_barrier((down_state, gwdown_first, gwin_far))
    gwdown_far = gather_far(gwdown_first)
    down = reduce_last(down_state)
    output = (hidden + total_of(down)).astype(LOW)
    gwdown_parts = gather_rest(gwdown_first, gwdown_far)
    lanes = min(256, width)
    gwdown = run_spread(
        place_arr,
        gwdown_parts,
        (piece, lanes),
        width // lanes,
        lambda i: [(0, lanes, (slice(i * piece, (i + 1) * piece), slice(None)))],
        (hidden_part, width),
        (hidden_part, lanes),
        lambda g: (0, g),
        "spread_down",
    )
    gwin_parts = gather_rest(gwin_first, gwin_far)
    gwout_first = gather_start(after(gwout, *gwin_first))
    gwout_parts = gather_rest(gwout_first, gather_far(gwout_first, False))
    gwin = run_spread(
        place_arr,
        gwin_parts,
        (tall, 3 * wide),
        part // tall,
        lambda i: [
            (
                (h * 3 + c) * dim,
                dim,
                (c, slice(None), slice((i * heads + h) * dim, (i * heads + h + 1) * dim)),
            )
            for c in range(3)
            for h in range(heads)
        ],
        (3, part, width),
        (3, tall, width),
        lambda g: (0, g, 0),
        "spread_inputs",
    )
    gwout = run_spread(
        place_arr,
        gwout_parts,
        (tall, wide),
        part // tall,
        lambda i: [(0, wide, (slice(None), slice(i * wide, (i + 1) * wide)))],
        (part, width),
        (tall, width),
        lambda g: (g, 0),
        "spread_output",
    )
    extra = jnp.stack([e[0][part:] for e in gwout_parts]).astype(WIDE)
    summed = jnp.sum(extra, axis=0)
    gains = summed[: 2 * cells].reshape(2, part)
    ggain = summed[used - 1, : dim // shards]
    gbeta, gtaps = [], []
    for i in range(count):
        rows_i = lax.dynamic_index_in_dim(extra, place ^ i, 0, False)
        gbeta.append(rows_i[2 * cells : (2 + heads) * cells].reshape(heads, part))
    for i in range(cells):
        rows_i = lax.dynamic_index_in_dim(extra, place ^ (shard * cells + i), 0, False)
        gtaps.append(rows_i[(2 + heads) * cells : used - 1])
    gbeta = jnp.concatenate(gbeta).T
    gtaps = jnp.concatenate(gtaps, axis=1).reshape(3, taps, part)
    return (
        output.reshape(tokens.shape),
        input_grad.reshape(tokens.shape),
        gains[0],
        gwin,
        gtaps,
        gbeta,
        ggain,
        gwout,
        gains[1],
        gwgu,
        gwdown,
    )


def solution(mesh):
    in_specs = (
        P("fsdp", "seq", None),
        P("fsdp", "seq", None),
        P("fsdp"),
        P(None, "fsdp", None),
        P(None, None, "fsdp"),
        P("fsdp", None),
        P("fsdp"),
        P("fsdp", None),
        P("fsdp"),
        P(None, "fsdp", None),
        P("fsdp", None),
    )
    out_specs = (
        P("fsdp", "seq", None),
        P("fsdp", "seq", None),
        P("fsdp"),
        P(None, "fsdp", None),
        P(None, None, "fsdp"),
        P("fsdp", None),
        P("fsdp"),
        P("fsdp", None),
        P("fsdp"),
        P(None, "fsdp", None),
        P("fsdp", None),
    )
    return jax.shard_map(local, mesh=mesh, in_specs=in_specs, out_specs=out_specs, check_vma=False)
```

```python
import functools

import jax
import jax.numpy as jnp
from jax import lax
from jax.experimental import pallas as pl
from jax.experimental.pallas import tpu as pltpu
from jax.sharding import PartitionSpec as P

LOW = jnp.bfloat16
WIDE = jnp.float32


def swap(x, bits):
    count = lax.axis_size("seq")
    return lax.ppermute(x, "seq", [(i, i ^ bits) for i in range(count)])


def gather_start(x, together=False):
    if lax.axis_size("seq") == 8:
        got = [swap(x, 1), swap(x, 2), swap(x, 4)]
        return [x] + list(lax.optimization_barrier(got) if together else got)
    return [x]


def gather_far(first, split=True):
    if lax.axis_size("seq") != 8:
        return []
    x, _, side, back = first
    half = x.shape[0] // 2
    if split and x.shape[0] % 32 == 0:
        return [swap(back[:half], 2), swap(side[half:], 4)]
    return [swap(back, 2)]


def gather_rest(first, far):
    count, x = lax.axis_size("seq"), first[0]
    if count == 8:
        _, twin, side, back = first
        side_twin, back_twin = swap(side, 1), swap(back, 1)
        return [[x], [twin], [side], [side_twin], [back], [back_twin], far, [swap(f, 1) for f in far]]
    held, bits = x[None], 1
    while bits < count:
        held = jnp.concatenate([held, swap(held, bits)])
        bits *= 2
    return [[held[b]] for b in range(count)]


def gather_xor(x):
    first = gather_start(x)
    return gather_rest(first, gather_far(first))


def add(first, second):
    return (first.astype(WIDE) + second.astype(WIDE)).astype(LOW)


def reduce_start(odd):
    return swap(odd, 1) if lax.axis_size("seq") == 8 else odd


def reduce_add(even, twin):
    count = lax.axis_size("seq")
    if count == 8:
        half = even.shape[1] // 2
        top, low = slice(None, half), slice(half, None)
        return [
            even,
            twin,
            add(even[1, low], twin[1, low]),
            add(even[2, top], twin[2, top]),
            add(even[1::2, top], twin[1::2, top]),
            add(even[2:, low], twin[2:, low]),
        ]
    parts = jnp.stack([even, twin], axis=1).reshape((count,) + even.shape[1:])
    bits = count // 2
    while bits:
        parts = add(parts[:bits], swap(parts[bits:], bits))
        bits //= 2
    return [parts]


def reduce_far(state):
    if len(state) == 1:
        return state
    sends = lax.optimization_barrier(state[4:])
    return state[:4] + list(lax.optimization_barrier([swap(sends[0], 2), swap(sends[1], 4)]))


def reduce_more(state):
    if len(state) == 1:
        return state
    even, twin, side, back, from_side, from_back = state
    return [even, twin, add(side, from_back[1]), add(back, from_side[1]), from_side, from_back]


def reduce_last(state):
    if len(state) == 1:
        return [state]
    even, twin, side, back, from_side, from_back = state
    side, back = lax.optimization_barrier([swap(side, 2), swap(back, 4)])
    return [[even], [twin], [from_side, side], [back, from_back]]


def total_of(parts):
    width = parts[0][0].shape[-1]
    rows = [jnp.concatenate([a[0] if a.ndim == 3 else a for a in e]) for e in parts]
    return sum(r.reshape(-1, width).astype(WIDE) for r in rows)


def exchange(parts):
    return lax.all_to_all(parts, "seq", split_axis=0, concat_axis=0, tiled=True)


def after(x, *others):
    return lax.optimization_barrier((x,) + others)[0]


def dot(a, b, left=1, right=0):
    return lax.dot_general(
        a.astype(LOW), b.astype(LOW), (((left,), (right,)), ((), ())), preferred_element_type=WIDE
    )


def iota(shape, dim):
    return lax.broadcasted_iota(jnp.int32, shape, dim)


def shifted(x, by):
    rows = x.shape[0]
    turned = pltpu.roll(x, by % rows, 0)
    row = iota(x.shape, 0)
    return jnp.where(row >= by if by > 0 else row < rows + by, turned, 0.0)


def conv_silu(x, taps):
    count = taps.shape[0]
    moved = [shifted(x, count - 1 - j) if j < count - 1 else x for j in range(count)]
    conved = sum(taps[j : j + 1] * moved[j] for j in range(count))
    gate = jax.nn.sigmoid(conved)
    return moved, conved, gate, conved * gate


def unit_scale(values):
    return lax.rsqrt(jnp.sum(values * values, axis=-1, keepdims=True) + 1e-06)


def pick_lane(block, lane):
    return jnp.sum(jnp.where(iota(block.shape, 1) == lane, block, 0.0), axis=-1, keepdims=True)


def invert_unit_lower(mats):
    size = mats[0].shape[0]
    row, col = iota((size, size), 0), iota((size, size), 1)
    invs = [jnp.where(row == col, 1.0, jnp.where(row // 2 == col // 2, -a, 0.0)) for a in mats]
    width = 2
    while width < size:
        mask = (row // (2 * width) == col // (2 * width)) & (row // width != col // width)
        part = [dot(t, jnp.where(mask, a, 0.0)) for t, a in zip(invs, mats)]
        invs = [t - dot(p, t) for t, p in zip(invs, part)]
        width *= 2
    return invs


def mixer_forward(
    place_ref, proj_ref, taps_ref, logit_ref, gain_ref, *refs
):
    out_ref, mixed_ref, state_ref, inv_ref, w_ref, fresh_ref = refs[-6:]
    place, head = place_ref[0], pl.program_id(0)
    count, _, length, _ = proj_ref.shape
    dim = mixed_ref.shape[-1]
    spot = [jnp.bitwise_xor(place, i) for i in range(count)]
    whole = jnp.concatenate([proj_ref[j, 0] for j in spot]).astype(WIDE)
    acts = [conv_silu(whole[:, c * dim : (c + 1) * dim], taps_ref[0, c])[3] for c in range(3)]
    queries = (acts[0] * (unit_scale(acts[0]) * dim ** (-0.5))).astype(LOW)
    key_rows = (acts[1] * unit_scale(acts[1])).astype(LOW)
    value_rows = acts[2].astype(LOW)

    def cut(x):
        return [x[i * length : (i + 1) * length] for i in range(count)]

    q, k, v = cut(queries), cut(key_rows), cut(value_rows)
    beta = [jax.nn.sigmoid(pick_lane(logit_ref[j, 0], head)) for j in spot]
    row, col = iota((length, length), 0), iota((length, length), 1)
    lower = [jnp.where(row > col, b * dot(x, x, 1, 1), 0.0) for b, x in zip(beta, k)]
    invs = [t.astype(LOW) for t in invert_unit_lower(lower)]
    w = [dot(t, b * x.astype(WIDE)).astype(LOW) for t, b, x in zip(invs, beta, k)]
    u = [dot(t, b * x.astype(WIDE)) for t, b, x in zip(invs, beta, v)]
    scores = [jnp.where(row >= col, dot(a, b, 1, 1), 0.0).astype(LOW) for a, b in zip(q, k)]
    turn = [dot(a, b, 0, 0).astype(LOW) for a, b in zip(k, w)]
    push = [dot(a, b, 0, 0) for a, b in zip(k, u)]
    state = jnp.zeros((dim, dim), WIDE)
    states = []
    for i in range(count):
        states.append(state.astype(LOW))
        state = state + (push[i] - dot(turn[i], states[i]))
    fresh = [(a - dot(b, c)).astype(LOW) for a, b, c in zip(u, w, states)]
    gain = gain_ref[...]
    for i in range(count):
        mixed = dot(q[i], states[i]) + dot(scores[i], fresh[i])
        scale = lax.rsqrt(jnp.mean(mixed * mixed, axis=-1, keepdims=True) + 1e-05)
        mixed_ref[0, 0, i] = mixed
        out_ref[i] = (mixed * scale * gain).astype(LOW)
        state_ref[0, 0, i] = states[i]
        inv_ref[0, 0, i] = invs[i]
        w_ref[0, 0, i] = w[i]
        fresh_ref[0, 0, i] = fresh[i]


def mixer_backward(place_ref, proj_ref, taps_ref, logit_ref, gain_ref, gout_ref, *refs):
    mixed_ref, state_ref, inv_ref, w_ref, fresh_ref = refs[:5]
    gproj_ref, glogit_ref, gtaps_ref, ggain_ref = refs[-4:]
    place, head = place_ref[0], pl.program_id(1)
    count, _, length, _ = proj_ref.shape
    dim = mixed_ref.shape[-1]
    spot = [jnp.bitwise_xor(place, i) for i in range(count)]
    whole = jnp.concatenate([proj_ref[j, 0] for j in spot]).astype(WIDE)
    convs = [conv_silu(whole[:, c * dim : (c + 1) * dim], taps_ref[0, c]) for c in range(3)]
    acts = [c[3] for c in convs]
    q_scale, k_scale = unit_scale(acts[0]), unit_scale(acts[1])
    factor = dim ** (-0.5)

    def cut(x):
        return [x[i * length : (i + 1) * length] for i in range(count)]

    q = cut((acts[0] * (q_scale * factor)).astype(LOW))
    k = cut((acts[1] * k_scale).astype(LOW))
    v = cut(acts[2].astype(LOW))
    beta = [jax.nn.sigmoid(pick_lane(logit_ref[j, 0], head)) for j in spot]
    row, col = iota((length, length), 0), iota((length, length), 1)
    gain = gain_ref[...]
    gain_sum = jnp.zeros((1, dim), WIDE)
    gm = []
    for i in range(count):
        mixed = mixed_ref[0, 0, i]
        scale = lax.rsqrt(jnp.mean(mixed * mixed, axis=-1, keepdims=True) + 1e-05)
        grad = gout_ref[i].astype(WIDE)
        gain_sum = gain_sum + jnp.sum(grad * mixed * scale, axis=0, keepdims=True)
        weighted = grad * gain
        back = scale * weighted - mixed * (
            scale * scale * scale * jnp.mean(mixed * weighted, axis=-1, keepdims=True)
        )
        gm.append(back.astype(LOW))
    ggain_ref[0, 0] = gain_sum
    inv, w, fresh, states = ([r[0, 0, i] for i in range(count)] for r in (inv_ref, w_ref, fresh_ref, state_ref))
    gram = [dot(x, x, 1, 1) for x in k]
    scores = [jnp.where(row >= col, dot(a, b, 1, 1), 0.0).astype(LOW) for a, b in zip(q, k)]
    turn = [dot(a, b, 0, 0).astype(LOW) for a, b in zip(k, w)]
    direct = [dot(a, b, 0, 0) for a, b in zip(scores, gm)]
    enter = [dot(a, b, 0, 0) - dot(c, d, 0, 0) for a, b, c, d in zip(q, gm, w, direct)]
    gstate = jnp.zeros((dim, dim), WIDE)
    late = [None] * count
    for i in reversed(range(count)):
        late[i] = gstate.astype(LOW)
        gstate = gstate + (enter[i] - dot(turn[i], late[i], 0, 0))
    gfresh = [a + dot(b, c) for a, b, c in zip(direct, k, late)]
    g = [dot(a, b, 0, 0) for a, b in zip(inv, gfresh)]
    g_low = [x.astype(LOW) for x in g]
    gs = [dot(a, b, 1, 1) for a, b in zip(g_low, states)]
    ga = [jnp.where(row > col, -dot(a, b, 1, 1), 0.0) for a, b in zip(g_low, fresh)]
    gscore = [jnp.where(row >= col, dot(a, b, 1, 1), 0.0).astype(LOW) for a, b in zip(gm, fresh)]
    gq = [dot(a, b, 1, 1) + dot(c, d) for a, b, c, d in zip(gm, states, gscore, k)]
    weighted_a = [b * a for b, a in zip(beta, ga)]
    gk = [
        dot(f, d, 1, 1) + dot(sc, qq, 0, 0) - b * s + dot(wa, kk) + dot(wa, kk, 0, 0)
        for f, d, sc, qq, b, s, wa, kk in zip(fresh, late, gscore, q, beta, gs, weighted_a, k)
    ]
    gv = [b * x for b, x in zip(beta, g)]
    lane = iota((length, glogit_ref.shape[-1]), 1)
    for i in range(count):
        gbeta = jnp.sum(
            g[i] * v[i].astype(WIDE) - gs[i] * k[i].astype(WIDE) + ga[i] * gram[i], axis=-1, keepdims=True
        )
        glogit = gbeta * beta[i] * (1.0 - beta[i])
        before = glogit_ref[spot[i], 0]
        keep = jnp.where(lane < head, before.astype(WIDE), 0.0)
        glogit_ref[spot[i], 0] = jnp.where(lane == head, glogit, keep).astype(LOW)

    def unit_back(values, scale, grad):
        return scale * grad - values * (
            scale * scale * scale * jnp.sum(values * grad, axis=-1, keepdims=True)
        )

    gacts = [
        unit_back(acts[0], q_scale, jnp.concatenate(gq) * factor),
        unit_back(acts[1], k_scale, jnp.concatenate(gk)),
        jnp.concatenate(gv),
    ]
    for c in range(3):
        moved, conved, gate, _ = convs[c]
        gconv = gacts[c] * gate * (1.0 + conved * (1.0 - gate))
        taps = taps_ref[0, c]
        gtaps_ref[0, 0, c] = jnp.concatenate([jnp.sum(gconv * m, axis=0, keepdims=True) for m in moved])
        last = len(moved) - 1
        gp = taps[last : last + 1] * gconv
        for j in range(last):
            gp = gp + taps[j : j + 1] * shifted(gconv, j - last)
        gp = gp.astype(LOW)
        for i in range(count):
            gproj_ref[spot[i], 0, :, c * dim : (c + 1) * dim] = gp[i * length : (i + 1) * length]


def mixer_specs(at, count, length, dim, lanes, taps):
    def spec(shape, place):
        return pl.BlockSpec(shape, lambda *g: place(*at(*g)))

    small = [
        spec((count, 1, length, 3 * dim), lambda b, h: (0, b, 0, h)),
        spec((1, 3, taps, dim), lambda b, h: (h, 0, 0, 0)),
        spec((count, 1, length, lanes), lambda b, h: (0, b, 0, 0)),
        spec((1, dim), lambda b, h: (0, 0)),
    ]
    saved = spec((1, 1, count, length, dim), lambda b, h: (b, h, 0, 0, 0))
    square = spec((1, 1, count, dim, dim), lambda b, h: (b, h, 0, 0, 0))
    inverse = spec((1, 1, count, length, length), lambda b, h: (b, h, 0, 0, 0))
    return small, [saved, square, inverse, saved, saved], spec


def run_mixer_forward(b, place, proj, taps, logits, gain, held):
    count, seqs, length, width = proj.shape
    heads, _, tap_count, dim = taps.shape
    small, saved, spec = mixer_specs(lambda h, p: (b, h), count, length, dim, logits.shape[-1], tap_count)
    shapes = [
        jax.ShapeDtypeStruct((count, length, heads * dim), LOW),
        jax.ShapeDtypeStruct((seqs, heads, count, length, dim), WIDE),
        jax.ShapeDtypeStruct((seqs, heads, count, dim, dim), LOW),
        jax.ShapeDtypeStruct((seqs, heads, count, length, length), LOW),
        jax.ShapeDtypeStruct((seqs, heads, count, length, dim), LOW),
        jax.ShapeDtypeStruct((seqs, heads, count, length, dim), LOW),
    ]
    held = list(held or [])
    return pl.pallas_call(
        mixer_forward,
        out_shape=shapes,
        grid_spec=pltpu.PrefetchScalarGridSpec(
            num_scalar_prefetch=1,
            grid=(heads,),
            in_specs=small + [ANY] * len(held),
            out_specs=[spec((count, length, dim), lambda b, h: (0, 0, h))] + saved,
        ),
        input_output_aliases={1 + len(small) + n: 1 + n for n in range(len(held))},
        compiler_params=pltpu.CompilerParams(vmem_limit_bytes=56 * 2**20),
        cost_estimate=cost(10),
        name="mixer_forward",
    )(place, proj, taps, logits, gain, *held)


def run_mixer_backward(place, proj, taps, logits, gain, gout, saved_values):
    count, seqs, length, width = proj.shape
    heads, _, tap_count, dim = taps.shape
    small, saved, spec = mixer_specs(lambda b, h, p: (b, h), count, length, dim, logits.shape[-1], tap_count)
    shapes = [
        jax.ShapeDtypeStruct(proj.shape, LOW),
        jax.ShapeDtypeStruct(logits.shape, LOW),
        jax.ShapeDtypeStruct((seqs, heads, 3, tap_count, dim), WIDE),
        jax.ShapeDtypeStruct((seqs, heads, 1, dim), WIDE),
    ]
    outs = [
        small[0],
        small[2],
        spec((1, 1, 3, tap_count, dim), lambda b, h: (b, h, 0, 0, 0)),
        spec((1, 1, 1, dim), lambda b, h: (b, h, 0, 0)),
    ]
    return pl.pallas_call(
        mixer_backward,
        out_shape=shapes,
        grid_spec=pltpu.PrefetchScalarGridSpec(
            num_scalar_prefetch=1,
            grid=(seqs, heads),
            in_specs=small + [spec((count, length, dim), lambda b, h: (0, b, h))] + saved,
            out_specs=outs,
        ),
        compiler_params=pltpu.CompilerParams(vmem_limit_bytes=56 * 2**20),
        cost_estimate=cost(26),
        name="mixer_backward",
    )(place, proj, taps, logits, gain, gout, *saved_values)


ANY = pl.BlockSpec(memory_space=pl.ANY)
FULL = pltpu.VMEM
PARAMS = pltpu.CompilerParams(vmem_limit_bytes=60 * 2**20)


def cost(micros):
    return pl.CostEstimate(flops=int(micros * 1.15e9), transcendentals=0, bytes_accessed=int(micros * 3.5e6))


def fetch(entries, refs, buf, sems):
    copies, n = [], 0
    for b, entry in enumerate(entries):
        row, mine = 0, []
        for size in entry:
            mine.append(pltpu.make_async_copy(refs[n], buf.at[b, pl.ds(row, size)], sems.at[n]))
            row, n = row + size, n + 1
        copies.append(mine)
    return copies


def start_all(copies):
    for mine in copies:
        for c in mine:
            c.start()


def stream(copies, outs):
    step, last = pl.program_id(0), len(copies) // 2 - 1

    @pl.when(step == 0)
    def _():
        start_all(copies)

    for i in range(last + 1):

        @pl.when(step == i)
        def _(i=i):
            for b in (2 * i, 2 * i + 1):
                for c in copies[b]:
                    c.wait()
                outs[b].start()

    def finish():
        @pl.when(step == last)
        def _():
            for out in outs:
                out.wait()

    return finish


def heights(entries):
    return [[a.shape[0] for a in entry] for entry in entries]


def flat(entries):
    return [a for entry in entries for a in entry]


def project_kernel(entries, *refs):
    n = sum(len(e) for e in entries)
    w_ref, beta_ref, proj_ref, logit_ref, all_ref, buf, sems, out_sems = refs[n:]
    count, rows, width = buf.shape
    outs = [pltpu.make_async_copy(buf.at[b], all_ref.at[b], out_sems.at[b]) for b in range(count)]
    finish = stream(fetch(entries, refs[:n], buf, sems), outs)
    x = buf[pl.ds(2 * pl.program_id(0), 2)].reshape(2 * rows, width)
    proj_ref[...] = dot(x, w_ref[...]).astype(LOW).reshape(proj_ref.shape)
    logit_ref[...] = dot(x, beta_ref[...], 1, 1).reshape(logit_ref.shape)
    finish()


def run_project(entries, w, beta, cols):
    sizes = heights(entries)
    count, rows = len(sizes), sum(sizes[0])
    pieces = flat(entries)
    width = pieces[0].shape[1]
    lanes = beta.shape[0]
    return pl.pallas_call(
        functools.partial(project_kernel, sizes),
        grid=(count // 2,),
        in_specs=[ANY] * len(pieces)
        + [
            pl.BlockSpec((width, cols), lambda g: (0, 0), pipeline_mode=pl.Buffered(1)),
            pl.BlockSpec(beta.shape, lambda g: (0, 0), pipeline_mode=pl.Buffered(1)),
        ],
        out_specs=[
            pl.BlockSpec((2, rows, cols), lambda g: (g, 0, 0)),
            pl.BlockSpec((2, rows, lanes), lambda g: (g, 0, 0)),
            ANY,
        ],
        out_shape=[
            jax.ShapeDtypeStruct((count, rows, cols), LOW),
            jax.ShapeDtypeStruct((count, rows, lanes), WIDE),
            jax.ShapeDtypeStruct((count, rows, width), LOW),
        ],
        scratch_shapes=[
            pltpu.VMEM((count, rows, width), LOW),
            pltpu.SemaphoreType.DMA((len(pieces),)),
            pltpu.SemaphoreType.DMA((count,)),
        ],
        compiler_params=PARAMS,
        cost_estimate=cost(16),
        name="project",
    )(*pieces, w, beta)


def gate_kernel(entries, others, *refs):
    n = sum(len(e) for e in entries)
    m = n + sum(len(e) for e in others)
    w_ref, inner_ref, up_ref, gate_ref, all_ref, side_ref = refs[m : m + 6]
    buf, side, sems, out_sems, side_sems, back_sems = refs[m + 6 :]
    count, rows, width = buf.shape
    outs = [pltpu.make_async_copy(buf.at[b], all_ref.at[b], out_sems.at[b]) for b in range(count)]
    backs = [pltpu.make_async_copy(side.at[b], side_ref.at[b], back_sems.at[b]) for b in range(count)]
    finish = stream(fetch(entries, refs[:n], buf, sems), outs)
    finish_side = stream(fetch(others, refs[n:m], side, side_sems), backs)
    ff = inner_ref.shape[-1]
    both = dot(buf[pl.ds(2 * pl.program_id(0), 2)].reshape(2 * rows, width), w_ref[...])
    gate, up = both[:, :ff], both[:, ff:]
    sig = jax.nn.sigmoid(gate)
    swish = gate * sig
    inner_ref[...] = (swish * up).astype(LOW).reshape(inner_ref.shape)
    gate_ref[...] = (up * sig * (1.0 + gate * (1.0 - sig))).astype(LOW).reshape(gate_ref.shape)
    up_ref[...] = swish.astype(LOW).reshape(up_ref.shape)
    finish()
    finish_side()


def run_gate(entries, others, w):
    sizes = heights(entries)
    beside = flat(others)
    count, rows = len(sizes), sum(sizes[0])
    pieces = flat(entries)
    width, ff = pieces[0].shape[1], w.shape[1] // 2
    return pl.pallas_call(
        functools.partial(gate_kernel, sizes, heights(others)),
        grid=(count // 2,),
        in_specs=[ANY] * (len(pieces) + len(beside))
        + [pl.BlockSpec(w.shape, lambda g: (0, 0), pipeline_mode=pl.Buffered(1))],
        out_specs=[pl.BlockSpec((2, rows, ff), lambda g: (g, 0, 0))] * 3 + [ANY] * 2,
        out_shape=[jax.ShapeDtypeStruct((count, rows, ff), LOW)] * 3
        + [jax.ShapeDtypeStruct((count, rows, width), LOW)] * 2,
        scratch_shapes=[
            pltpu.VMEM((count, rows, width), LOW),
            pltpu.VMEM((count, rows, width), LOW),
            pltpu.SemaphoreType.DMA((len(pieces),)),
            pltpu.SemaphoreType.DMA((count,)),
            pltpu.SemaphoreType.DMA((len(beside),)),
            pltpu.SemaphoreType.DMA((count,)),
        ],
        compiler_params=PARAMS,
        cost_estimate=cost(25),
        name="gate",
    )(*pieces, *beside, w)


def gate_back_kernel(cot_ref, up_ref, gate_ref, down_ref, w_ref, grad_ref, even_ref, odd_ref):
    _, rows, width = cot_ref.shape
    grad = dot(cot_ref[...].reshape(2 * rows, width), down_ref[...], 1, 1)
    gate, up = (r[...].reshape(2 * rows, r.shape[-1]).astype(WIDE) for r in (gate_ref, up_ref))
    both = jnp.concatenate([grad * gate, grad * up], axis=1).astype(LOW)
    grad_ref[...] = both.reshape(grad_ref.shape)
    two = dot(both, w_ref[...], 1, 1).astype(LOW)
    even_ref[0] = two[:rows]
    odd_ref[0] = two[rows:]


def run_gate_back(cot, up, gate, down, w):
    count, rows, width = cot.shape
    ff = up.shape[-1]

    def block(cols, depth=2):
        return pl.BlockSpec((depth, rows, cols), lambda b: (b, 0, 0))

    def once(x):
        return pl.BlockSpec(x.shape, lambda b: (0, 0), pipeline_mode=pl.Buffered(1))

    half = jax.ShapeDtypeStruct((count // 2, rows, width), LOW)
    return pl.pallas_call(
        gate_back_kernel,
        grid=(count // 2,),
        in_specs=[block(width), block(ff), block(ff), once(down), once(w)],
        out_specs=[block(2 * ff), block(width, 1), block(width, 1)],
        out_shape=[jax.ShapeDtypeStruct((count, rows, 2 * ff), LOW), half, half],
        compiler_params=PARAMS,
        cost_estimate=cost(32),
        name="gate_back",
    )(cot, up, gate, down, w)


def pairs_kernel(count, right, *refs):
    even_ref, odd_ref = refs[2 * count :]
    rows = even_ref.shape[1]
    total = 0.0
    for n in range(count):
        x, w = refs[n], refs[count + n]
        total = total + dot(x[...].reshape(2 * rows, x.shape[-1]), w[...], 1, right[n])
    total = total.astype(LOW)
    even_ref[0] = total[:rows]
    odd_ref[0] = total[rows:]


def run_pairs(terms, width, name, micros):
    count, rows, _ = terms[0][0].shape
    half = jax.ShapeDtypeStruct((count // 2, rows, width), LOW)
    weight_specs = []
    for x, w, right in terms:
        shape = (x.shape[-1], width) if right == 0 else (width, x.shape[-1])
        weight_specs.append(pl.BlockSpec(shape, lambda b: (0, 0), pipeline_mode=pl.Buffered(1)))
    return pl.pallas_call(
        functools.partial(pairs_kernel, len(terms), [t[2] for t in terms]),
        grid=(count // 2,),
        in_specs=[pl.BlockSpec((2, rows, t[0].shape[-1]), lambda b: (b, 0, 0)) for t in terms] + weight_specs,
        out_specs=[pl.BlockSpec((1, rows, width), lambda b: (b, 0, 0))] * 2,
        out_shape=[half, half],
        compiler_params=PARAMS,
        cost_estimate=cost(micros),
        name=name,
    )(*[t[0] for t in terms], *[t[1] for t in terms])


def branch_kernel(entries, place_ref, *refs):
    n = sum(len(e) for e in entries)
    count = len(entries)
    parts, (token_ref, gain_ref, hidden_ref, two_ref, rows_ref, buf, sems) = refs[n:-7], refs[-7:]
    copies = fetch(entries, refs[:n], buf, sems)
    start_all(copies)
    place = place_ref[0]
    wide = parts[0].shape[-1]

    def spot(b):
        return pl.ds(pl.multiple_of(jnp.bitwise_xor(place, b) * wide, wide), wide)

    for n, ref in enumerate(parts):
        length = ref.shape[1]
        for i in range(count):
            rows_ref[n * length : (n + 1) * length, i * wide : (i + 1) * wide] = ref[i]
    rows = rows_ref[...]
    for b, mine in enumerate(copies):
        for c in mine:
            c.wait()
        hidden_ref[:, spot(b)] = dot(rows, buf[b])
    hidden = hidden_ref[...] + token_ref[...].astype(WIDE)
    hidden_ref[...] = hidden
    scale = lax.rsqrt(jnp.mean(hidden * hidden, axis=-1, keepdims=True) + 1e-05)
    two_ref[...] = (hidden * scale * gain_ref[...]).astype(LOW)


def run_branch(place, entries, parts, tokens, gain):
    sizes = heights(entries)
    pieces = flat(entries)
    depth, wide = sum(sizes[0]), parts[0].shape[-1]
    vmem = pl.BlockSpec(memory_space=FULL)
    return pl.pallas_call(
        functools.partial(branch_kernel, sizes),
        in_specs=[pl.BlockSpec(memory_space=pltpu.SMEM)] + [ANY] * len(pieces) + [vmem] * (len(parts) + 2),
        out_specs=[vmem] * 3,
        out_shape=[
            jax.ShapeDtypeStruct(tokens.shape, WIDE),
            jax.ShapeDtypeStruct(tokens.shape, LOW),
            jax.ShapeDtypeStruct((tokens.shape[0], depth), LOW),
        ],
        scratch_shapes=[
            pltpu.VMEM((len(sizes), depth, wide), LOW),
            pltpu.SemaphoreType.DMA((len(pieces),)),
        ],
        compiler_params=PARAMS,
        cost_estimate=cost(10),
        name="branch",
    )(place, *pieces, *parts, tokens, gain)


def branch_back_kernel(entries, grads, place_ref, *refs):
    n = sum(len(e) for e in entries)
    m = sum(len(e) for e in grads)
    count = len(entries)
    adds, (hidden_ref, cot_ref, gain_ref) = refs[n : n + m], refs[n + m : n + m + 3]
    ghidden_ref, gsum_ref, gbranch_ref, gout_ref, buf, gout_all, sems = refs[n + m + 3 :]
    copies = fetch(entries, refs[:n], buf, sems)
    start_all(copies)
    place = place_ref[0]
    wide = gbranch_ref.shape[-1]
    total, at = 0.0, 0
    for entry in grads:
        here = [adds[at + i][...].astype(WIDE).reshape(-1, hidden_ref.shape[-1]) for i in range(len(entry))]
        at += len(entry)
        total = total + (jnp.concatenate(here) if len(here) > 1 else here[0])
    hidden = hidden_ref[...]
    scale = lax.rsqrt(jnp.mean(hidden * hidden, axis=-1, keepdims=True) + 1e-05)
    gsum_ref[...] = jnp.sum(total * hidden * scale, axis=0, keepdims=True)
    weighted = total * gain_ref[...]
    back = scale * weighted - hidden * (
        scale * scale * scale * jnp.mean(hidden * weighted, axis=-1, keepdims=True)
    )
    ghidden_ref[...] = cot_ref[...].astype(WIDE) + back

    def spot(b):
        return pl.ds(pl.multiple_of(jnp.bitwise_xor(place, b) * wide, wide), wide)

    for b, mine in enumerate(copies):
        for c in mine:
            c.wait()
        gbranch_ref[b] = ghidden_ref[:, b * wide : (b + 1) * wide].astype(LOW)
        part = dot(ghidden_ref[:, spot(b)], buf[b], 1, 1)
        if b == 0:
            gout_all[...] = part
        else:
            gout_all[...] += part
    for b in range(count):
        gout_ref[b] = gout_all[:, b * wide : (b + 1) * wide].astype(LOW)


def run_branch_back(place, entries, grads, hidden, cot, gain):
    sizes, grad_sizes = heights(entries), heights(grads)
    pieces, adds = flat(entries), flat(grads)
    count, depth, wide = len(sizes), sum(sizes[0]), pieces[0].shape[1]
    rows = hidden.shape[0]

    def first(x):
        shape = x.shape if len(x.shape) == 2 else (1,) + x.shape[1:]
        return pl.BlockSpec(shape, lambda g: (0,) * len(shape))

    def whole(shape):
        return pl.BlockSpec(shape, lambda g: (0,) * len(shape))

    return pl.pallas_call(
        functools.partial(branch_back_kernel, sizes, grad_sizes),
        grid=(1,),
        in_specs=[pl.BlockSpec(memory_space=pltpu.SMEM)]
        + [ANY] * len(pieces)
        + [first(x) for x in adds]
        + [whole(x.shape) for x in (hidden, cot, gain)],
        out_specs=[
            whole(hidden.shape),
            whole((1, hidden.shape[1])),
            whole((count, rows, wide)),
            whole((count, rows, wide)),
        ],
        out_shape=[
            jax.ShapeDtypeStruct(hidden.shape, WIDE),
            jax.ShapeDtypeStruct((1, hidden.shape[1]), WIDE),
            jax.ShapeDtypeStruct((count, rows, wide), LOW),
            jax.ShapeDtypeStruct((count, rows, wide), LOW),
        ],
        scratch_shapes=[
            pltpu.VMEM((count, depth, wide), LOW),
            pltpu.VMEM((rows, depth), WIDE),
            pltpu.SemaphoreType.DMA((len(pieces),)),
        ],
        compiler_params=PARAMS,
        cost_estimate=cost(10),
        name="branch_back",
    )(place, *pieces, *adds, hidden, cot, gain)


def outer_kernel(entries, place_ref, cols_ref, *refs):
    out_ref, total_ref = refs[-2:]
    at = 0
    for b, entry in enumerate(entries):
        cols = cols_ref[jnp.bitwise_xor(place_ref[0], b)]
        row = 0
        for size in entry:
            part = dot(refs[at][...], cols[row : row + size], 0, 0)
            total_ref[...] = part if at == 0 else total_ref[...] + part
            row, at = row + size, at + 1
    out_ref[...] = total_ref[...].astype(LOW)


def run_outer(place, entries, cols, name):
    pieces = flat(entries)
    shape = (pieces[0].shape[1], cols.shape[-1])
    vmem = pl.BlockSpec(memory_space=FULL)
    return pl.pallas_call(
        functools.partial(outer_kernel, heights(entries)),
        in_specs=[pl.BlockSpec(memory_space=pltpu.SMEM)] + [vmem] * (len(pieces) + 1),
        out_specs=vmem,
        out_shape=jax.ShapeDtypeStruct(shape, LOW),
        scratch_shapes=[pltpu.VMEM(shape, WIDE)],
        compiler_params=PARAMS,
        cost_estimate=cost(8),
        name=name,
    )(place, cols, *pieces)


def spread_kernel(entries, layout, place_ref, *refs):
    n = sum(len(e) for e in entries)
    out_ref, held = refs[n:]
    step, steps, at = pl.program_id(0), pl.num_programs(0), 0
    for b, entry in enumerate(entries):
        value = refs[at][...]
        if len(entry) > 1:
            value = jnp.where(step < steps // 2, value, refs[at + 1][...])
        held[jnp.bitwise_xor(place_ref[0], b)] = value
        at += len(entry)
    for i in range(len(entries)):
        for src, width, index in layout(i):
            out_ref[index] = held[i, :, src : src + width].astype(WIDE)


def run_spread(place, entries, piece_block, steps, layout, shape, block, index, name):
    specs = []
    for entry in entries:
        if len(entry) > 1:
            specs.append(pl.BlockSpec(piece_block, lambda g: (jnp.minimum(g, steps // 2 - 1), 0)))
            specs.append(pl.BlockSpec(piece_block, lambda g: (jnp.maximum(g - steps // 2, 0), 0)))
        elif piece_block[0] == entry[0].shape[0]:
            specs.append(pl.BlockSpec(piece_block, lambda g: (0, g)))
        else:
            specs.append(pl.BlockSpec(piece_block, lambda g: (g, 0)))
    return pl.pallas_call(
        functools.partial(spread_kernel, heights(entries), layout),
        grid=(steps,),
        in_specs=[pl.BlockSpec(memory_space=pltpu.SMEM)] + specs,
        out_specs=pl.BlockSpec(block, index),
        out_shape=jax.ShapeDtypeStruct(shape, WIDE),
        scratch_shapes=[pltpu.VMEM((len(entries),) + piece_block, LOW)],
        compiler_params=PARAMS,
        cost_estimate=cost(10),
        name=name,
    )(place, *flat(entries))


def norm_back(values, scale, grad, gain):
    weighted = grad * gain
    return scale * weighted - values * scale**3 * jnp.mean(values * weighted, axis=-1, keepdims=True)


def local(
    tokens,
    cotangent,
    gain_first,
    w_inputs,
    w_conv,
    w_beta,
    gain_heads,
    w_output,
    gain_second,
    w_gate_up,
    w_down,
):
    shards, count, place = lax.axis_size("fsdp"), lax.axis_size("seq"), lax.axis_index("seq")
    shard = lax.axis_index("fsdp")
    seqs, length, width = tokens.shape
    rows = seqs * length
    part = width // shards
    all_heads = w_beta.shape[1]
    heads = all_heads // count
    wide = heads * (w_output.shape[0] * shards // all_heads)
    dim = wide // heads
    hidden_part = w_down.shape[0]
    piece = hidden_part // count
    taps = w_conv.shape[1]
    place_arr = jnp.reshape(place, (1,)).astype(jnp.int32)

    def over_shards(x, axis=0):
        return lax.all_gather(x, "fsdp", axis=axis, tiled=True)

    packed = jnp.concatenate(
        [
            gain_first[None],
            gain_second[None],
            jnp.pad(gain_heads[None], ((0, 0), (0, part - gain_heads.shape[0]))),
            w_conv.reshape(3 * taps, part),
            w_beta.T,
        ]
    )
    packed = lax.all_gather(packed, "fsdp", axis=0)
    first_weight = packed[:, 0].reshape(width).astype(WIDE)
    second_weight = packed[:, 1].reshape(width).astype(WIDE)
    head_weight = packed[:, 2, : gain_heads.shape[0]].reshape(1, dim).astype(WIDE)
    conv_all = packed[:, 3 : 3 + 3 * taps].transpose(1, 0, 2).reshape(3, taps, width)
    conv_own = lax.dynamic_slice_in_dim(conv_all, place * wide, wide, 2).astype(WIDE)
    conv_own = conv_own.reshape(3, taps, heads, dim).transpose(2, 0, 1, 3)
    beta_all = packed[:, 3 + 3 * taps :].transpose(1, 0, 2).reshape(all_heads, width)
    beta_own = lax.dynamic_slice_in_dim(beta_all, place * heads, heads, 0)
    beta_own = jnp.pad(beta_own, ((0, 128 - heads), (0, 0)))

    ff = piece * shards
    win = lax.dynamic_slice_in_dim(w_inputs, place * wide, wide, 2)
    win = win.reshape(3, part, heads, dim).transpose(1, 2, 0, 3).reshape(part, 3 * wide)
    wio = jnp.concatenate([win, lax.dynamic_slice_in_dim(w_output, place * wide, wide, 1)], axis=1)
    later = after(place, wio)
    pieces = [
        lax.dynamic_slice(w_gate_up, (0, 0, f * hidden_part + later * piece), (2, part, piece)) for f in range(shards)
    ]
    wgu_own = jnp.concatenate([p[c] for c in range(2) for p in pieces], axis=1)
    later = after(later, wgu_own)
    wdown_own = lax.dynamic_slice_in_dim(w_down, later * piece, piece, 0)
    wio = over_shards(wio)
    wgu = over_shards(wgu_own)
    wdown = over_shards(wdown_own)

    inputs = tokens.reshape(rows, width).astype(WIDE)
    first_scale = lax.rsqrt(jnp.mean(inputs * inputs, axis=-1, keepdims=True) + 1e-05)
    normed = (inputs * first_scale * first_weight).astype(LOW)
    cot_own = cotangent.reshape(rows, width)
    cot_first = gather_start(cot_own)
    normed_first = gather_start(after(normed, wgu_own, wdown_own, *cot_first))
    normed_far = gather_far(normed_first)
    normed_parts = gather_rest(normed_first, normed_far)
    cot_far = gather_far([after(c, *normed_far) for c in cot_first])
    cot_parts = gather_rest(cot_first, cot_far)

    wio_late = after(wio, *normed_far, *cot_far)
    proj, logits, normed_all = run_project(normed_parts, wio_late, beta_own, 3 * wide)
    wout_first = gather_start(wio_late[:, 3 * wide :])
    proj = proj.reshape(count, seqs, length, 3 * wide)
    logits = logits.reshape(count, seqs, length, 128)
    wout_far, out_parts, saved = [], [], None
    for b in range(seqs):
        late = [after(proj, *wout_first), after(proj, *wout_far)][min(b - 1, 1)] if b else proj
        mixed_out, *saved = run_mixer_forward(b, place_arr, late, conv_own, logits, head_weight, saved)
        if b == 0:
            wout_far = gather_far(wout_first)
            wout_parts = gather_rest(wout_first, wout_far)
        if b == seqs - 1:
            mixed_out = after(mixed_out, *wout_far, *out_parts)
        out_parts.append(exchange(mixed_out))
    hidden, normed_two, out_rows = run_branch(
        place_arr, wout_parts, out_parts, tokens.reshape(rows, width), second_weight[None]
    )
    two_parts = gather_xor(normed_two)
    inner, up_slope, gate_slope, two_all, cot_all = run_gate(two_parts, cot_parts, wgu)

    def to_owner(partial):
        return lax.psum_scatter(partial, "fsdp", scatter_dimension=0, tiled=True)

    out_first = gather_start(after(out_rows, *two_parts[6]))
    up_slope = after(up_slope, *out_first)
    ggu, gtwo_even, gtwo_odd = run_gate_back(cot_all, up_slope, gate_slope, wdown, wgu)
    gtwo_twin = reduce_start(gtwo_odd)
    gwdown = jnp.einsum("brf,brd->fd", after(inner, ggu), cot_all, preferred_element_type=WIDE).astype(LOW)
    gtwo_even, gwdown = lax.optimization_barrier((gtwo_even, gwdown))
    gwdown = to_owner(gwdown)
    gtwo_state = reduce_add(gtwo_even, gtwo_twin)
    ggu, *gtwo_state = lax.optimization_barrier((ggu, *gtwo_state))
    gtwo_state = reduce_far(gtwo_state)
    gwgu = jnp.einsum("brd,brf->df", two_all, ggu, preferred_element_type=WIDE).astype(LOW)
    gtwo_state[0], gwgu = lax.optimization_barrier((gtwo_state[0], gwgu))
    gtwo_parts = reduce_last(reduce_more(gtwo_state))
    down_even, down_odd = run_pairs([(after(inner, gwgu), wdown, 0)], width, "down", 12)
    hidden_late = after(hidden, down_odd)
    gwgu = to_owner(gwgu)

    ghidden, gsecond, gbranch, gout = run_branch_back(
        place_arr, wout_parts, gtwo_parts, hidden_late, cot_own, second_weight[None]
    )
    down_twin = reduce_start(after(down_odd, ghidden))
    gout = exchange(gout)
    down_state = reduce_add(down_even, down_twin)
    gout, gwdown, *down_state = lax.optimization_barrier((gout, gwdown, *down_state))
    gwdown_first = gather_start(gwdown, True)
    out_far = gather_far([after(x, gout) for x in out_first])
    down_state = reduce_far(down_state)
    gproj, glogit, gtaps, ggain = run_mixer_backward(
        place_arr, proj, conv_own, logits, head_weight, gout, saved
    )
    gbranch_cols = exchange(after(gbranch, gproj))
    gproj, *both = lax.optimization_barrier((gproj, *out_far, *down_state))
    out_far, down_state = both[: len(out_far)], both[len(out_far) :]
    gproj = gproj.reshape(count, rows, 3 * wide)
    glogit = glogit.reshape(count, rows, 128)
    gnormed_even, gnormed_odd = run_pairs([(gproj, wio, 1), (glogit, beta_own, 0)], width, "input_back", 1)
    gnormed_twin = reduce_start(gnormed_odd)
    gbeta = jnp.einsum(
        "brh,brd->hd", after(glogit, gnormed_even), normed_all, preferred_element_type=WIDE
    )[:heads]
    gnormed_twin, gbeta, gbranch_cols, *gwdown_first = lax.optimization_barrier(
        (gnormed_twin, gbeta, gbranch_cols, *gwdown_first)
    )
    gnormed_state = reduce_add(gnormed_even, gnormed_twin)
    gproj, gnormed_odd = lax.optimization_barrier((gproj, gnormed_odd))
    gwin = jnp.einsum("brd,bre->de", normed_all, gproj, preferred_element_type=WIDE).astype(LOW)
    gnormed_state = reduce_far(gnormed_state)
    gwin = to_owner(gwin)
    gnormed_state = reduce_more(gnormed_state)
    gnormed = reduce_last(gnormed_state)
    down_state[0] = after(down_state[0], *gnormed_state)
    down_state = reduce_more(down_state)
    gwgu_first = gather_start(after(gwgu, *[e[-1] for e in gnormed]), True)
    gnormed = total_of(gnormed)
    input_grad = ghidden + norm_back(inputs, first_scale, gnormed, first_weight)
    gfirst = jnp.sum(gnormed * inputs * first_scale, axis=0)


    out_all_parts = gather_rest(out_first, out_far)
    gwout = run_outer(place_arr, out_all_parts, after(gbranch_cols, *gnormed_state), "output_weights")
    gtaps = jnp.sum(gtaps, axis=0).transpose(1, 2, 0, 3).reshape(3 * taps, wide)
    ggain = jnp.sum(ggain, axis=(0, 1)).reshape(shards, 1, dim // shards)
    ggain = jnp.pad(ggain, ((0, 0), (0, 0), (0, wide - dim // shards)))
    owner = (iota((shards, 1, 1), 0) == place * wide // part).astype(WIDE)
    cells = part // wide
    gains = jnp.stack([gfirst, gsecond[0]]).reshape(2, shards, cells, wide).transpose(1, 0, 2, 3)
    gbeta = gbeta.reshape(heads, shards, cells, wide).transpose(1, 0, 2, 3)
    extra = jnp.concatenate(
        [
            gains.reshape(shards, 2 * cells, wide),
            gbeta.reshape(shards, heads * cells, wide),
            owner * gtaps[None],
            ggain,
        ],
        axis=1,
    )
    used = extra.shape[1]
    extra = jnp.pad(extra, ((0, 0), (0, -used % 32), (0, 0))).astype(LOW)
    more = extra.shape[1]
    gwout = jnp.concatenate([gwout.reshape(shards, part, wide), extra], axis=1)
    gwout = gwout.reshape(shards * (part + more), wide)
    gwgu_first, gwout = lax.optimization_barrier((gwgu_first, gwout))
    gwgu_far = gather_far(gwgu_first)
    gwout = to_owner(gwout)

    gwgu_parts = gather_rest(gwgu_first, gwgu_far)
    tall = min(128, part)
    gwin_first = gather_start(after(gwin, *gwgu_first))
    gwgu = run_spread(
        place_arr,
        gwgu_parts,
        (tall, 2 * ff),
        part // tall,
        lambda i: [
            (
                c * ff + f * piece,
                piece,
                (c, slice(None), slice(f * hidden_part + i * piece, f * hidden_part + (i + 1) * piece)),
            )
            for c in range(2)
            for f in range(shards)
        ],
        (2, part, hidden_part * shards),
        (2, tall, hidden_part * shards),
        lambda g: (0, g, 0),
        "spread_gate_up",
    )
    gwin_far = gather_far([after(g, gwgu) for g in gwin_first])
    down_state, gwdown_first, gwin_far = lax.optimization_barrier((down_state, gwdown_first, gwin_far))
    gwdown_far = gather_far(gwdown_first)
    down = reduce_last(down_state)
    output = (hidden + total_of(down)).astype(LOW)
    gwdown_parts = gather_rest(gwdown_first, gwdown_far)
    lanes = min(512, width)
    gwdown = run_spread(
        place_arr,
        gwdown_parts,
        (piece, lanes),
        width // lanes,
        lambda i: [(0, lanes, (slice(i * piece, (i + 1) * piece), slice(None)))],
        (hidden_part, width),
        (hidden_part, lanes),
        lambda g: (0, g),
        "spread_down",
    )
    gwin_parts = gather_rest(gwin_first, gwin_far)
    gwout_first = gather_start(after(gwout, *gwin_first))
    gwout_parts = gather_rest(gwout_first, gather_far(gwout_first, False))
    gwin = run_spread(
        place_arr,
        gwin_parts,
        (tall, 3 * wide),
        part // tall,
        lambda i: [
            (
                (h * 3 + c) * dim,
                dim,
                (c, slice(None), slice((i * heads + h) * dim, (i * heads + h + 1) * dim)),
            )
            for c in range(3)
            for h in range(heads)
        ],
        (3, part, width),
        (3, tall, width),
        lambda g: (0, g, 0),
        "spread_inputs",
    )
    gwout = run_spread(
        place_arr,
        gwout_parts,
        (tall, wide),
        part // tall,
        lambda i: [(0, wide, (slice(None), slice(i * wide, (i + 1) * wide)))],
        (part, width),
        (tall, width),
        lambda g: (g, 0),
        "spread_output",
    )
    extra = jnp.stack([e[0][part:] for e in gwout_parts]).astype(WIDE)
    summed = jnp.sum(extra, axis=0)
    gains = summed[: 2 * cells].reshape(2, part)
    ggain = summed[used - 1, : dim // shards]
    gbeta, gtaps = [], []
    for i in range(count):
        rows_i = lax.dynamic_index_in_dim(extra, place ^ i, 0, False)
        gbeta.append(rows_i[2 * cells : (2 + heads) * cells].reshape(heads, part))
    for i in range(cells):
        rows_i = lax.dynamic_index_in_dim(extra, place ^ (shard * cells + i), 0, False)
        gtaps.append(rows_i[(2 + heads) * cells : used - 1])
    gbeta = jnp.concatenate(gbeta).T
    gtaps = jnp.concatenate(gtaps, axis=1).reshape(3, taps, part)
    return (
        output.reshape(tokens.shape),
        input_grad.reshape(tokens.shape),
        gains[0],
        gwin,
        gtaps,
        gbeta,
        ggain,
        gwout,
        gains[1],
        gwgu,
        gwdown,
    )


def solution(mesh):
    in_specs = (
        P("fsdp", "seq", None),
        P("fsdp", "seq", None),
        P("fsdp"),
        P(None, "fsdp", None),
        P(None, None, "fsdp"),
        P("fsdp", None),
        P("fsdp"),
        P("fsdp", None),
        P("fsdp"),
        P(None, "fsdp", None),
        P("fsdp", None),
    )
    out_specs = (
        P("fsdp", "seq", None),
        P("fsdp", "seq", None),
        P("fsdp"),
        P(None, "fsdp", None),
        P(None, None, "fsdp"),
        P("fsdp", None),
        P("fsdp"),
        P("fsdp", None),
        P("fsdp"),
        P(None, "fsdp", None),
        P("fsdp", None),
    )
    return jax.shard_map(local, mesh=mesh, in_specs=in_specs, out_specs=out_specs, check_vma=False)
```
